256 devices in a mesh: freq: 64 (over x, z, core), kgrp: 4 (over y).
Axes of the slice: x: 4, y: 4, z: 8, core: 2. Of those that a mesh axis runs over, the one named last changes fastest.
Arguments:
- hamiltonian: float32 [256, 64, 128], P(('freq', 'kgrp')), may hold values from -1 to 1, as said below
- self_energy: float32 [128, 64, 128], P('freq'), may hold values from -0.8 to 0.3, as said below
- guess_factor: float32 [128, 64, 128], P('freq'), may hold values from -0.05 to 1.25
- weights: int32 [256], replicated, may hold values from 1 to 48
- counts: int32 [128], replicated, may hold values from 1 to 3, as said below
Outputs:
- local_green: float32 [4096, 256], P(('freq', 'kgrp'))
The draws below stay inside these ranges and needn't reach their ends.
Inputs may be any that keep to these rules, and one draw needn't show every extreme that they name: `hamiltonian`: each k-point's matrix is Hermitian: the left half symmetric, the right half antisymmetric. `self_energy`: the diagonal of the right half lies between -0.8 and -0.4. `counts`: the number of Newton-Schulz steps taken at each frequency.
All inputs are finite; a program needn't handle non-finite values.
Results may differ from the reference program's by a relative error of at most 0.0001.
Values sent between devices are 32-bit elements.
A program may use at most 64 MiB of HBM per device.

```python
import math
import jax
import jax.numpy as jnp
from jax import lax

NORB = 64
MAXIT = 3
FREQ = 128
KPTS = 256


def noise_draw(key, shape, spread):
    return jax.random.truncated_normal(key, -4.0, 4.0, shape, jnp.float32) * spread


def draw_hamiltonian(key, part):
    first_key, second_key, third_key = jax.random.split(key, 3)
    identity = jnp.eye(NORB, dtype=jnp.float32)
    left_noise = noise_draw(first_key, (KPTS, NORB, NORB), 0.018)
    right_noise = noise_draw(second_key, (KPTS, NORB, NORB), 0.018)
    symmetric = (left_noise + jnp.swapaxes(left_noise, 1, 2)) * 0.70710678 * (1.0 - identity)
    skewed = (right_noise - jnp.swapaxes(right_noise, 1, 2)) * 0.70710678
    levels = jax.random.uniform(third_key, (KPTS, NORB), jnp.float32, -1.0, 1.0)
    real_part = symmetric + levels[:, :, None] * identity
    return jnp.concatenate([real_part, skewed], -1).astype(jnp.float32)


def draw_self_energy(key, part):
    first_key, second_key, third_key, fourth_key = jax.random.split(key, 4)
    identity = jnp.eye(NORB, dtype=jnp.float32)
    real_off = noise_draw(first_key, (FREQ, NORB, NORB), 0.012) * (1.0 - identity)
    imag_off = noise_draw(second_key, (FREQ, NORB, NORB), 0.012) * (1.0 - identity)
    real_diag = jax.random.uniform(third_key, (FREQ, NORB), jnp.float32, -0.3, 0.3)
    damping = jax.random.uniform(fourth_key, (FREQ, NORB), jnp.float32, -0.8, -0.4)
    real_part = real_off + real_diag[:, :, None] * identity
    imag_part = imag_off + damping[:, :, None] * identity
    return jnp.concatenate([real_part, imag_part], -1).astype(jnp.float32)


def draw_guess_factor(key, part):
    first_key, second_key, third_key = jax.random.split(key, 3)
    identity = jnp.eye(NORB, dtype=jnp.float32)
    real_off = noise_draw(first_key, (FREQ, NORB, NORB), 0.01) * (1.0 - identity)
    imag_part = noise_draw(second_key, (FREQ, NORB, NORB), 0.01)
    scales = jax.random.uniform(third_key, (FREQ, NORB), jnp.float32, 0.75, 1.25)
    real_part = real_off + scales[:, :, None] * identity
    return jnp.concatenate([real_part, imag_part], -1).astype(jnp.float32)


def draw_counts(key, part):
    positions = jnp.arange(FREQ, dtype=jnp.int32)
    extra = jax.random.randint(key, (FREQ,), 0, 4)
    lowest = (8 * positions < FREQ).astype(jnp.int32)
    bumped = ((extra == 0) & (positions < FREQ - 1)).astype(jnp.int32)
    return jnp.minimum(MAXIT, 1 + 2 * lowest + bumped).astype(jnp.int32)


def set_ends(drawn, stream_key, smallest, high):
    longest = drawn.shape.index(max(drawn.shape))
    spots = []
    for shift in (0, 1):
        where = [jax.random.randint(jax.random.fold_in(stream_key, axis), (), 0, length) for axis, length in enumerate(drawn.shape)]
        where[longest] = (where[longest] + shift) % drawn.shape[longest]
        spots.append(tuple(where))
    return drawn.at[spots[0]].set(smallest).at[spots[1]].set(high)


def setup_inputs(seed: int = 0) -> dict:
    keys = jax.random.split(jax.random.key(seed), 6)
    hamiltonian = draw_hamiltonian(jax.random.fold_in(keys[5], 71), 0)
    self_energy = draw_self_energy(jax.random.fold_in(keys[5], 71), 0)
    guess_factor = draw_guess_factor(jax.random.fold_in(keys[5], 71), 0)
    weights = set_ends(jax.random.randint(keys[3], (KPTS,), 1, 49), jax.random.fold_in(keys[3], 1), 1, 48).astype(jnp.int32)
    counts = draw_counts(jax.random.fold_in(keys[5], 71), 0)
    return dict(hamiltonian=hamiltonian, self_energy=self_energy, guess_factor=guess_factor, weights=weights, counts=counts)


chem_potential = 0.2


def blockify(right_side):
    order = right_side.shape[-1] // 2
    real_part = right_side[..., :order]
    imag_part = right_side[..., order:]
    upper_row = jnp.concatenate([real_part, imag_part], -1)
    lower_row = jnp.concatenate([-imag_part, real_part], -1)
    return jnp.concatenate([upper_row, lower_row], -2)


def complex_product(left_side, right_side):
    return jnp.einsum('...ij,...jl->...il', left_side, blockify(right_side), precision=lax.Precision.HIGHEST)


def build_matrix(kpoint_rows, sigma_rows, matsubara):
    orbitals = kpoint_rows.shape[1]
    identity = jnp.eye(orbitals, dtype=jnp.float32)
    real_shift = jnp.broadcast_to(chem_potential * identity, matsubara.shape + identity.shape)
    imag_shift = matsubara[:, None, None] * identity
    diagonal_shift = jnp.concatenate([real_shift, imag_shift], -1)
    return diagonal_shift[:, None] - kpoint_rows[None] - sigma_rows[:, None]


def start_guess(matrix, factor_rows):
    orbitals = matrix.shape[-2]
    diag_real = jnp.diagonal(matrix[..., :orbitals], axis1=-2, axis2=-1)
    diag_imag = jnp.diagonal(matrix[..., orbitals:], axis1=-2, axis2=-1)
    modulus = diag_real * diag_real + diag_imag * diag_imag
    recip_real = (diag_real / modulus)[..., None]
    recip_imag = (-diag_imag / modulus)[..., None]
    factor_real = factor_rows[..., :orbitals]
    factor_imag = factor_rows[..., orbitals:]
    guess_real = recip_real * factor_real - recip_imag * factor_imag
    guess_imag = recip_real * factor_imag + recip_imag * factor_real
    return jnp.concatenate([guess_real, guess_imag], -1)


def reference(hamiltonian, self_energy, guess_factor, weights, counts):
    orbitals = hamiltonian.shape[1]
    factors = weights.astype(jnp.float32)
    weight_total = jnp.sum(factors)
    identity = jnp.eye(orbitals, dtype=jnp.float32)
    doubled = jnp.concatenate([2.0 * identity, jnp.zeros_like(identity)], -1)

    def one_frequency(inputs):
        sigma_row, factor_row, step_count, freq_id = inputs
        matsubara = (2 * freq_id + 1).astype(jnp.float32)[None] * (math.pi / (2 * FREQ))
        matrix = build_matrix(hamiltonian, sigma_row[None], matsubara)
        initial = start_guess(matrix, factor_row[None, None])

        def newton_step(sweep, current):
            return complex_product(current, doubled - complex_product(matrix, current))

        final = lax.fori_loop(0, step_count, newton_step, initial)
        summed = jnp.einsum('k,fkij->fij', factors, final, precision=lax.Precision.HIGHEST)
        return summed[0] / weight_total

    greens = lax.map(one_frequency, (self_energy, guess_factor, counts, jnp.arange(FREQ, dtype=jnp.int32)))
    arranged = greens.reshape(FREQ, orbitals, 2, orbitals).transpose(1, 3, 2, 0)
    return arranged.reshape(orbitals * orbitals, 2 * FREQ)
```

```python
import functools
import math

import jax
import jax.numpy as jnp
from jax import lax
from jax.experimental import pallas as pl
from jax.experimental.pallas import tpu as pltpu
from jax.sharding import PartitionSpec as P

chem_potential = 0.2

NORB = 64
WIDE = 2 * NORB
XS, YS, ZS, CORES = 4, 4, 8, 2
LINE = ZS * CORES
PER_FREQ = 2
N_LOCAL = XS * PER_FREQ
PAIRS = LINE // 2
FREQ = 128
KPTS = 256
BF = jnp.bfloat16
F32 = jnp.float32


def vmem():
    return pl.BlockSpec(memory_space=pltpu.VMEM)


def smem():
    return pl.BlockSpec(memory_space=pltpu.SMEM)


def on_freq(index):
    return {"freq": index}


def greet(targets):
    barrier = pltpu.get_barrier_semaphore()
    for target in targets:
        pl.semaphore_signal(barrier, inc=1, device_id=target, device_id_type=pl.DeviceIdType.MESH)
    pl.semaphore_wait(barrier, len(targets))


def send(src, dst, send_sem, recv_sem, target):
    return pltpu.make_async_remote_copy(
        src_ref=src,
        dst_ref=dst,
        send_sem=send_sem,
        recv_sem=recv_sem,
        device_id=target,
        device_id_type=pl.DeviceIdType.MESH,
    )


Z_ORDER = (4, 3, 5, 2, 6, 1, 7)


def gather_kernel(h_ref, s_ref, g_ref, hall, sall, gall, zs, zr, ps, pr, ss, sr, gs, gr):
    f = lax.axis_index("freq")
    x, t = f // LINE, f % LINE
    z, c = t // CORES, t % CORES
    partner = on_freq(x * LINE + z * CORES + (1 - c))

    def along_z(dz):
        return on_freq(x * LINE + (z + dz) % ZS * CORES + c)

    def along_x(dx):
        return on_freq((x + dx) % XS * LINE + t)

    greet([partner] + [along_z(dz) for dz in range(1, ZS)] + [along_x(dx) for dx in range(1, XS)])
    started = []
    for dz in Z_ORDER:
        copy = send(h_ref.at[0], hall.at[t], zs.at[dz], zr.at[dz], along_z(dz))
        copy.start()
        started.append(copy)
    copy = send(h_ref.at[0], hall.at[t], ps.at[0], pr.at[0], partner)
    copy.start()
    started.append(copy)
    mine = pl.ds(x * PER_FREQ, PER_FREQ)
    for dx in (2, 1, 3):
        for src, dst, s_sem, r_sem in ((g_ref, gall, gs, gr), (s_ref, sall, ss, sr)):
            copy = send(src, dst.at[mine], s_sem.at[dx], r_sem.at[dx], along_x(dx))
            copy.start()
            started.append(copy)
    hall[pl.ds(t, 1)] = h_ref[...]
    sall[mine] = s_ref[...]
    gall[mine] = g_ref[...]
    for dz in (1, 7, 2, 6, 3, 5, 4):
        source = (z + ZS - dz) % ZS * CORES + c
        send(h_ref.at[0], hall.at[source], zs.at[dz], zr.at[dz], along_z(dz)).wait_recv()
        copy = send(hall.at[source], hall.at[source], ps.at[dz], pr.at[dz], partner)
        copy.start()
        started.append(copy)
    for dx in (1, 3, 2):
        theirs = pl.ds((x + XS - dx) % XS * PER_FREQ, PER_FREQ)
        for src, dst, s_sem, r_sem in ((g_ref, gall, gs, gr), (s_ref, sall, ss, sr)):
            send(src, dst.at[theirs], s_sem.at[dx], r_sem.at[dx], along_x(dx)).wait_recv()
    for dz in range(ZS):
        source = (z + ZS - dz) % ZS * CORES + (1 - c)
        send(h_ref.at[0], hall.at[source], ps.at[dz], pr.at[dz], partner).wait_recv()
    for copy in started:
        copy.wait_send()


def gather(hamiltonian, self_energy, guess_factor):
    dma = pltpu.SemaphoreType.DMA
    return pl.pallas_call(
        gather_kernel,
        name="gather",
        out_shape=(
            jax.ShapeDtypeStruct((LINE, NORB, WIDE), F32),
            jax.ShapeDtypeStruct((N_LOCAL, NORB, WIDE), F32),
            jax.ShapeDtypeStruct((N_LOCAL, NORB, WIDE), F32),
        ),
        in_specs=[vmem()] * 3,
        out_specs=(vmem(),) * 3,
        scratch_shapes=[dma((ZS,))] * 4 + [dma((XS,))] * 4,
        compiler_params=pltpu.CompilerParams(collective_id=0, has_side_effects=True),
    )(hamiltonian, self_energy, guess_factor)


def halves(value):
    high = value.astype(BF)
    low = (value - high.astype(F32)).astype(BF)
    return high, low


def dot(left, right):
    return jnp.dot(left, right, preferred_element_type=F32)


def product3(left, right):
    left_high, left_low = left
    right_high, right_low = right
    return dot(
        jnp.concatenate([left_high, left_low], 1), jnp.concatenate([right_high, right_high], 0)
    ) + dot(left_high, right_low)


def invert_kernel(w_ref, n_ref, h_ref, s_ref, g_ref, out_ref, wh, wl, hcol, hrow, gcat, gz, zcol, zrow, er_ref, ei_ref, gh_ref, x_ref):
    f = lax.axis_index("freq")
    y = lax.axis_index("kgrp")
    x, t = f // LINE, f % LINE
    rows = lax.broadcasted_iota(jnp.int32, (NORB, WIDE), 0)
    lanes = lax.broadcasted_iota(jnp.int32, (NORB, WIDE), 1)
    first = lanes < NORB
    eye_mask = rows == lanes % NORB
    eye = eye_mask.astype(F32)
    first_bf = first.astype(F32).astype(BF)
    second_bf = (1.0 - first.astype(F32)).astype(BF)

    def swap(value):
        return pltpu.roll(value, NORB, 1)

    def paired(one, two):
        return jnp.where(first, one, swap(two)), jnp.where(first, swap(one), two)

    def as_right(real, imag):
        real_high, real_low = halves(real)
        imag_high, imag_low = halves(imag)
        high = jnp.concatenate(
            [jnp.concatenate([real_high, imag_high], 1), jnp.concatenate([-imag_high, real_high], 1)], 0
        )
        low = jnp.concatenate(
            [jnp.concatenate([real_low, imag_low], 1), jnp.concatenate([-imag_low, real_low], 1)], 0
        )
        return high, low

    def diagonal_columns(value):
        kept = jnp.where(eye_mask, value, 0.0)
        left = jnp.sum(jnp.where(first, kept, 0.0), 1, keepdims=True)
        right = jnp.sum(jnp.where(first, 0.0, kept), 1, keepdims=True)
        return jnp.where(first, left, right)

    def diagonal_row(value):
        return jnp.sum(jnp.where(eye_mask, value, 0.0), 0, keepdims=True)

    def add_up(i, total):
        for j in range(16):
            total = total + w_ref[i * 16 + j]
        return total

    inv_total = 1.0 / lax.fori_loop(0, KPTS // 16, add_up, jnp.int32(0)).astype(F32)

    def prepare_pair(p, carry):
        real, imag = paired(h_ref[2 * p], h_ref[2 * p + 1])
        high, low = as_right(real, imag)
        wh[p] = high
        wl[p] = low
        hcol[p] = diagonal_columns(real)
        hrow[p] = jnp.broadcast_to(diagonal_row(real), (8, WIDE))
        return carry

    lax.fori_loop(0, PAIRS, prepare_pair, 0)

    def prepare_freq(n, carry):
        freq_id = n // PER_FREQ * (PER_FREQ * LINE) + t * PER_FREQ + n % PER_FREQ
        matsubara = (2 * freq_id + 1).astype(F32) * (math.pi / (2 * FREQ))
        shift = jnp.where(first, chem_potential, matsubara)
        zed = jnp.where(eye_mask, shift, 0.0) - s_ref[n]
        real, imag = paired(zed, zed)
        g_high, g_low = halves(g_ref[n])
        gz[n] = product3((g_high, g_low), as_right(real, imag))
        gcat[n] = jnp.concatenate([g_high, g_low], 1)
        zcol[n] = jnp.concatenate([diagonal_columns(real), diagonal_columns(imag)], 1)
        row = jnp.concatenate([diagonal_row(real), diagonal_row(imag)], 1)
        zrow[n] = jnp.broadcast_to(row, (8, 2 * WIDE))
        return carry

    lax.fori_loop(0, N_LOCAL, prepare_freq, 0)

    def residual_pair(p, carry):
        left = gcat[...].reshape(N_LOCAL * NORB, 2 * WIDE)
        high = wh[p]
        gh_ref[...] = dot(left, jnp.concatenate([high, high], 0)) + dot(left[:, :WIDE], wl[p])
        h_diag = hcol[p]

        def one_freq(n, inner):
            gh = gh_ref[pl.ds(pl.multiple_of(n * NORB, NORB), NORB)]
            a = gz[n] - gh
            a_real, a_imag = a[:, :WIDE], a[:, WIDE:]
            d = zcol[n]
            d_real, d_imag = d[:, :WIDE] - h_diag, d[:, WIDE:]
            inv = 1.0 / (d_real * d_real + d_imag * d_imag)
            v_real, v_imag = d_real * inv, d_imag * inv
            er_ref[n, p] = eye - (v_real * a_real + v_imag * a_imag)
            ei_ref[n, p] = v_imag * a_real - v_real * a_imag
            return inner

        return lax.fori_loop(0, N_LOCAL, one_freq, carry, unroll=2)

    lax.fori_loop(0, PAIRS, residual_pair, 0)

    def column_scale(n, p):
        d = zrow[n]
        d_real, d_imag = d[:, :WIDE] - hrow[p], d[:, WIDE:]
        kpt = (x * LINE + 2 * p) * YS + y
        w_one = w_ref[kpt].astype(F32) * inv_total
        w_two = w_ref[kpt + YS].astype(F32) * inv_total
        weight = jnp.where(first[:8], w_one, w_two)
        inv = weight / (d_real * d_real + d_imag * d_imag)
        return (d_real * inv)[:1], (-d_imag * inv)[:1]

    def right_blocks(real, imag):
        def build(r, i):
            return jnp.concatenate(
                [
                    jnp.concatenate([r * first_bf, i * first_bf], 1),
                    jnp.concatenate([r * second_bf, i * second_bf], 1),
                ],
                0,
            )

        r_high, r_low = halves(real)
        i_high, i_low = halves(imag)
        return build(r_high, i_high), build(r_low, i_low)

    def left_rows(real, imag):
        return halves(jnp.concatenate([real, imag], 0))

    def combine(out):
        return out[:NORB, :WIDE] - out[NORB:, WIDE:], out[:NORB, WIDE:] + out[NORB:, :WIDE]

    def series(steps, e_real, e_imag):
        q_real, q_imag = eye + e_real, e_imag
        if steps == 1:
            return q_real, q_imag
        p_real, p_imag = combine(product3(left_rows(e_real, e_imag), right_blocks(e_real, e_imag)))
        for level in range(steps - 1):
            right = right_blocks(p_real, p_imag)
            t_real, t_imag = combine(product3(left_rows(q_real, q_imag), right))
            if level < steps - 2:
                p_real, p_imag = combine(product3(left_rows(p_real, p_imag), right))
            q_real, q_imag = q_real + t_real, q_imag + t_imag
        return q_real, q_imag

    def one_freq_sum(n, carry):
        freq_id = n // PER_FREQ * (PER_FREQ * LINE) + t * PER_FREQ + n % PER_FREQ
        count = n_ref[freq_id]

        def summed(steps):
            def body(p, total):
                t_real, t_imag = total
                q_real, q_imag = series(steps, er_ref[n, p], ei_ref[n, p])
                u_real, u_imag = column_scale(n, p)
                return (
                    t_real + (q_real * u_real - q_imag * u_imag),
                    t_imag + (q_real * u_imag + q_imag * u_real),
                )

            zero = jnp.zeros((NORB, WIDE), F32)
            t_real, t_imag = lax.fori_loop(0, PAIRS, body, (zero, zero), unroll=2)
            g = g_ref[n]
            turned = jnp.where(first, -swap(g), swap(g))
            right = jnp.concatenate([g, g, turned, turned], 0)
            r_high, r_low = halves(right)
            l_high, l_low = halves(jnp.concatenate([t_real, t_imag], 1))
            x_ref[n] = dot(l_high, r_high) + dot(l_low, r_high) + dot(l_high, r_low)

        for steps in (1, 2, 3):
            pl.when(count == steps)(functools.partial(summed, steps))
        return carry

    lax.fori_loop(0, N_LOCAL, one_freq_sum, 0)

    quarter = lanes % NORB // (NORB // YS)
    for n_high in range(2):
        for to_y in range(YS):
            mixed = None
            for n_low in range(4):
                value = x_ref[n_high * 4 + n_low]
                shift = (n_low - to_y) * (NORB // YS) % WIDE
                moved = pltpu.roll(value, shift, 1) if shift else value
                mixed = moved if mixed is None else jnp.where(quarter == n_low, moved, mixed)
            for to_x in range(XS):
                out_ref[to_x, to_y, n_high] = mixed[to_x * LINE : (to_x + 1) * LINE]


def invert(weights, counts, h_all, s_all, g_all):
    return pl.pallas_call(
        invert_kernel,
        name="invert",
        out_shape=jax.ShapeDtypeStruct((XS, YS, 2, LINE, WIDE), F32),
        in_specs=[smem(), smem(), vmem(), vmem(), vmem()],
        out_specs=vmem(),
        scratch_shapes=[
            pltpu.VMEM((PAIRS, WIDE, 2 * WIDE), BF),
            pltpu.VMEM((PAIRS, WIDE, 2 * WIDE), BF),
            pltpu.VMEM((PAIRS, NORB, WIDE), F32),
            pltpu.VMEM((PAIRS, 8, WIDE), F32),
            pltpu.VMEM((N_LOCAL, NORB, 2 * WIDE), BF),
            pltpu.VMEM((N_LOCAL, NORB, 2 * WIDE), F32),
            pltpu.VMEM((N_LOCAL, NORB, 2 * WIDE), F32),
            pltpu.VMEM((N_LOCAL, 8, 2 * WIDE), F32),
            pltpu.VMEM((N_LOCAL, PAIRS, NORB, WIDE), F32),
            pltpu.VMEM((N_LOCAL, PAIRS, NORB, WIDE), F32),
            pltpu.VMEM((N_LOCAL * NORB, 2 * WIDE), F32),
            pltpu.VMEM((N_LOCAL, NORB, WIDE), F32),
        ],
    )(weights, counts, h_all, s_all, g_all)


def exit_kernel(o_ref, q_ref, landed, rows_ref, as_, ar, bs, br):
    f = lax.axis_index("freq")
    y = lax.axis_index("kgrp")
    x, t = f // LINE, f % LINE
    z, c = t // CORES, t % CORES
    plane = [(dx, dy) for dx in range(XS) for dy in range(YS) if dx or dy]
    line = [(dz, dc) for dz in range(ZS) for dc in range(CORES) if dz or dc]

    def in_plane(dx, dy):
        return {"freq": (x + dx) % XS * LINE + t, "kgrp": (y + dy) % YS}

    def place(dz, dc):
        return (z + dz) % ZS * CORES + (c + dc) % CORES

    greet([in_plane(*d) for d in plane] + [on_freq(x * LINE + place(*d)) for d in line])
    started = []
    for dx, dy in plane:
        slot = dx * YS + dy
        copy = send(
            o_ref.at[(x + dx) % XS, (y + dy) % YS], landed.at[slot], as_.at[slot], ar.at[slot], in_plane(dx, dy)
        )
        copy.start()
        started.append(copy)
    total = o_ref[x, y]
    for dx, dy in plane:
        slot = dx * YS + dy
        send(o_ref.at[x, y], landed.at[slot], as_.at[slot], ar.at[slot], in_plane(dx, dy)).wait_recv()
        total = total + landed[slot]
    for to in range(LINE):
        for n_high in range(2):
            rows_ref[to, n_high : n_high + 1] = total[n_high, to : to + 1]
    for dz, dc in line:
        slot = dz * CORES + dc
        to = place(dz, dc)
        copy = send(rows_ref.at[to], q_ref.at[t], bs.at[slot], br.at[slot], on_freq(x * LINE + to))
        copy.start()
        started.append(copy)
    q_ref[pl.ds(t, 1)] = rows_ref[pl.ds(t, 1)]
    for dz, dc in line:
        slot = dz * CORES + dc
        source = (z + ZS - dz) % ZS * CORES + (c + CORES - dc) % CORES
        send(rows_ref.at[source], q_ref.at[source], bs.at[slot], br.at[slot], on_freq(x * LINE + place(dz, dc))).wait_recv()
    for copy in started:
        copy.wait_send()


def leave(sums):
    dma = pltpu.SemaphoreType.DMA
    return pl.pallas_call(
        exit_kernel,
        name="leave",
        out_shape=jax.ShapeDtypeStruct((LINE, 2, WIDE), F32),
        in_specs=[vmem()],
        out_specs=vmem(),
        scratch_shapes=[
            pltpu.VMEM((XS * YS, 2, LINE, WIDE), F32),
            pltpu.VMEM((LINE, 2, WIDE), F32),
            dma((XS * YS,)),
            dma((XS * YS,)),
            dma((LINE,)),
            dma((LINE,)),
        ],
        compiler_params=pltpu.CompilerParams(collective_id=1, has_side_effects=True),
    )(sums)


def per_device(hamiltonian, self_energy, guess_factor, weights, counts):
    h_all, s_all, g_all = gather(hamiltonian, self_energy, guess_factor)
    sums = invert(weights, counts, h_all, s_all, g_all)
    arrived = leave(sums)
    pieces = arrived.reshape(LINE, 2, 2, 2, 2, NORB // YS)
    return pieces.transpose(5, 2, 1, 3, 0, 4).reshape(NORB // YS, 2 * FREQ)


def solution(mesh):
    return jax.shard_map(
        per_device,
        mesh=mesh,
        in_specs=(
            P(("freq", "kgrp"), None, None),
            P("freq", None, None),
            P("freq", None, None),
            P(),
            P(),
        ),
        out_specs=P(("freq", "kgrp"), None),
        check_vma=False,
    )
```

```python
import functools
import math

import jax
import jax.numpy as jnp
from jax import lax
from jax.experimental import pallas as pl
from jax.experimental.pallas import tpu as pltpu
from jax.sharding import PartitionSpec as P

chem_potential = 0.2

NORB = 64
WIDE = 2 * NORB
XS, YS, ZS, CORES = 4, 4, 8, 2
LINE = ZS * CORES
PER_FREQ = 2
N_LOCAL = XS * PER_FREQ
PAIRS = LINE // 2
FREQ = 128
KPTS = 256
BF = jnp.bfloat16
F32 = jnp.float32


def vmem():
    return pl.BlockSpec(memory_space=pltpu.VMEM)


def smem():
    return pl.BlockSpec(memory_space=pltpu.SMEM)


def on_freq(index):
    return {"freq": index}


def greet(targets):
    barrier = pltpu.get_barrier_semaphore()
    for target in targets:
        pl.semaphore_signal(barrier, inc=1, device_id=target, device_id_type=pl.DeviceIdType.MESH)
    pl.semaphore_wait(barrier, len(targets))


def send(src, dst, send_sem, recv_sem, target):
    return pltpu.make_async_remote_copy(
        src_ref=src,
        dst_ref=dst,
        send_sem=send_sem,
        recv_sem=recv_sem,
        device_id=target,
        device_id_type=pl.DeviceIdType.MESH,
    )


Z_ORDER = (4, 3, 5, 2, 6, 1, 7)


def halves(value):
    high = value.astype(BF)
    low = (value - high.astype(F32)).astype(BF)
    return high, low


def dot(left, right):
    return jnp.dot(left, right, preferred_element_type=F32)


def product3(left, right):
    left_high, left_low = left
    right_high, right_low = right
    return dot(
        jnp.concatenate([left_high, left_low], 1), jnp.concatenate([right_high, right_high], 0)
    ) + dot(left_high, right_low)


def swap(value):
    return pltpu.roll(value, NORB, 1)


def lane_masks():
    rows = lax.broadcasted_iota(jnp.int32, (NORB, WIDE), 0)
    lanes = lax.broadcasted_iota(jnp.int32, (NORB, WIDE), 1)
    return lanes, lanes < NORB, rows == lanes % NORB


def gather_kernel(
    w_ref, h_ref, s_ref, g_ref,
    gall, er_ref, ei_ref, ur_ref, ui_ref, tr_ref, ti_ref,
    hall, sall, wh, wl, hcol, hrow, gcat, gz, zcol, zrow, gh_ref,
    zs, zr, ps, pr, ss, sr, gs, gr,
):
    f = lax.axis_index("freq")
    y = lax.axis_index("kgrp")
    x, t = f // LINE, f % LINE
    z, c = t // CORES, t % CORES
    partner = on_freq(x * LINE + z * CORES + (1 - c))
    _, first, eye_mask = lane_masks()
    eye = eye_mask.astype(F32)

    def along_z(dz):
        return on_freq(x * LINE + (z + dz) % ZS * CORES + c)

    def along_x(dx):
        return on_freq((x + dx) % XS * LINE + t)

    def paired(one, two):
        return jnp.where(first, one, swap(two)), jnp.where(first, swap(one), two)

    def as_right(real, imag):
        def build(r, i):
            return jnp.concatenate([jnp.concatenate([r, i], 1), jnp.concatenate([-i, r], 1)], 0)

        real_high, real_low = halves(real)
        imag_high, imag_low = halves(imag)
        return build(real_high, imag_high), build(real_low, imag_low)

    def diagonal_columns(value):
        kept = jnp.where(eye_mask, value, 0.0)
        left = jnp.sum(jnp.where(first, kept, 0.0), 1, keepdims=True)
        right = jnp.sum(jnp.where(first, 0.0, kept), 1, keepdims=True)
        return jnp.where(first, left, right)

    def diagonal_row(value):
        return jnp.sum(jnp.where(eye_mask, value, 0.0), 0, keepdims=True)

    def prepare_freqs(dx):
        owner = (x + XS - dx) % XS
        for b in range(PER_FREQ):
            n = dx * PER_FREQ + b
            matsubara = (2 * (owner * (PER_FREQ * LINE) + t * PER_FREQ + b) + 1).astype(F32) * (
                math.pi / (2 * FREQ)
            )
            shift = jnp.where(first, chem_potential, matsubara)
            zed = jnp.where(eye_mask, shift, 0.0) - sall[n]
            real, imag = paired(zed, zed)
            g_high, g_low = halves(gall[n])
            gz[n] = product3((g_high, g_low), as_right(real, imag))
            gcat[n] = jnp.concatenate([g_high, g_low], 1)
            zcol[n] = jnp.concatenate([diagonal_columns(real), diagonal_columns(imag)], 1)
            zrow[n : n + 1] = jnp.concatenate([diagonal_row(real), diagonal_row(imag)], 1)

    def prepare_pair(p):
        real, imag = paired(hall[p, 0], hall[p, 1])
        high, low = as_right(real, imag)
        wh[p] = high
        wl[p] = low
        hcol[p] = diagonal_columns(real)
        hrow[p : p + 1] = diagonal_row(real)

    def signal_all(targets):
        barrier = pltpu.get_barrier_semaphore()
        for target in targets:
            pl.semaphore_signal(barrier, inc=1, device_id=target, device_id_type=pl.DeviceIdType.MESH)
        return barrier

    greeted = [partner] + [along_z(dz) for dz in range(1, ZS)] + [along_x(dx) for dx in range(1, XS)]
    barrier = signal_all(greeted)
    hall[0, 0] = h_ref[0]
    sall[:PER_FREQ] = s_ref[...]
    gall[:PER_FREQ] = g_ref[...]
    prepare_freqs(0)

    def add_up(i, total):
        for j in range(16):
            total = total + w_ref[i * 16 + j]
        return total

    inv_total = 1.0 / lax.fori_loop(0, KPTS // 16, add_up, jnp.int32(0)).astype(F32)
    tr_ref[...] = jnp.zeros_like(tr_ref)
    ti_ref[...] = jnp.zeros_like(ti_ref)
    pl.semaphore_wait(barrier, len(greeted))

    started = []
    for dz in Z_ORDER:
        copy = send(h_ref.at[0], hall.at[dz, 0], zs.at[dz], zr.at[dz], along_z(dz))
        copy.start()
        started.append(copy)
    copy = send(h_ref.at[0], hall.at[0, 1], ps.at[0], pr.at[0], partner)
    copy.start()
    started.append(copy)

    def freq_copies(dx):
        rows = pl.ds(dx * PER_FREQ, PER_FREQ)
        return (
            send(g_ref, gall.at[rows], gs.at[dx], gr.at[dx], along_x(dx)),
            send(s_ref, sall.at[rows], ss.at[dx], sr.at[dx], along_x(dx)),
        )

    for dx in (2, 1, 3):
        for copy in freq_copies(dx):
            copy.start()
            started.append(copy)

    def arrived_z(dz):
        send(h_ref.at[0], hall.at[dz, 0], zs.at[dz], zr.at[dz], along_z(dz)).wait_recv()
        copy = send(hall.at[dz, 0], hall.at[dz, 1], ps.at[dz], pr.at[dz], partner)
        copy.start()
        started.append(copy)

    def arrived_x(dx):
        for copy in freq_copies(dx):
            copy.wait_recv()
        prepare_freqs(dx)

    def arrived_partner(dz):
        send(h_ref.at[0], hall.at[dz, 1], ps.at[dz], pr.at[dz], partner).wait_recv()
        prepare_pair(dz)

    for dz in (1, 7, 2, 6):
        arrived_z(dz)
    arrived_partner(0)
    arrived_x(1)
    for dz in (3, 5):
        arrived_z(dz)
    arrived_x(3)
    arrived_z(4)
    arrived_x(2)
    for dz in (1, 7, 2, 6, 3, 5, 4):
        arrived_partner(dz)

    def residual_pair(p, carry):
        left = gcat[...].reshape(N_LOCAL * NORB, 2 * WIDE)
        high = wh[p]
        gh_ref[...] = dot(left, jnp.concatenate([high, high], 0)) + dot(left[:, :WIDE], wl[p])
        h_diag = hcol[p]
        chip = x * LINE + (z + ZS - p) % ZS * CORES
        w_one = w_ref[(chip + c) * YS + y].astype(F32) * inv_total
        w_two = w_ref[(chip + 1 - c) * YS + y].astype(F32) * inv_total
        weight = jnp.where(first[:N_LOCAL], w_one, w_two)
        d_real, d_imag = zrow[:, :WIDE] - hrow[pl.ds(p, 1)], zrow[:, WIDE:]
        inv = weight / (d_real * d_real + d_imag * d_imag)
        ur_ref[p] = d_real * inv
        ui_ref[p] = -d_imag * inv
        for n in range(N_LOCAL):
            a = gz[n] - gh_ref[n * NORB : (n + 1) * NORB]
            a_real, a_imag = a[:, :WIDE], a[:, WIDE:]
            d = zcol[n]
            d_real, d_imag = d[:, :WIDE] - h_diag, d[:, WIDE:]
            inv = 1.0 / (d_real * d_real + d_imag * d_imag)
            v_real, v_imag = d_real * inv, d_imag * inv
            e_real = eye - (v_real * a_real + v_imag * a_imag)
            e_imag = v_imag * a_real - v_real * a_imag
            er_ref[n, p] = e_real
            ei_ref[n, p] = e_imag
            u_real, u_imag = ur_ref[p, n : n + 1], ui_ref[p, n : n + 1]
            q_real = eye + e_real
            tr_ref[n] += q_real * u_real - e_imag * u_imag
            ti_ref[n] += q_real * u_imag + e_imag * u_real
        return carry

    lax.fori_loop(0, PAIRS, residual_pair, 0)
    for copy in started:
        copy.wait_send()


def gather(weights, hamiltonian, self_energy, guess_factor):
    dma = pltpu.SemaphoreType.DMA
    powers = jax.ShapeDtypeStruct((N_LOCAL, PAIRS, NORB, WIDE), F32)
    scales = jax.ShapeDtypeStruct((PAIRS, N_LOCAL, WIDE), F32)
    totals = jax.ShapeDtypeStruct((N_LOCAL, NORB, WIDE), F32)
    return pl.pallas_call(
        gather_kernel,
        name="gather",
        out_shape=(totals, powers, powers, scales, scales, totals, totals),
        in_specs=[smem()] + [vmem()] * 3,
        out_specs=(vmem(),) * 7,
        scratch_shapes=[
            pltpu.VMEM((ZS, CORES, NORB, WIDE), F32),
            pltpu.VMEM((N_LOCAL, NORB, WIDE), F32),
            pltpu.VMEM((PAIRS, WIDE, 2 * WIDE), BF),
            pltpu.VMEM((PAIRS, WIDE, 2 * WIDE), BF),
            pltpu.VMEM((PAIRS, NORB, WIDE), F32),
            pltpu.VMEM((PAIRS, WIDE), F32),
            pltpu.VMEM((N_LOCAL, NORB, 2 * WIDE), BF),
            pltpu.VMEM((N_LOCAL, NORB, 2 * WIDE), F32),
            pltpu.VMEM((N_LOCAL, NORB, 2 * WIDE), F32),
            pltpu.VMEM((N_LOCAL, 2 * WIDE), F32),
            pltpu.VMEM((N_LOCAL * NORB, 2 * WIDE), F32),
        ]
        + [dma((ZS,))] * 4
        + [dma((XS,))] * 4,
        compiler_params=pltpu.CompilerParams(
            collective_id=0, has_side_effects=True, vmem_limit_bytes=20 << 20
        ),
    )(weights, hamiltonian, self_energy, guess_factor)


def power_kernel(n_ref, g_ref, er_ref, ei_ref, ur_ref, ui_ref, t1r_ref, t1i_ref, out_ref, sr_ref, si_ref, qr_ref, qi_ref, tr_ref, ti_ref):
    f = lax.axis_index("freq")
    x, t = f // LINE, f % LINE
    lanes, first, eye_mask = lane_masks()
    eye = eye_mask.astype(F32)
    first_bf = first.astype(F32).astype(BF)
    second_bf = (1.0 - first.astype(F32)).astype(BF)

    def right_blocks(real, imag):
        def build(r, i):
            return jnp.concatenate(
                [
                    jnp.concatenate([r * first_bf, i * first_bf], 1),
                    jnp.concatenate([r * second_bf, i * second_bf], 1),
                ],
                0,
            )

        r_high, r_low = halves(real)
        i_high, i_low = halves(imag)
        return build(r_high, i_high), build(r_low, i_low)

    def left_rows(real, imag):
        return halves(jnp.concatenate([real, imag], 0))

    def combine(out):
        return out[:NORB, :WIDE] - out[NORB:, WIDE:], out[:NORB, WIDE:] + out[NORB:, :WIDE]

    def weighted(n, p, real, imag):
        u_real, u_imag = ur_ref[p, pl.ds(n, 1)], ui_ref[p, pl.ds(n, 1)]
        return real * u_real - imag * u_imag, real * u_imag + imag * u_real

    def two_steps(n):
        for p in range(PAIRS):
            e_real, e_imag = er_ref[n, p], ei_ref[n, p]
            sr_ref[p], si_ref[p] = combine(product3(left_rows(e_real, e_imag), right_blocks(e_real, e_imag)))
        total = t1r_ref[n], t1i_ref[n]
        for p in range(PAIRS):
            left = left_rows(eye + er_ref[n, p], ei_ref[n, p])
            real, imag = combine(product3(left, right_blocks(sr_ref[p], si_ref[p])))
            real, imag = weighted(n, p, real, imag)
            total = total[0] + real, total[1] + imag
        tr_ref[n], ti_ref[n] = total

    def three_steps(n):
        for p in range(PAIRS):
            e_real, e_imag = er_ref[n, p], ei_ref[n, p]
            sr_ref[p], si_ref[p] = combine(product3(left_rows(e_real, e_imag), right_blocks(e_real, e_imag)))
        for p in range(PAIRS):
            e_real, e_imag = er_ref[n, p], ei_ref[n, p]
            s_real, s_imag = sr_ref[p], si_ref[p]
            right = right_blocks(s_real, s_imag)
            real, imag = combine(product3(left_rows(eye + e_real, e_imag), right))
            qr_ref[p], qi_ref[p] = eye + e_real + real, e_imag + imag
            sr_ref[p], si_ref[p] = combine(product3(left_rows(s_real, s_imag), right))
        total = None
        for p in range(PAIRS):
            q_real, q_imag = qr_ref[p], qi_ref[p]
            real, imag = combine(product3(left_rows(q_real, q_imag), right_blocks(sr_ref[p], si_ref[p])))
            real, imag = weighted(n, p, q_real + real, q_imag + imag)
            total = (real, imag) if total is None else (total[0] + real, total[1] + imag)
        tr_ref[n], ti_ref[n] = total

    tr_ref[...] = t1r_ref[...]
    ti_ref[...] = t1i_ref[...]

    def one_freq(n, carry):
        owner = (x + XS - n // PER_FREQ) % XS
        count = n_ref[owner * (PER_FREQ * LINE) + t * PER_FREQ + n % PER_FREQ]
        pl.when(count == 2)(functools.partial(two_steps, n))
        pl.when(count == 3)(functools.partial(three_steps, n))
        return carry

    lax.fori_loop(0, N_LOCAL, one_freq, 0)

    quarter = lanes % NORB // (NORB // YS)
    for n_high in range(2):
        mixed = [None] * YS
        for n_low in range(4):
            n = (x + XS - n_high * 2 - n_low // 2) % XS * PER_FREQ + n_low % 2
            g = g_ref[n]
            turned = jnp.where(first, -swap(g), swap(g))
            r_high, r_low = halves(jnp.concatenate([g, g, turned, turned], 0))
            l_high, l_low = halves(jnp.concatenate([tr_ref[n], ti_ref[n]], 1))
            both = dot(l_high, jnp.concatenate([r_high, r_low], 1))
            value = both[:, :WIDE] + both[:, WIDE:] + dot(l_low, r_high)
            for to_y in range(YS):
                shift = (n_low - to_y) * (NORB // YS) % WIDE
                moved = pltpu.roll(value, shift, 1) if shift else value
                mixed[to_y] = moved if n_low == 0 else jnp.where(quarter == n_low, moved, mixed[to_y])
        for to_y in range(YS):
            for to_x in range(XS):
                out_ref[to_x, to_y, n_high] = mixed[to_y][to_x * LINE : (to_x + 1) * LINE]


def invert(counts, *gathered):
    slots = pltpu.VMEM((PAIRS, NORB, WIDE), F32)
    totals = pltpu.VMEM((N_LOCAL, NORB, WIDE), F32)
    return pl.pallas_call(
        power_kernel,
        name="invert",
        out_shape=jax.ShapeDtypeStruct((XS, YS, 2, LINE, WIDE), F32),
        in_specs=[smem()] + [vmem()] * 7,
        out_specs=vmem(),
        scratch_shapes=[slots] * 4 + [totals] * 2,
        compiler_params=pltpu.CompilerParams(vmem_limit_bytes=16 << 20),
    )(counts, *gathered)


def exit_kernel(o_ref, q_ref, landed, rows_ref, as_, ar, bs, br):
    f = lax.axis_index("freq")
    y = lax.axis_index("kgrp")
    x, t = f // LINE, f % LINE
    z, c = t // CORES, t % CORES
    plane = [(dx, dy) for dx in range(XS) for dy in range(YS) if dx or dy]
    line = [(dz, dc) for dz in range(ZS) for dc in range(CORES) if dz or dc]

    def in_plane(dx, dy):
        return {"freq": (x + dx) % XS * LINE + t, "kgrp": (y + dy) % YS}

    def place(dz, dc):
        return (z + dz) % ZS * CORES + (c + dc) % CORES

    greet([in_plane(*d) for d in plane] + [on_freq(x * LINE + place(*d)) for d in line])
    started = []
    for dx, dy in plane:
        slot = dx * YS + dy
        copy = send(
            o_ref.at[(x + dx) % XS, (y + dy) % YS], landed.at[slot], as_.at[slot], ar.at[slot], in_plane(dx, dy)
        )
        copy.start()
        started.append(copy)
    total = o_ref[x, y]
    for dx, dy in plane:
        slot = dx * YS + dy
        send(o_ref.at[x, y], landed.at[slot], as_.at[slot], ar.at[slot], in_plane(dx, dy)).wait_recv()
        total = total + landed[slot]
    for to in range(LINE):
        for n_high in range(2):
            rows_ref[to, n_high : n_high + 1] = total[n_high, to : to + 1]
    for dz, dc in line:
        slot = dz * CORES + dc
        to = place(dz, dc)
        copy = send(rows_ref.at[to], q_ref.at[t], bs.at[slot], br.at[slot], on_freq(x * LINE + to))
        copy.start()
        started.append(copy)
    q_ref[pl.ds(t, 1)] = rows_ref[pl.ds(t, 1)]
    for dz, dc in line:
        slot = dz * CORES + dc
        source = (z + ZS - dz) % ZS * CORES + (c + CORES - dc) % CORES
        send(rows_ref.at[source], q_ref.at[source], bs.at[slot], br.at[slot], on_freq(x * LINE + place(dz, dc))).wait_recv()
    for copy in started:
        copy.wait_send()


def leave(sums):
    dma = pltpu.SemaphoreType.DMA
    return pl.pallas_call(
        exit_kernel,
        name="leave",
        out_shape=jax.ShapeDtypeStruct((LINE, 2, WIDE), F32),
        in_specs=[vmem()],
        out_specs=vmem(),
        scratch_shapes=[
            pltpu.VMEM((XS * YS, 2, LINE, WIDE), F32),
            pltpu.VMEM((LINE, 2, WIDE), F32),
            dma((XS * YS,)),
            dma((XS * YS,)),
            dma((LINE,)),
            dma((LINE,)),
        ],
        compiler_params=pltpu.CompilerParams(
            collective_id=1, has_side_effects=True, vmem_limit_bytes=8 << 20
        ),
    )(sums)


def per_device(hamiltonian, self_energy, guess_factor, weights, counts):
    gathered = gather(weights, hamiltonian, self_energy, guess_factor)
    sums = invert(counts, *gathered)
    arrived = leave(sums)
    pieces = arrived.reshape(LINE, 2, 2, 2, 2, NORB // YS)
    return pieces.transpose(5, 2, 1, 3, 0, 4).reshape(NORB // YS, 2 * FREQ)


def solution(mesh):
    return jax.shard_map(
        per_device,
        mesh=mesh,
        in_specs=(
            P(("freq", "kgrp"), None, None),
            P("freq", None, None),
            P("freq", None, None),
            P(),
            P(),
        ),
        out_specs=P(("freq", "kgrp"), None),
        check_vma=False,
    )
```

```python
import functools
import math

import jax
import jax.numpy as jnp
from jax import lax
from jax.experimental import pallas as pl
from jax.experimental.pallas import tpu as pltpu
from jax.sharding import PartitionSpec as P

chem_potential = 0.2

NORB = 64
WIDE = 2 * NORB
XS, YS, ZS, CORES = 4, 4, 8, 2
LINE = ZS * CORES
PER_FREQ = 2
N_LOCAL = XS * PER_FREQ
PAIRS = LINE // 2
FREQ = 128
KPTS = 256
BF = jnp.bfloat16
F32 = jnp.float32


def vmem():
    return pl.BlockSpec(memory_space=pltpu.VMEM)


def smem():
    return pl.BlockSpec(memory_space=pltpu.SMEM)


def hbm():
    return pl.BlockSpec(memory_space=pltpu.HBM)


def on_freq(index):
    return {"freq": index}


def greet(targets):
    barrier = pltpu.get_barrier_semaphore()
    for target in targets:
        pl.semaphore_signal(barrier, inc=1, device_id=target, device_id_type=pl.DeviceIdType.MESH)
    return lambda: pl.semaphore_wait(barrier, len(targets))


def send(src, dst, send_sem, recv_sem, target):
    return pltpu.make_async_remote_copy(
        src_ref=src,
        dst_ref=dst,
        send_sem=send_sem,
        recv_sem=recv_sem,
        device_id=target,
        device_id_type=pl.DeviceIdType.MESH,
    )


Z_ORDER = (4, 3, 5, 2, 6, 1, 7)
SLOT_DX = (0, 1, 3, 2)


def halves(value):
    high = value.astype(BF)
    low = (value - high.astype(F32)).astype(BF)
    return high, low


def dot(left, right):
    return jnp.dot(left, right, preferred_element_type=F32)


def product3(left, right):
    left_high, left_low = left
    right_high, right_low = right
    return dot(
        jnp.concatenate([left_high, left_low], 1), jnp.concatenate([right_high, right_high], 0)
    ) + dot(left_high, right_low)


def swap(value):
    return pltpu.roll(value, NORB, 1)


def lane_masks():
    rows = lax.broadcasted_iota(jnp.int32, (NORB, WIDE), 0)
    lanes = lax.broadcasted_iota(jnp.int32, (NORB, WIDE), 1)
    return lanes, lanes < NORB, rows == lanes % NORB


def gather_kernel(
    w_hbm, n_hbm, h_hbm, s_hbm, g_hbm,
    gall, er_ref, ei_ref, ur_ref, ui_ref, tr_ref, ti_ref, count_ref,
    w_ref, n_ref, hall, sall, wh, wl, hcol, hrow, gcat, gz, zcol, zrow, gh_ref,
    zs, zr, ps, pr, ss, sr, gs, gr, own,
):
    f = lax.axis_index("freq")
    y = lax.axis_index("kgrp")
    x, t = f // LINE, f % LINE
    z, c = t // CORES, t % CORES
    partner = on_freq(x * LINE + z * CORES + (1 - c))
    _, first, eye_mask = lane_masks()
    eye = eye_mask.astype(F32)

    def along_z(dz):
        return on_freq(x * LINE + (z + dz) % ZS * CORES + c)

    def along_x(dx):
        return on_freq((x + dx) % XS * LINE + t)

    def paired(one, two):
        return jnp.where(first, one, swap(two)), jnp.where(first, swap(one), two)

    def as_right(real, imag):
        def build(r, i):
            return jnp.concatenate([jnp.concatenate([r, i], 1), jnp.concatenate([-i, r], 1)], 0)

        real_high, real_low = halves(real)
        imag_high, imag_low = halves(imag)
        return build(real_high, imag_high), build(real_low, imag_low)

    def diagonal_columns(value):
        kept = jnp.where(eye_mask, value, 0.0)
        left = jnp.sum(jnp.where(first, kept, 0.0), 1, keepdims=True)
        right = jnp.sum(jnp.where(first, 0.0, kept), 1, keepdims=True)
        return jnp.where(first, left, right)

    def diagonal_row(value):
        return jnp.sum(jnp.where(eye_mask, value, 0.0), 0, keepdims=True)

    def prepare_freqs(slot):
        owner = (x + XS - SLOT_DX[slot]) % XS
        for b in range(PER_FREQ):
            n = slot * PER_FREQ + b
            freq_id = owner * (PER_FREQ * LINE) + t * PER_FREQ + b
            count_ref[n : n + 1] = jnp.full((1, WIDE), n_ref[freq_id].astype(F32))
            matsubara = (2 * freq_id + 1).astype(F32) * (math.pi / (2 * FREQ))
            shift = jnp.where(first, chem_potential, matsubara)
            zed = jnp.where(eye_mask, shift, 0.0) - sall[n]
            real, imag = paired(zed, zed)
            g_high, g_low = halves(gall[n])
            gz[n] = product3((g_high, g_low), as_right(real, imag))
            gcat[n] = jnp.concatenate([g_high, g_low], 1)
            zcol[n] = jnp.concatenate([diagonal_columns(real), diagonal_columns(imag)], 1)
            zrow[n : n + 1] = jnp.concatenate([diagonal_row(real), diagonal_row(imag)], 1)

    def prepare_pair(p):
        real, imag = paired(hall[p, 0], hall[p, 1])
        high, low = as_right(real, imag)
        wh[p] = high
        wl[p] = low
        hcol[p] = diagonal_columns(real)
        hrow[p : p + 1] = diagonal_row(real)

    first_rows = pl.ds(0, PER_FREQ)
    own_h, own_s, own_g = hall.at[0, 0], sall.at[first_rows], gall.at[first_rows]
    loads = [
        pltpu.make_async_copy(src, dst, own.at[i])
        for i, (src, dst) in enumerate(
            ((h_hbm.at[0], own_h), (g_hbm, own_g), (s_hbm, own_s), (w_hbm, w_ref), (n_hbm, n_ref))
        )
    ]
    for load in loads:
        load.start()
    await_greetings = greet(
        [partner] + [along_z(dz) for dz in range(1, ZS)] + [along_x(dx) for dx in range(1, XS)]
    )
    tr_ref[...] = jnp.zeros_like(tr_ref)
    ti_ref[...] = jnp.zeros_like(ti_ref)
    for load in loads:
        load.wait()
    prepare_freqs(0)

    def add_up(i, total):
        for j in range(16):
            total = total + w_ref[i * 16 + j]
        return total

    inv_total = 1.0 / lax.fori_loop(0, KPTS // 16, add_up, jnp.int32(0)).astype(F32)
    await_greetings()

    def z_copy(dz):
        return send(own_h, hall.at[dz, 0], zs.at[dz], zr.at[dz], along_z(dz))

    def partner_copy(dz):
        return send(hall.at[dz, 0], hall.at[dz, 1], ps.at[dz], pr.at[dz], partner)

    def freq_copies(slot):
        rows = pl.ds(slot * PER_FREQ, PER_FREQ)
        target = along_x(SLOT_DX[slot])
        return (
            send(own_g, gall.at[rows], gs.at[slot], gr.at[slot], target),
            send(own_s, sall.at[rows], ss.at[slot], sr.at[slot], target),
        )

    started = []

    def begin(copy):
        copy.start()
        started.append(copy)

    begin(partner_copy(0))
    for dz in Z_ORDER:
        begin(z_copy(dz))
    for slot in (3, 1, 2):
        for copy in freq_copies(slot):
            begin(copy)

    def residuals(p, low, high):
        left = gcat[low:high].reshape((high - low) * NORB, 2 * WIDE)
        right = wh[p]
        gh_ref[: (high - low) * NORB] = dot(left, jnp.concatenate([right, right], 0)) + dot(
            left[:, :WIDE], wl[p]
        )
        h_diag = hcol[p]
        chip = x * LINE + (z + ZS - p) % ZS * CORES
        w_one = w_ref[(chip + c) * YS + y].astype(F32) * inv_total
        w_two = w_ref[(chip + 1 - c) * YS + y].astype(F32) * inv_total
        weight = jnp.where(first[: high - low], w_one, w_two)
        d_real, d_imag = zrow[low:high, :WIDE] - hrow[pl.ds(p, 1)], zrow[low:high, WIDE:]
        inv = weight / (d_real * d_real + d_imag * d_imag)
        ur_ref[p, low:high] = d_real * inv
        ui_ref[p, low:high] = -d_imag * inv
        for n in range(low, high):
            a = gz[n] - gh_ref[(n - low) * NORB : (n - low + 1) * NORB]
            a_real, a_imag = a[:, :WIDE], a[:, WIDE:]
            d = zcol[n]
            d_real, d_imag = d[:, :WIDE] - h_diag, d[:, WIDE:]
            inv = 1.0 / (d_real * d_real + d_imag * d_imag)
            v_real, v_imag = d_real * inv, d_imag * inv
            e_real = eye - (v_real * a_real + v_imag * a_imag)
            e_imag = v_imag * a_real - v_real * a_imag
            er_ref[n, p] = e_real
            ei_ref[n, p] = e_imag
            u_real, u_imag = ur_ref[p, n : n + 1], ui_ref[p, n : n + 1]
            q_real = eye + e_real
            tr_ref[n] += q_real * u_real - e_imag * u_imag
            ti_ref[n] += q_real * u_imag + e_imag * u_real

    def residuals_of_all(low, high):
        def body(p, carry):
            residuals(p, low, high)
            return carry

        lax.fori_loop(0, PAIRS, body, 0, unroll=2)

    def arrived_z(*steps):
        for dz in steps:
            z_copy(dz).wait_recv()
            begin(partner_copy(dz))

    def arrived_x(*slots):
        for slot in slots:
            for copy in freq_copies(slot):
                copy.wait_recv()
        for slot in slots:
            prepare_freqs(slot)

    def arrived_pair(*steps):
        for dz in steps:
            partner_copy(dz).wait_recv()
        for dz in steps:
            prepare_pair(dz)
        for dz in steps:
            residuals(dz, 0, PER_FREQ)

    arrived_pair(0)
    arrived_z(1, 7, 2, 6)
    arrived_pair(1, 7)
    arrived_z(3, 5)
    arrived_pair(2, 6)
    arrived_z(4)
    arrived_x(1, 2)
    arrived_pair(3, 5)
    arrived_pair(4)
    residuals_of_all(PER_FREQ, 3 * PER_FREQ)
    arrived_x(3)
    residuals_of_all(3 * PER_FREQ, N_LOCAL)
    for copy in started:
        copy.wait_send()


def gather(*values):
    dma = pltpu.SemaphoreType.DMA
    powers = jax.ShapeDtypeStruct((N_LOCAL, PAIRS, NORB, WIDE), F32)
    scales = jax.ShapeDtypeStruct((PAIRS, N_LOCAL, WIDE), F32)
    totals = jax.ShapeDtypeStruct((N_LOCAL, NORB, WIDE), F32)
    counted = jax.ShapeDtypeStruct((N_LOCAL, WIDE), F32)
    return pl.pallas_call(
        gather_kernel,
        name="gather",
        out_shape=(totals, powers, powers, scales, scales, totals, totals, counted),
        in_specs=[hbm()] * 5,
        out_specs=(vmem(),) * 8,
        scratch_shapes=[
            pltpu.SMEM((KPTS,), jnp.int32),
            pltpu.SMEM((FREQ,), jnp.int32),
            pltpu.VMEM((ZS, CORES, NORB, WIDE), F32),
            pltpu.VMEM((N_LOCAL, NORB, WIDE), F32),
            pltpu.VMEM((PAIRS, WIDE, 2 * WIDE), BF),
            pltpu.VMEM((PAIRS, WIDE, 2 * WIDE), BF),
            pltpu.VMEM((PAIRS, NORB, WIDE), F32),
            pltpu.VMEM((PAIRS, WIDE), F32),
            pltpu.VMEM((N_LOCAL, NORB, 2 * WIDE), BF),
            pltpu.VMEM((N_LOCAL, NORB, 2 * WIDE), F32),
            pltpu.VMEM((N_LOCAL, NORB, 2 * WIDE), F32),
            pltpu.VMEM((N_LOCAL, 2 * WIDE), F32),
            pltpu.VMEM((N_LOCAL * NORB, 2 * WIDE), F32),
        ]
        + [dma((ZS,))] * 4
        + [dma((XS,))] * 4
        + [dma((5,))],
        compiler_params=pltpu.CompilerParams(
            collective_id=0, has_side_effects=True, vmem_limit_bytes=20 << 20
        ),
    )(*(pltpu.with_memory_space_constraint(value, pltpu.HBM) for value in values))


def power_kernel(
    er_ref, ei_ref, ur_ref, ui_ref, t1r_ref, t1i_ref, count_ref, tr_ref, ti_ref, sr_ref, si_ref, qr_ref, qi_ref, steps_ref
):
    _, first, eye_mask = lane_masks()
    eye = eye_mask.astype(F32)
    first_bf = first.astype(F32).astype(BF)
    second_bf = (1.0 - first.astype(F32)).astype(BF)

    def right_blocks(real, imag):
        def build(r, i):
            return jnp.concatenate(
                [
                    jnp.concatenate([r * first_bf, i * first_bf], 1),
                    jnp.concatenate([r * second_bf, i * second_bf], 1),
                ],
                0,
            )

        r_high, r_low = halves(real)
        i_high, i_low = halves(imag)
        return build(r_high, i_high), build(r_low, i_low)

    def left_rows(real, imag):
        return halves(jnp.concatenate([real, imag], 0))

    def combine(out):
        return out[:NORB, :WIDE] - out[NORB:, WIDE:], out[:NORB, WIDE:] + out[NORB:, :WIDE]

    def weighted(n, p, real, imag):
        u_real, u_imag = ur_ref[p, pl.ds(n, 1)], ui_ref[p, pl.ds(n, 1)]
        return real * u_real - imag * u_imag, real * u_imag + imag * u_real

    def two_steps(n):
        for p in range(PAIRS):
            e_real, e_imag = er_ref[n, p], ei_ref[n, p]
            sr_ref[p], si_ref[p] = combine(product3(left_rows(e_real, e_imag), right_blocks(e_real, e_imag)))
        total = t1r_ref[n], t1i_ref[n]
        for p in range(PAIRS):
            left = left_rows(eye + er_ref[n, p], ei_ref[n, p])
            real, imag = combine(product3(left, right_blocks(sr_ref[p], si_ref[p])))
            real, imag = weighted(n, p, real, imag)
            total = total[0] + real, total[1] + imag
        tr_ref[n], ti_ref[n] = total

    def three_steps(n):
        for p in range(PAIRS):
            e_real, e_imag = er_ref[n, p], ei_ref[n, p]
            sr_ref[p], si_ref[p] = combine(product3(left_rows(e_real, e_imag), right_blocks(e_real, e_imag)))
        for p in range(PAIRS):
            e_real, e_imag = er_ref[n, p], ei_ref[n, p]
            s_real, s_imag = sr_ref[p], si_ref[p]
            right = right_blocks(s_real, s_imag)
            real, imag = combine(product3(left_rows(eye + e_real, e_imag), right))
            qr_ref[p], qi_ref[p] = eye + e_real + real, e_imag + imag
            sr_ref[p], si_ref[p] = combine(product3(left_rows(s_real, s_imag), right))
        total = None
        for p in range(PAIRS):
            q_real, q_imag = qr_ref[p], qi_ref[p]
            real, imag = combine(product3(left_rows(q_real, q_imag), right_blocks(sr_ref[p], si_ref[p])))
            real, imag = weighted(n, p, q_real + real, q_imag + imag)
            total = (real, imag) if total is None else (total[0] + real, total[1] + imag)
        tr_ref[n], ti_ref[n] = total

    for n in range(N_LOCAL):
        steps_ref[n] = jnp.max(count_ref[n : n + 1])
    tr_ref[...] = t1r_ref[...]
    ti_ref[...] = t1i_ref[...]

    def one_freq(n, carry):
        steps = steps_ref[n]
        pl.when((steps > 1.5) & (steps < 2.5))(functools.partial(two_steps, n))
        pl.when(steps > 2.5)(functools.partial(three_steps, n))
        return carry

    lax.fori_loop(0, N_LOCAL, one_freq, 0)


def invert(*gathered):
    slots = pltpu.VMEM((PAIRS, NORB, WIDE), F32)
    totals = jax.ShapeDtypeStruct((N_LOCAL, NORB, WIDE), F32)
    return pl.pallas_call(
        power_kernel,
        name="invert",
        out_shape=(totals, totals),
        in_specs=[vmem()] * 7,
        out_specs=(vmem(),) * 2,
        scratch_shapes=[slots] * 4 + [pltpu.SMEM((N_LOCAL,), F32)],
        compiler_params=pltpu.CompilerParams(vmem_limit_bytes=16 << 20),
    )(*gathered)


def exit_kernel(g_ref, tr_ref, ti_ref, q_ref, o_ref, landed, rows_ref, as_, ar, bs, br):
    f = lax.axis_index("freq")
    y = lax.axis_index("kgrp")
    x, t = f // LINE, f % LINE
    z, c = t // CORES, t % CORES
    plane = [(dx, dy) for dx in range(XS) for dy in range(YS) if dx or dy]
    line = [(dz, dc) for dz in range(ZS) for dc in range(CORES) if dz or dc]

    def in_plane(dx, dy):
        return {"freq": (x + dx) % XS * LINE + t, "kgrp": (y + dy) % YS}

    def place(dz, dc):
        return (z + dz) % ZS * CORES + (c + dc) % CORES

    await_greetings = greet([in_plane(*d) for d in plane] + [on_freq(x * LINE + place(*d)) for d in line])
    lanes, first, _ = lane_masks()
    quarter = lanes % NORB // (NORB // YS)
    for n_high in range(2):
        mixed = [None] * YS
        for n_low in range(4):
            dx = (x + XS - n_high * 2 - n_low // 2) % XS
            n = (dx + dx // 2 * (5 - 2 * dx)) * PER_FREQ + n_low % 2
            g = g_ref[n]
            turned = jnp.where(first, -swap(g), swap(g))
            r_high, r_low = halves(jnp.concatenate([g, g, turned, turned], 0))
            l_high, l_low = halves(jnp.concatenate([tr_ref[n], ti_ref[n]], 1))
            both = dot(l_high, jnp.concatenate([r_high, r_low], 1))
            value = both[:, :WIDE] + both[:, WIDE:] + dot(l_low, r_high)
            for to_y in range(YS):
                shift = (n_low - to_y) * (NORB // YS) % WIDE
                moved = pltpu.roll(value, shift, 1) if shift else value
                mixed[to_y] = moved if n_low == 0 else jnp.where(quarter == n_low, moved, mixed[to_y])
        for to_y in range(YS):
            for to_x in range(XS):
                o_ref[to_x, to_y, n_high] = mixed[to_y][to_x * LINE : (to_x + 1) * LINE]
    await_greetings()
    started = []
    for dx, dy in plane:
        slot = dx * YS + dy
        copy = send(
            o_ref.at[(x + dx) % XS, (y + dy) % YS], landed.at[slot], as_.at[slot], ar.at[slot], in_plane(dx, dy)
        )
        copy.start()
        started.append(copy)
    total = o_ref[x, y]
    for dx, dy in plane:
        slot = dx * YS + dy
        send(o_ref.at[x, y], landed.at[slot], as_.at[slot], ar.at[slot], in_plane(dx, dy)).wait_recv()
        total = total + landed[slot]
    for to in range(LINE):
        for n_high in range(2):
            rows_ref[to, n_high : n_high + 1] = total[n_high, to : to + 1]
    for dz, dc in line:
        slot = dz * CORES + dc
        to = place(dz, dc)
        copy = send(rows_ref.at[to], q_ref.at[t], bs.at[slot], br.at[slot], on_freq(x * LINE + to))
        copy.start()
        started.append(copy)
    q_ref[pl.ds(t, 1)] = rows_ref[pl.ds(t, 1)]
    for dz, dc in line:
        slot = dz * CORES + dc
        source = (z + ZS - dz) % ZS * CORES + (c + CORES - dc) % CORES
        send(rows_ref.at[source], q_ref.at[source], bs.at[slot], br.at[slot], on_freq(x * LINE + place(dz, dc))).wait_recv()
    for copy in started:
        copy.wait_send()


def leave(*parts):
    dma = pltpu.SemaphoreType.DMA
    return pl.pallas_call(
        exit_kernel,
        name="leave",
        out_shape=jax.ShapeDtypeStruct((LINE, 2, WIDE), F32),
        in_specs=[vmem()] * 3,
        out_specs=vmem(),
        scratch_shapes=[
            pltpu.VMEM((XS, YS, 2, LINE, WIDE), F32),
            pltpu.VMEM((XS * YS, 2, LINE, WIDE), F32),
            pltpu.VMEM((LINE, 2, WIDE), F32),
            dma((XS * YS,)),
            dma((XS * YS,)),
            dma((LINE,)),
            dma((LINE,)),
        ],
        compiler_params=pltpu.CompilerParams(
            collective_id=1, has_side_effects=True, vmem_limit_bytes=8 << 20
        ),
    )(*parts)


def per_device(hamiltonian, self_energy, guess_factor, weights, counts):
    g_all, *gathered = gather(weights, counts, hamiltonian, self_energy, guess_factor)
    arrived = leave(g_all, *invert(*gathered))
    pieces = arrived.reshape(LINE, 2, 2, 2, 2, NORB // YS)
    return pieces.transpose(5, 2, 1, 3, 0, 4).reshape(NORB // YS, 2 * FREQ)


def solution(mesh):
    return jax.shard_map(
        per_device,
        mesh=mesh,
        in_specs=(
            P(("freq", "kgrp"), None, None),
            P("freq", None, None),
            P("freq", None, None),
            P(),
            P(),
        ),
        out_specs=P(("freq", "kgrp"), None),
        check_vma=False,
    )
```

```python
import functools
import math

import jax
import jax.numpy as jnp
from jax import lax
from jax.experimental import pallas as pl
from jax.experimental.pallas import tpu as pltpu
from jax.sharding import PartitionSpec as P

chem_potential = 0.2

NORB = 64
WIDE = 2 * NORB
XS, YS, ZS, CORES = 4, 4, 8, 2
LINE = ZS * CORES
PER_FREQ = 2
N_LOCAL = XS * PER_FREQ
PAIRS = LINE // 2
FREQ = 128
KPTS = 256
BF = jnp.bfloat16
F32 = jnp.float32


def vmem():
    return pl.BlockSpec(memory_space=pltpu.VMEM)


def smem():
    return pl.BlockSpec(memory_space=pltpu.SMEM)


def hbm():
    return pl.BlockSpec(memory_space=pltpu.HBM)


def on_freq(index):
    return {"freq": index}


def greet(targets):
    barrier = pltpu.get_barrier_semaphore()
    for target in targets:
        pl.semaphore_signal(barrier, inc=1, device_id=target, device_id_type=pl.DeviceIdType.MESH)
    return lambda: pl.semaphore_wait(barrier, len(targets))


def send(src, dst, send_sem, recv_sem, target):
    return pltpu.make_async_remote_copy(
        src_ref=src,
        dst_ref=dst,
        send_sem=send_sem,
        recv_sem=recv_sem,
        device_id=target,
        device_id_type=pl.DeviceIdType.MESH,
    )


Z_ORDER = (4, 3, 5, 2, 6, 1, 7)
SLOT_DX = (0, 1, 3, 2)


def halves(value):
    high = value.astype(BF)
    low = (value - high.astype(F32)).astype(BF)
    return high, low


def dot(left, right):
    return jnp.dot(left, right, preferred_element_type=F32)


def product3(left, right):
    left_high, left_low = left
    right_high, right_low = right
    return dot(
        jnp.concatenate([left_high, left_low], 1), jnp.concatenate([right_high, right_high], 0)
    ) + dot(left_high, right_low)


def swap(value):
    return pltpu.roll(value, NORB, 1)


def lane_masks():
    rows = lax.broadcasted_iota(jnp.int32, (NORB, WIDE), 0)
    lanes = lax.broadcasted_iota(jnp.int32, (NORB, WIDE), 1)
    return lanes, lanes < NORB, rows == lanes % NORB


def gather_kernel(
    w_hbm, n_hbm, h_hbm, s_hbm, g_hbm,
    gall, er_ref, ei_ref, ur_ref, ui_ref, tr_ref, ti_ref, count_ref,
    w_ref, n_ref, h_ref, hall, sall, wh, wl, hcol, hrow, gcat, gz, zcol, zrow, gh_ref,
    zs, zr, ps, pr, ss, sr, gs, gr, own,
):
    f = lax.axis_index("freq")
    y = lax.axis_index("kgrp")
    x, t = f // LINE, f % LINE
    z, c = t // CORES, t % CORES
    partner = on_freq(x * LINE + z * CORES + (1 - c))
    lanes, first, eye_mask = lane_masks()
    eye = eye_mask.astype(F32)
    half = NORB // 2
    row_ids = lax.broadcasted_iota(jnp.int32, (NORB, WIDE), 0)
    below, above = row_ids > lanes % NORB, row_ids < lanes % NORB

    def along_z(dz):
        return on_freq(x * LINE + (z + dz) % ZS * CORES + c)

    def along_x(dx):
        return on_freq((x + dx) % XS * LINE + t)

    def paired(one, two):
        return jnp.where(first, one, swap(two)), jnp.where(first, swap(one), two)

    def as_right(real, imag):
        def build(r, i):
            return jnp.concatenate([jnp.concatenate([r, i], 1), jnp.concatenate([-i, r], 1)], 0)

        real_high, real_low = halves(real)
        imag_high, imag_low = halves(imag)
        return build(real_high, imag_high), build(real_low, imag_low)

    def diagonal_columns(value):
        kept = jnp.where(eye_mask, value, 0.0)
        left = jnp.sum(jnp.where(first, kept, 0.0), 1, keepdims=True)
        right = jnp.sum(jnp.where(first, 0.0, kept), 1, keepdims=True)
        return jnp.where(first, left, right)

    def diagonal_row(value):
        return jnp.sum(jnp.where(eye_mask, value, 0.0), 0, keepdims=True)

    def prepare_freqs(slot):
        owner = (x + XS - SLOT_DX[slot]) % XS
        for b in range(PER_FREQ):
            n = slot * PER_FREQ + b
            freq_id = owner * (PER_FREQ * LINE) + t * PER_FREQ + b
            count_ref[n : n + 1] = jnp.full((1, WIDE), n_ref[freq_id].astype(F32))
            matsubara = (2 * freq_id + 1).astype(F32) * (math.pi / (2 * FREQ))
            shift = jnp.where(first, chem_potential, matsubara)
            zed = jnp.where(eye_mask, shift, 0.0) - sall[n]
            real, imag = paired(zed, zed)
            g_high, g_low = halves(gall[n])
            gz[n] = product3((g_high, g_low), as_right(real, imag))
            gcat[n] = jnp.concatenate([g_high, g_low], 1)
            zcol[n] = jnp.concatenate([diagonal_columns(real), diagonal_columns(imag)], 1)
            zrow[n : n + 1] = jnp.concatenate([diagonal_row(real), diagonal_row(imag)], 1)

    def prepare_pair(p):
        one, two = hall[p, 0], hall[p, 1]
        packed = jnp.concatenate(
            [jnp.where(first[:half], one, swap(two)), jnp.where(first[:half], swap(one), two)], 0
        )
        flipped = jnp.concatenate([packed, swap(packed)], 0).T[:NORB]
        real = jnp.where(above, flipped, packed)
        imag = jnp.where(above, packed, jnp.where(below, -flipped, 0.0))
        high, low = as_right(real, imag)
        wh[p] = high
        wl[p] = low
        hcol[p] = diagonal_columns(real)
        hrow[p : p + 1] = diagonal_row(real)

    first_rows = pl.ds(0, PER_FREQ)
    own_h, own_s, own_g = hall.at[0, 0], sall.at[first_rows], gall.at[first_rows]
    loads = [
        pltpu.make_async_copy(src, dst, own.at[i])
        for i, (src, dst) in enumerate(
            ((h_hbm.at[0], h_ref), (g_hbm, own_g), (s_hbm, own_s), (w_hbm, w_ref), (n_hbm, n_ref))
        )
    ]
    for load in loads:
        load.start()
    await_greetings = greet(
        [partner] + [along_z(dz) for dz in range(1, ZS)] + [along_x(dx) for dx in range(1, XS)]
    )
    tr_ref[...] = jnp.zeros_like(tr_ref)
    ti_ref[...] = jnp.zeros_like(ti_ref)
    for load in loads:
        load.wait()
    h = h_ref[...]
    folded = jnp.where(above ^ first, h, swap(h))
    own_h[...] = jnp.where(first[:half], folded[:half], folded[half:])
    prepare_freqs(0)

    def add_up(i, total):
        for j in range(16):
            total = total + w_ref[i * 16 + j]
        return total

    inv_total = 1.0 / lax.fori_loop(0, KPTS // 16, add_up, jnp.int32(0)).astype(F32)
    await_greetings()

    def z_copy(dz):
        return send(own_h, hall.at[dz, 0], zs.at[dz], zr.at[dz], along_z(dz))

    def partner_copy(dz):
        return send(hall.at[dz, 0], hall.at[dz, 1], ps.at[dz], pr.at[dz], partner)

    def freq_copies(slot):
        rows = pl.ds(slot * PER_FREQ, PER_FREQ)
        if slot < 3:
            g_from, s_from = own_g, own_s
            g_to = s_to = along_x(SLOT_DX[slot])
        else:
            g_from, g_to = gall.at[pl.ds(1 * PER_FREQ, PER_FREQ)], along_x(1)
            s_from, s_to = sall.at[pl.ds(2 * PER_FREQ, PER_FREQ)], along_x(XS - 1)
        return (
            send(g_from, gall.at[rows], gs.at[slot], gr.at[slot], g_to),
            send(s_from, sall.at[rows], ss.at[slot], sr.at[slot], s_to),
        )

    started = []

    def begin(copy):
        copy.start()
        started.append(copy)

    begin(partner_copy(0))
    for dz in Z_ORDER:
        begin(z_copy(dz))
    begin(freq_copies(1)[0])
    begin(freq_copies(2)[1])
    begin(freq_copies(1)[1])
    begin(freq_copies(2)[0])

    def residuals(p, low, high):
        left = gcat[low:high].reshape((high - low) * NORB, 2 * WIDE)
        right = wh[p]
        gh_ref[: (high - low) * NORB] = dot(left, jnp.concatenate([right, right], 0)) + dot(
            left[:, :WIDE], wl[p]
        )
        h_diag = hcol[p]
        chip = x * LINE + (z + ZS - p) % ZS * CORES
        w_one = w_ref[(chip + c) * YS + y].astype(F32) * inv_total
        w_two = w_ref[(chip + 1 - c) * YS + y].astype(F32) * inv_total
        weight = jnp.where(first[: high - low], w_one, w_two)
        d_real, d_imag = zrow[low:high, :WIDE] - hrow[pl.ds(p, 1)], zrow[low:high, WIDE:]
        inv = weight / (d_real * d_real + d_imag * d_imag)
        ur_ref[p, low:high] = d_real * inv
        ui_ref[p, low:high] = -d_imag * inv
        for n in range(low, high):
            a = gz[n] - gh_ref[(n - low) * NORB : (n - low + 1) * NORB]
            a_real, a_imag = a[:, :WIDE], a[:, WIDE:]
            d = zcol[n]
            d_real, d_imag = d[:, :WIDE] - h_diag, d[:, WIDE:]
            inv = 1.0 / (d_real * d_real + d_imag * d_imag)
            v_real, v_imag = d_real * inv, d_imag * inv
            e_real = eye - (v_real * a_real + v_imag * a_imag)
            e_imag = v_imag * a_real - v_real * a_imag
            er_ref[n, p] = e_real
            ei_ref[n, p] = e_imag
            u_real, u_imag = ur_ref[p, n : n + 1], ui_ref[p, n : n + 1]
            q_real = eye + e_real
            tr_ref[n] += q_real * u_real - e_imag * u_imag
            ti_ref[n] += q_real * u_imag + e_imag * u_real

    def arrived_z(*steps):
        for dz in steps:
            z_copy(dz).wait_recv()
            begin(partner_copy(dz))

    def arrived_pair(*steps):
        for dz in steps:
            partner_copy(dz).wait_recv()
        for dz in steps:
            prepare_pair(dz)
        for dz in steps:
            residuals(dz, 0, PER_FREQ)

    near_g, near_s = freq_copies(1), freq_copies(2)
    far = freq_copies(3)
    arrived_pair(0)
    arrived_z(1, 7)
    near_g[0].wait_recv()
    begin(far[0])
    near_s[1].wait_recv()
    begin(far[1])
    arrived_z(2, 6)
    arrived_pair(1, 7)
    arrived_z(3, 5)
    arrived_pair(2, 6)
    near_g[1].wait_recv()
    near_s[0].wait_recv()
    prepare_freqs(1)
    prepare_freqs(2)
    arrived_z(4)
    arrived_pair(3, 5)

    def near_freqs(q, carry):
        residuals(1 + q, PER_FREQ, 3 * PER_FREQ)
        residuals(ZS - 1 - q, PER_FREQ, 3 * PER_FREQ)
        return carry

    lax.fori_loop(0, 3, near_freqs, 0)
    arrived_pair(4)
    residuals(0, PER_FREQ, 3 * PER_FREQ)
    residuals(4, PER_FREQ, 3 * PER_FREQ)
    for copy in far:
        copy.wait_recv()
    prepare_freqs(3)

    def far_freqs(p, carry):
        residuals(p, 3 * PER_FREQ, N_LOCAL)
        return carry

    lax.fori_loop(0, PAIRS, far_freqs, 0, unroll=4)
    for copy in started:
        copy.wait_send()


def gather(*values):
    dma = pltpu.SemaphoreType.DMA
    powers = jax.ShapeDtypeStruct((N_LOCAL, PAIRS, NORB, WIDE), F32)
    scales = jax.ShapeDtypeStruct((PAIRS, N_LOCAL, WIDE), F32)
    totals = jax.ShapeDtypeStruct((N_LOCAL, NORB, WIDE), F32)
    counted = jax.ShapeDtypeStruct((N_LOCAL, WIDE), F32)
    return pl.pallas_call(
        gather_kernel,
        name="gather",
        out_shape=(totals, powers, powers, scales, scales, totals, totals, counted),
        in_specs=[hbm()] * 5,
        out_specs=(vmem(),) * 8,
        scratch_shapes=[
            pltpu.SMEM((KPTS,), jnp.int32),
            pltpu.SMEM((FREQ,), jnp.int32),
            pltpu.VMEM((NORB, WIDE), F32),
            pltpu.VMEM((ZS, CORES, NORB // 2, WIDE), F32),
            pltpu.VMEM((N_LOCAL, NORB, WIDE), F32),
            pltpu.VMEM((PAIRS, WIDE, 2 * WIDE), BF),
            pltpu.VMEM((PAIRS, WIDE, 2 * WIDE), BF),
            pltpu.VMEM((PAIRS, NORB, WIDE), F32),
            pltpu.VMEM((PAIRS, WIDE), F32),
            pltpu.VMEM((N_LOCAL, NORB, 2 * WIDE), BF),
            pltpu.VMEM((N_LOCAL, NORB, 2 * WIDE), F32),
            pltpu.VMEM((N_LOCAL, NORB, 2 * WIDE), F32),
            pltpu.VMEM((N_LOCAL, 2 * WIDE), F32),
            pltpu.VMEM((N_LOCAL * NORB, 2 * WIDE), F32),
        ]
        + [dma((ZS,))] * 4
        + [dma((XS,))] * 4
        + [dma((5,))],
        compiler_params=pltpu.CompilerParams(
            collective_id=0, has_side_effects=True, vmem_limit_bytes=20 << 20
        ),
    )(*(pltpu.with_memory_space_constraint(value, pltpu.HBM) for value in values))


def power_kernel(
    er_ref, ei_ref, ur_ref, ui_ref, t1r_ref, t1i_ref, count_ref, tr_ref, ti_ref, sr_ref, si_ref, qr_ref, qi_ref, steps_ref
):
    _, first, eye_mask = lane_masks()
    eye = eye_mask.astype(F32)
    first_bf = first.astype(F32).astype(BF)
    second_bf = (1.0 - first.astype(F32)).astype(BF)

    def right_blocks(real, imag):
        def build(r, i):
            return jnp.concatenate(
                [
                    jnp.concatenate([r * first_bf, i * first_bf], 1),
                    jnp.concatenate([r * second_bf, i * second_bf], 1),
                ],
                0,
            )

        r_high, r_low = halves(real)
        i_high, i_low = halves(imag)
        return build(r_high, i_high), build(r_low, i_low)

    def left_rows(real, imag):
        return halves(jnp.concatenate([real, imag], 0))

    def combine(out):
        return out[:NORB, :WIDE] - out[NORB:, WIDE:], out[:NORB, WIDE:] + out[NORB:, :WIDE]

    def weighted(n, p, real, imag):
        u_real, u_imag = ur_ref[p, pl.ds(n, 1)], ui_ref[p, pl.ds(n, 1)]
        return real * u_real - imag * u_imag, real * u_imag + imag * u_real

    def two_steps(n):
        for p in range(PAIRS):
            e_real, e_imag = er_ref[n, p], ei_ref[n, p]
            sr_ref[p], si_ref[p] = combine(product3(left_rows(e_real, e_imag), right_blocks(e_real, e_imag)))
        total = t1r_ref[n], t1i_ref[n]
        for p in range(PAIRS):
            left = left_rows(eye + er_ref[n, p], ei_ref[n, p])
            real, imag = combine(product3(left, right_blocks(sr_ref[p], si_ref[p])))
            real, imag = weighted(n, p, real, imag)
            total = total[0] + real, total[1] + imag
        tr_ref[n], ti_ref[n] = total

    def three_steps(n):
        for p in range(PAIRS):
            e_real, e_imag = er_ref[n, p], ei_ref[n, p]
            sr_ref[p], si_ref[p] = combine(product3(left_rows(e_real, e_imag), right_blocks(e_real, e_imag)))
        for p in range(PAIRS):
            e_real, e_imag = er_ref[n, p], ei_ref[n, p]
            s_real, s_imag = sr_ref[p], si_ref[p]
            right = right_blocks(s_real, s_imag)
            real, imag = combine(product3(left_rows(eye + e_real, e_imag), right))
            qr_ref[p], qi_ref[p] = eye + e_real + real, e_imag + imag
            sr_ref[p], si_ref[p] = combine(product3(left_rows(s_real, s_imag), right))
        total = None
        for p in range(PAIRS):
            q_real, q_imag = qr_ref[p], qi_ref[p]
            real, imag = combine(product3(left_rows(q_real, q_imag), right_blocks(sr_ref[p], si_ref[p])))
            real, imag = weighted(n, p, q_real + real, q_imag + imag)
            total = (real, imag) if total is None else (total[0] + real, total[1] + imag)
        tr_ref[n], ti_ref[n] = total

    for n in range(N_LOCAL):
        steps_ref[n] = jnp.max(count_ref[n : n + 1])
    tr_ref[...] = t1r_ref[...]
    ti_ref[...] = t1i_ref[...]

    def one_freq(n, carry):
        steps = steps_ref[n]
        pl.when((steps > 1.5) & (steps < 2.5))(functools.partial(two_steps, n))
        pl.when(steps > 2.5)(functools.partial(three_steps, n))
        return carry

    lax.fori_loop(0, N_LOCAL, one_freq, 0)


def invert(*gathered):
    slots = pltpu.VMEM((PAIRS, NORB, WIDE), F32)
    totals = jax.ShapeDtypeStruct((N_LOCAL, NORB, WIDE), F32)
    return pl.pallas_call(
        power_kernel,
        name="invert",
        out_shape=(totals, totals),
        in_specs=[vmem()] * 7,
        out_specs=(vmem(),) * 2,
        scratch_shapes=[slots] * 4 + [pltpu.SMEM((N_LOCAL,), F32)],
        compiler_params=pltpu.CompilerParams(vmem_limit_bytes=16 << 20),
    )(*gathered)


def exit_kernel(g_ref, tr_ref, ti_ref, q_ref, o_ref, landed, rows_ref, as_, ar, bs, br):
    f = lax.axis_index("freq")
    y = lax.axis_index("kgrp")
    x, t = f // LINE, f % LINE
    z, c = t // CORES, t % CORES
    plane = [(dx, dy) for dx in range(XS) for dy in range(YS) if dx or dy]
    line = [(dz, dc) for dz in range(ZS) for dc in range(CORES) if dz or dc]

    def in_plane(dx, dy):
        return {"freq": (x + dx) % XS * LINE + t, "kgrp": (y + dy) % YS}

    def place(dz, dc):
        return (z + dz) % ZS * CORES + (c + dc) % CORES

    await_greetings = greet([in_plane(*d) for d in plane] + [on_freq(x * LINE + place(*d)) for d in line])
    lanes, first, _ = lane_masks()
    quarter = lanes % NORB // (NORB // YS)
    for n_high in range(2):
        mixed = [None] * YS
        for n_low in range(4):
            dx = (x + XS - n_high * 2 - n_low // 2) % XS
            n = (dx + dx // 2 * (5 - 2 * dx)) * PER_FREQ + n_low % 2
            g = g_ref[n]
            turned = jnp.where(first, -swap(g), swap(g))
            r_high, r_low = halves(jnp.concatenate([g, g, turned, turned], 0))
            l_high, l_low = halves(jnp.concatenate([tr_ref[n], ti_ref[n]], 1))
            both = dot(l_high, jnp.concatenate([r_high, r_low], 1))
            value = both[:, :WIDE] + both[:, WIDE:] + dot(l_low, r_high)
            for to_y in range(YS):
                shift = (n_low - to_y) * (NORB // YS) % WIDE
                moved = pltpu.roll(value, shift, 1) if shift else value
                mixed[to_y] = moved if n_low == 0 else jnp.where(quarter == n_low, moved, mixed[to_y])
        for to_y in range(YS):
            for to_x in range(XS):
                o_ref[to_x, to_y, n_high] = mixed[to_y][to_x * LINE : (to_x + 1) * LINE]
    await_greetings()
    started = []
    for dx, dy in plane:
        slot = dx * YS + dy
        copy = send(
            o_ref.at[(x + dx) % XS, (y + dy) % YS], landed.at[slot], as_.at[slot], ar.at[slot], in_plane(dx, dy)
        )
        copy.start()
        started.append(copy)
    total = o_ref[x, y]
    for dx, dy in plane:
        slot = dx * YS + dy
        send(o_ref.at[x, y], landed.at[slot], as_.at[slot], ar.at[slot], in_plane(dx, dy)).wait_recv()
        total = total + landed[slot]
    for to in range(LINE):
        for n_high in range(2):
            rows_ref[to, n_high : n_high + 1] = total[n_high, to : to + 1]
    for dz, dc in line:
        slot = dz * CORES + dc
        to = place(dz, dc)
        copy = send(rows_ref.at[to], q_ref.at[t], bs.at[slot], br.at[slot], on_freq(x * LINE + to))
        copy.start()
        started.append(copy)
    q_ref[pl.ds(t, 1)] = rows_ref[pl.ds(t, 1)]
    for dz, dc in line:
        slot = dz * CORES + dc
        source = (z + ZS - dz) % ZS * CORES + (c + CORES - dc) % CORES
        send(rows_ref.at[source], q_ref.at[source], bs.at[slot], br.at[slot], on_freq(x * LINE + place(dz, dc))).wait_recv()
    for copy in started:
        copy.wait_send()


def leave(*parts):
    dma = pltpu.SemaphoreType.DMA
    return pl.pallas_call(
        exit_kernel,
        name="leave",
        out_shape=jax.ShapeDtypeStruct((LINE, 2, WIDE), F32),
        in_specs=[vmem()] * 3,
        out_specs=vmem(),
        scratch_shapes=[
            pltpu.VMEM((XS, YS, 2, LINE, WIDE), F32),
            pltpu.VMEM((XS * YS, 2, LINE, WIDE), F32),
            pltpu.VMEM((LINE, 2, WIDE), F32),
            dma((XS * YS,)),
            dma((XS * YS,)),
            dma((LINE,)),
            dma((LINE,)),
        ],
        compiler_params=pltpu.CompilerParams(
            collective_id=1, has_side_effects=True, vmem_limit_bytes=8 << 20
        ),
    )(*parts)


def per_device(hamiltonian, self_energy, guess_factor, weights, counts):
    g_all, *gathered = gather(weights, counts, hamiltonian, self_energy, guess_factor)
    arrived = leave(g_all, *invert(*gathered))
    pieces = arrived.reshape(LINE, 2, 2, 2, 2, NORB // YS)
    return pieces.transpose(5, 2, 1, 3, 0, 4).reshape(NORB // YS, 2 * FREQ)


def solution(mesh):
    return jax.shard_map(
        per_device,
        mesh=mesh,
        in_specs=(
            P(("freq", "kgrp"), None, None),
            P("freq", None, None),
            P("freq", None, None),
            P(),
            P(),
        ),
        out_specs=P(("freq", "kgrp"), None),
        check_vma=False,
    )
```

```python
import functools
import math

import jax
import jax.numpy as jnp
from jax import lax
from jax.experimental import pallas as pl
from jax.experimental.pallas import tpu as pltpu
from jax.sharding import PartitionSpec as P

chem_potential = 0.2

NORB = 64
WIDE = 2 * NORB
XS, YS, ZS, CORES = 4, 4, 8, 2
LINE = ZS * CORES
PER_FREQ = 2
N_LOCAL = XS * PER_FREQ
PAIRS = LINE // 2
FREQ = 128
KPTS = 256
BF = jnp.bfloat16
F32 = jnp.float32


def vmem():
    return pl.BlockSpec(memory_space=pltpu.VMEM)


def smem():
    return pl.BlockSpec(memory_space=pltpu.SMEM)


def hbm():
    return pl.BlockSpec(memory_space=pltpu.HBM)


def on_freq(index):
    return {"freq": index}


def greet(targets):
    barrier = pltpu.get_barrier_semaphore()
    for target in targets:
        pl.semaphore_signal(barrier, inc=1, device_id=target, device_id_type=pl.DeviceIdType.MESH)
    return lambda: pl.semaphore_wait(barrier, len(targets))


def send(src, dst, send_sem, recv_sem, target):
    return pltpu.make_async_remote_copy(
        src_ref=src,
        dst_ref=dst,
        send_sem=send_sem,
        recv_sem=recv_sem,
        device_id=target,
        device_id_type=pl.DeviceIdType.MESH,
    )


Z_ORDER = (4, 3, 5, 2, 6, 1, 7)
SLOT_DX = (0, 1, 3, 2)


def halves(value):
    high = value.astype(BF)
    low = (value - high.astype(F32)).astype(BF)
    return high, low


def dot(left, right):
    return jnp.dot(left, right, preferred_element_type=F32)


def product3(left, right):
    left_high, left_low = left
    right_high, right_low = right
    return dot(
        jnp.concatenate([left_high, left_low], 1), jnp.concatenate([right_high, right_high], 0)
    ) + dot(left_high, right_low)


def swap(value):
    return pltpu.roll(value, NORB, 1)


def lane_masks():
    rows = lax.broadcasted_iota(jnp.int32, (NORB, WIDE), 0)
    lanes = lax.broadcasted_iota(jnp.int32, (NORB, WIDE), 1)
    return lanes, lanes < NORB, rows == lanes % NORB


def gather_kernel(
    w_hbm, n_hbm, h_hbm, s_hbm, g_hbm,
    gall, er_ref, ei_ref, ur_ref, ui_ref, tr_ref, ti_ref, count_ref,
    w_ref, n_ref, h_ref, s_ref, hall, zall, wh, wl, hcol, hrow, gcat, gz, zcol, zrow,
    zs, zr, ps, pr, ss, sr, gs, gr, own,
):
    f = lax.axis_index("freq")
    y = lax.axis_index("kgrp")
    x, t = f // LINE, f % LINE
    z, c = t // CORES, t % CORES
    partner = on_freq(x * LINE + z * CORES + (1 - c))
    lanes, first, eye_mask = lane_masks()
    eye = eye_mask.astype(F32)
    half = NORB // 2
    row_ids = lax.broadcasted_iota(jnp.int32, (NORB, WIDE), 0)
    below, above = row_ids > lanes % NORB, row_ids < lanes % NORB

    def along_z(dz):
        return on_freq(x * LINE + (z + dz) % ZS * CORES + c)

    def along_x(dx):
        return on_freq((x + dx) % XS * LINE + t)

    def both_parts(value):
        turned = swap(value)
        return jnp.concatenate([jnp.where(first, value, turned), jnp.where(first, turned, value)], 1)

    def as_right(real, imag):
        def build(r, i):
            return jnp.concatenate([jnp.concatenate([r, i], 1), jnp.concatenate([-i, r], 1)], 0)

        real_high, real_low = halves(real)
        imag_high, imag_low = halves(imag)
        return build(real_high, imag_high), build(real_low, imag_low)

    def diagonal_columns(value):
        kept = jnp.where(eye_mask, value, 0.0)
        left = jnp.sum(jnp.where(first, kept, 0.0), 1, keepdims=True)
        right = jnp.sum(jnp.where(first, 0.0, kept), 1, keepdims=True)
        return jnp.where(first, left, right)

    def diagonal_row(value):
        return jnp.sum(jnp.where(eye_mask, value, 0.0), 0, keepdims=True)

    def freq_of(slot, b):
        return (x + XS - SLOT_DX[slot]) % XS * (PER_FREQ * LINE) + t * PER_FREQ + b

    def share_freq(b):
        matsubara = (2 * freq_of(0, b) + 1).astype(F32) * (math.pi / (2 * FREQ))
        zed = jnp.where(eye_mask, jnp.where(first, chem_potential, matsubara), 0.0) - s_ref[b]
        turned = swap(zed)
        right = jnp.concatenate([zed, jnp.where(first, -turned, turned)], 0)
        zall[b, :NORB] = product3(halves(gall[b]), halves(right))
        zall[b, NORB:] = jnp.broadcast_to(diagonal_row(zed), (8, WIDE))

    def prepare_freqs(slot):
        for b in range(PER_FREQ):
            n = slot * PER_FREQ + b
            count_ref[n : n + 1] = jnp.full((1, WIDE), n_ref[freq_of(slot, b)].astype(F32))
            product, row = zall[n, :NORB], zall[n, NORB : NORB + 1]
            gcat[n] = jnp.concatenate(halves(gall[n]), 1)
            gz[n] = both_parts(product)
            zrow[n : n + 1] = jnp.concatenate(
                [jnp.where(first[:1], row, swap(row)), jnp.where(first[:1], swap(row), row)], 1
            )
            kept = jnp.where(eye_mask, row, 0.0)
            real = jnp.sum(jnp.where(first, kept, 0.0), 1, keepdims=True)
            imag = jnp.sum(jnp.where(first, 0.0, kept), 1, keepdims=True)
            zcol[n] = jnp.concatenate(
                [jnp.broadcast_to(part, (NORB, WIDE)) for part in (real, imag, imag * imag)], 1
            )

    def prepare_pair(p):
        one, two = hall[p, 0], hall[p, 1]
        packed = jnp.concatenate(
            [jnp.where(first[:half], one, swap(two)), jnp.where(first[:half], swap(one), two)], 0
        )
        flipped = jnp.concatenate([packed, swap(packed)], 0).T[:NORB]
        real = jnp.where(above, flipped, packed)
        imag = jnp.where(above, packed, jnp.where(below, -flipped, 0.0))
        high, low = as_right(real, imag)
        wh[p] = high
        wl[p] = low
        hcol[p] = diagonal_columns(real)
        hrow[p : p + 1] = diagonal_row(real)

    first_rows = pl.ds(0, PER_FREQ)
    own_h, own_z, own_g = hall.at[0, 0], zall.at[first_rows], gall.at[first_rows]
    loads = [
        pltpu.make_async_copy(src, dst, own.at[i])
        for i, (src, dst) in enumerate(
            ((h_hbm.at[0], h_ref), (g_hbm, own_g), (s_hbm, s_ref), (w_hbm, w_ref), (n_hbm, n_ref))
        )
    ]
    for load in loads:
        load.start()
    await_greetings = greet(
        [along_z(dz) for dz in Z_ORDER] + [along_x(dx) for dx in (2, 1, 3)] + [partner]
    )
    tr_ref[...] = jnp.zeros_like(tr_ref)
    ti_ref[...] = jnp.zeros_like(ti_ref)
    for load in loads:
        load.wait()
    h = h_ref[...]
    folded = jnp.where(above ^ first, h, swap(h))
    own_h[...] = jnp.where(first[:half], folded[:half], folded[half:])
    for b in range(PER_FREQ):
        share_freq(b)
    prepare_freqs(0)

    def add_up(i, total):
        for j in range(16):
            total = total + w_ref[i * 16 + j]
        return total

    inv_total = 1.0 / lax.fori_loop(0, KPTS // 16, add_up, jnp.int32(0)).astype(F32)
    await_greetings()

    def z_copy(dz):
        return send(own_h, hall.at[dz, 0], zs.at[dz], zr.at[dz], along_z(dz))

    def partner_copy(dz):
        return send(hall.at[dz, 0], hall.at[dz, 1], ps.at[dz], pr.at[dz], partner)

    def freq_copies(slot):
        rows = pl.ds(slot * PER_FREQ, PER_FREQ)
        if slot < 3:
            g_from, z_from = own_g, own_z
            g_to = z_to = along_x(SLOT_DX[slot])
        else:
            g_from, g_to = gall.at[pl.ds(1 * PER_FREQ, PER_FREQ)], along_x(1)
            z_from, z_to = zall.at[pl.ds(2 * PER_FREQ, PER_FREQ)], along_x(XS - 1)
        return (
            send(g_from, gall.at[rows], gs.at[slot], gr.at[slot], g_to),
            send(z_from, zall.at[rows], ss.at[slot], sr.at[slot], z_to),
        )

    started = []

    def begin(copy):
        copy.start()
        started.append(copy)

    begin(partner_copy(0))
    for dz in Z_ORDER:
        begin(z_copy(dz))
    begin(freq_copies(1)[0])
    begin(freq_copies(2)[1])
    begin(freq_copies(1)[1])
    begin(freq_copies(2)[0])

    def residuals(p, low, high):
        left = gcat[low:high].reshape((high - low) * NORB, 2 * WIDE)
        right = wh[p]
        gh = dot(left, jnp.concatenate([right, right], 0)) + dot(left[:, :WIDE], wl[p])
        h_diag = hcol[p]
        chip = x * LINE + (z + ZS - p) % ZS * CORES
        w_one = w_ref[(chip + c) * YS + y].astype(F32) * inv_total
        w_two = w_ref[(chip + 1 - c) * YS + y].astype(F32) * inv_total
        weight = jnp.where(first[: high - low], w_one, w_two)
        d_real, d_imag = zrow[low:high, :WIDE] - hrow[pl.ds(p, 1)], zrow[low:high, WIDE:]
        inv = weight / (d_real * d_real + d_imag * d_imag)
        ur_ref[p, low:high] = d_real * inv
        ui_ref[p, low:high] = -d_imag * inv
        for n in range(low, high):
            a = gz[n] - gh[(n - low) * NORB : (n - low + 1) * NORB]
            a_real, a_imag = a[:, :WIDE], a[:, WIDE:]
            d = zcol[n]
            d_real, d_imag = d[:, :WIDE] - h_diag, d[:, WIDE : 2 * WIDE]
            inv = 1.0 / (d_real * d_real + d[:, 2 * WIDE :])
            v_real, v_imag = d_real * inv, d_imag * inv
            e_real = eye - (v_real * a_real + v_imag * a_imag)
            e_imag = v_imag * a_real - v_real * a_imag
            er_ref[n, p] = e_real
            ei_ref[n, p] = e_imag
            u_real, u_imag = ur_ref[p, n : n + 1], ui_ref[p, n : n + 1]
            q_real = eye + e_real
            tr_ref[n] += q_real * u_real - e_imag * u_imag
            ti_ref[n] += q_real * u_imag + e_imag * u_real

    def arrived_z(*steps):
        for dz in steps:
            z_copy(dz).wait_recv()
            begin(partner_copy(dz))

    def arrived_pair(*steps):
        for dz in steps:
            partner_copy(dz).wait_recv()
        for dz in steps:
            prepare_pair(dz)
        for dz in steps:
            residuals(dz, 0, PER_FREQ)

    near_g, near_z = freq_copies(1), freq_copies(2)
    far = freq_copies(3)
    arrived_pair(0)
    arrived_z(1, 7)
    near_g[0].wait_recv()
    begin(far[0])
    near_z[1].wait_recv()
    begin(far[1])
    arrived_z(2, 6)
    arrived_pair(1, 7)
    near_g[1].wait_recv()
    near_z[0].wait_recv()
    prepare_freqs(1)
    prepare_freqs(2)
    arrived_z(3, 5)

    def near_freqs(*pairs):
        for p in pairs:
            residuals(p, PER_FREQ, 3 * PER_FREQ)

    near_freqs(0, 1, 7)
    arrived_z(4)
    arrived_pair(2, 6)
    near_freqs(2, 6)
    arrived_pair(3, 5)
    near_freqs(3, 5)
    arrived_pair(4)
    near_freqs(4)
    for copy in far:
        copy.wait_recv()
    prepare_freqs(3)

    def far_freqs(p, carry):
        residuals(p, 3 * PER_FREQ, N_LOCAL)
        return carry

    lax.fori_loop(0, PAIRS, far_freqs, 0, unroll=4)
    for copy in started:
        copy.wait_send()


def gather(*values):
    dma = pltpu.SemaphoreType.DMA
    powers = jax.ShapeDtypeStruct((N_LOCAL, PAIRS, NORB, WIDE), F32)
    scales = jax.ShapeDtypeStruct((PAIRS, N_LOCAL, WIDE), F32)
    totals = jax.ShapeDtypeStruct((N_LOCAL, NORB, WIDE), F32)
    counted = jax.ShapeDtypeStruct((N_LOCAL, WIDE), F32)
    return pl.pallas_call(
        gather_kernel,
        name="gather",
        out_shape=(totals, powers, powers, scales, scales, totals, totals, counted),
        in_specs=[hbm()] * 5,
        out_specs=(vmem(),) * 8,
        scratch_shapes=[
            pltpu.SMEM((KPTS,), jnp.int32),
            pltpu.SMEM((FREQ,), jnp.int32),
            pltpu.VMEM((NORB, WIDE), F32),
            pltpu.VMEM((PER_FREQ, NORB, WIDE), F32),
            pltpu.VMEM((ZS, CORES, NORB // 2, WIDE), F32),
            pltpu.VMEM((N_LOCAL, NORB + 8, WIDE), F32),
            pltpu.VMEM((PAIRS, WIDE, 2 * WIDE), BF),
            pltpu.VMEM((PAIRS, WIDE, 2 * WIDE), BF),
            pltpu.VMEM((PAIRS, NORB, WIDE), F32),
            pltpu.VMEM((PAIRS, WIDE), F32),
            pltpu.VMEM((N_LOCAL, NORB, 2 * WIDE), BF),
            pltpu.VMEM((N_LOCAL, NORB, 2 * WIDE), F32),
            pltpu.VMEM((N_LOCAL, NORB, 3 * WIDE), F32),
            pltpu.VMEM((N_LOCAL, 2 * WIDE), F32),
        ]
        + [dma((ZS,))] * 4
        + [dma((XS,))] * 4
        + [dma((5,))],
        compiler_params=pltpu.CompilerParams(
            collective_id=0, has_side_effects=True, vmem_limit_bytes=20 << 20
        ),
    )(*(pltpu.with_memory_space_constraint(value, pltpu.HBM) for value in values))


def power_kernel(
    er_ref, ei_ref, ur_ref, ui_ref, t1r_ref, t1i_ref, count_ref, tr_ref, ti_ref, sr_ref, si_ref, qr_ref, qi_ref, steps_ref
):
    _, first, eye_mask = lane_masks()
    eye = eye_mask.astype(F32)
    first_bf = first.astype(F32).astype(BF)
    second_bf = (1.0 - first.astype(F32)).astype(BF)

    def right_blocks(real, imag):
        def build(r, i):
            return jnp.concatenate(
                [
                    jnp.concatenate([r * first_bf, i * first_bf], 1),
                    jnp.concatenate([r * second_bf, i * second_bf], 1),
                ],
                0,
            )

        r_high, r_low = halves(real)
        i_high, i_low = halves(imag)
        return build(r_high, i_high), build(r_low, i_low)

    def left_rows(real, imag):
        return halves(jnp.concatenate([real, imag], 0))

    def combine(out):
        return out[:NORB, :WIDE] - out[NORB:, WIDE:], out[:NORB, WIDE:] + out[NORB:, :WIDE]

    def weighted(n, p, real, imag):
        u_real, u_imag = ur_ref[p, pl.ds(n, 1)], ui_ref[p, pl.ds(n, 1)]
        return real * u_real - imag * u_imag, real * u_imag + imag * u_real

    def two_steps(n):
        for p in range(PAIRS):
            e_real, e_imag = er_ref[n, p], ei_ref[n, p]
            sr_ref[p], si_ref[p] = combine(product3(left_rows(e_real, e_imag), right_blocks(e_real, e_imag)))
        total = t1r_ref[n], t1i_ref[n]
        for p in range(PAIRS):
            left = left_rows(eye + er_ref[n, p], ei_ref[n, p])
            real, imag = combine(product3(left, right_blocks(sr_ref[p], si_ref[p])))
            real, imag = weighted(n, p, real, imag)
            total = total[0] + real, total[1] + imag
        tr_ref[n], ti_ref[n] = total

    def three_steps(n):
        for p in range(PAIRS):
            e_real, e_imag = er_ref[n, p], ei_ref[n, p]
            sr_ref[p], si_ref[p] = combine(product3(left_rows(e_real, e_imag), right_blocks(e_real, e_imag)))
        for p in range(PAIRS):
            e_real, e_imag = er_ref[n, p], ei_ref[n, p]
            s_real, s_imag = sr_ref[p], si_ref[p]
            right = right_blocks(s_real, s_imag)
            real, imag = combine(product3(left_rows(eye + e_real, e_imag), right))
            qr_ref[p], qi_ref[p] = eye + e_real + real, e_imag + imag
            sr_ref[p], si_ref[p] = combine(product3(left_rows(s_real, s_imag), right))
        total = None
        for p in range(PAIRS):
            q_real, q_imag = qr_ref[p], qi_ref[p]
            real, imag = combine(product3(left_rows(q_real, q_imag), right_blocks(sr_ref[p], si_ref[p])))
            real, imag = weighted(n, p, q_real + real, q_imag + imag)
            total = (real, imag) if total is None else (total[0] + real, total[1] + imag)
        tr_ref[n], ti_ref[n] = total

    for n in range(N_LOCAL):
        steps_ref[n] = jnp.max(count_ref[n : n + 1])
    tr_ref[...] = t1r_ref[...]
    ti_ref[...] = t1i_ref[...]

    def one_freq(n, carry):
        steps = steps_ref[n]
        pl.when((steps > 1.5) & (steps < 2.5))(functools.partial(two_steps, n))
        pl.when(steps > 2.5)(functools.partial(three_steps, n))
        return carry

    lax.fori_loop(0, N_LOCAL, one_freq, 0)


def invert(*gathered):
    slots = pltpu.VMEM((PAIRS, NORB, WIDE), F32)
    totals = jax.ShapeDtypeStruct((N_LOCAL, NORB, WIDE), F32)
    return pl.pallas_call(
        power_kernel,
        name="invert",
        out_shape=(totals, totals),
        in_specs=[vmem()] * 7,
        out_specs=(vmem(),) * 2,
        scratch_shapes=[slots] * 4 + [pltpu.SMEM((N_LOCAL,), F32)],
        compiler_params=pltpu.CompilerParams(vmem_limit_bytes=16 << 20),
    )(*gathered)


def exit_kernel(g_ref, tr_ref, ti_ref, q_ref, o_ref, landed, rows_ref, as_, ar, bs, br):
    f = lax.axis_index("freq")
    y = lax.axis_index("kgrp")
    x, t = f // LINE, f % LINE
    z, c = t // CORES, t % CORES
    plane = [(dx, dy) for dx in (2, 1, 3, 0) for dy in (2, 1, 3, 0) if dx or dy]
    plane.sort(key=lambda step: -min(step[0], XS - step[0]) - min(step[1], YS - step[1]))
    line = [(dz, dc) for dz in (4, 3, 5, 2, 6, 1, 7, 0) for dc in (1, 0) if dz or dc]

    def in_plane(dx, dy):
        return {"freq": (x + dx) % XS * LINE + t, "kgrp": (y + dy) % YS}

    def place(dz, dc):
        return (z + dz) % ZS * CORES + (c + dc) % CORES

    await_greetings = greet([q for d, e in zip(plane, line) for q in (in_plane(*d), on_freq(x * LINE + place(*e)))])
    lanes, first, _ = lane_masks()
    quarter = lanes % NORB // (NORB // YS)
    for n_high in range(2):
        mixed = [None] * YS
        for n_low in range(4):
            dx = (x + XS - n_high * 2 - n_low // 2) % XS
            n = (dx + dx // 2 * (5 - 2 * dx)) * PER_FREQ + n_low % 2
            g = g_ref[n]
            turned = jnp.where(first, -swap(g), swap(g))
            r_high, r_low = halves(jnp.concatenate([g, g, turned, turned], 0))
            l_high, l_low = halves(jnp.concatenate([tr_ref[n], ti_ref[n]], 1))
            both = dot(l_high, jnp.concatenate([r_high, r_low], 1))
            value = both[:, :WIDE] + both[:, WIDE:] + dot(l_low, r_high)
            for to_y in range(YS):
                shift = (n_low - to_y) * (NORB // YS) % WIDE
                moved = pltpu.roll(value, shift, 1) if shift else value
                mixed[to_y] = moved if n_low == 0 else jnp.where(quarter == n_low, moved, mixed[to_y])
        for to_y in range(YS):
            for to_x in range(XS):
                o_ref[to_x, to_y, n_high] = mixed[to_y][to_x * LINE : (to_x + 1) * LINE]
    await_greetings()
    started = []
    for dx, dy in plane:
        slot = dx * YS + dy
        copy = send(
            o_ref.at[(x + dx) % XS, (y + dy) % YS], landed.at[slot], as_.at[slot], ar.at[slot], in_plane(dx, dy)
        )
        copy.start()
        started.append(copy)
    total = o_ref[x, y]
    for dx, dy in reversed(plane):
        slot = dx * YS + dy
        send(o_ref.at[x, y], landed.at[slot], as_.at[slot], ar.at[slot], in_plane(dx, dy)).wait_recv()
        total = total + landed[slot]
    for to in range(LINE):
        for n_high in range(2):
            rows_ref[to, n_high : n_high + 1] = total[n_high, to : to + 1]
    for dz, dc in line:
        slot = dz * CORES + dc
        to = place(dz, dc)
        copy = send(rows_ref.at[to], q_ref.at[t], bs.at[slot], br.at[slot], on_freq(x * LINE + to))
        copy.start()
        started.append(copy)
    q_ref[pl.ds(t, 1)] = rows_ref[pl.ds(t, 1)]
    for dz, dc in reversed(line):
        slot = dz * CORES + dc
        source = (z + ZS - dz) % ZS * CORES + (c + CORES - dc) % CORES
        send(rows_ref.at[source], q_ref.at[source], bs.at[slot], br.at[slot], on_freq(x * LINE + place(dz, dc))).wait_recv()
    for copy in started:
        copy.wait_send()


def leave(*parts):
    dma = pltpu.SemaphoreType.DMA
    return pl.pallas_call(
        exit_kernel,
        name="leave",
        out_shape=jax.ShapeDtypeStruct((LINE, 2, WIDE), F32),
        in_specs=[vmem()] * 3,
        out_specs=vmem(),
        scratch_shapes=[
            pltpu.VMEM((XS, YS, 2, LINE, WIDE), F32),
            pltpu.VMEM((XS * YS, 2, LINE, WIDE), F32),
            pltpu.VMEM((LINE, 2, WIDE), F32),
            dma((XS * YS,)),
            dma((XS * YS,)),
            dma((LINE,)),
            dma((LINE,)),
        ],
        compiler_params=pltpu.CompilerParams(
            collective_id=1, has_side_effects=True, vmem_limit_bytes=8 << 20
        ),
    )(*parts)


def per_device(hamiltonian, self_energy, guess_factor, weights, counts):
    g_all, *gathered = gather(weights, counts, hamiltonian, self_energy, guess_factor)
    arrived = leave(g_all, *invert(*gathered))
    pieces = arrived.reshape(LINE, 2, 2, 2, 2, NORB // YS)
    return pieces.transpose(5, 2, 1, 3, 0, 4).reshape(NORB // YS, 2 * FREQ)


def solution(mesh):
    return jax.shard_map(
        per_device,
        mesh=mesh,
        in_specs=(
            P(("freq", "kgrp"), None, None),
            P("freq", None, None),
            P("freq", None, None),
            P(),
            P(),
        ),
        out_specs=P(("freq", "kgrp"), None),
        check_vma=False,
    )
```

```python
import functools
import math

import jax
import jax.numpy as jnp
from jax import lax
from jax.experimental import pallas as pl
from jax.experimental.pallas import tpu as pltpu
from jax.sharding import PartitionSpec as P

chem_potential = 0.2

NORB = 64
WIDE = 2 * NORB
XS, YS, ZS, CORES = 4, 4, 8, 2
LINE = ZS * CORES
PER_FREQ = 2
N_LOCAL = XS * PER_FREQ
PAIRS = LINE // 2
FREQ = 128
KPTS = 256
BF = jnp.bfloat16
F32 = jnp.float32


def vmem():
    return pl.BlockSpec(memory_space=pltpu.VMEM)


def smem():
    return pl.BlockSpec(memory_space=pltpu.SMEM)


def hbm():
    return pl.BlockSpec(memory_space=pltpu.HBM)


def on_freq(index):
    return {"freq": index}


def greet(targets):
    barrier = pltpu.get_barrier_semaphore()
    for target in targets:
        pl.semaphore_signal(barrier, inc=1, device_id=target, device_id_type=pl.DeviceIdType.MESH)
    return lambda: pl.semaphore_wait(barrier, len(targets))


def send(src, dst, send_sem, recv_sem, target):
    return pltpu.make_async_remote_copy(
        src_ref=src,
        dst_ref=dst,
        send_sem=send_sem,
        recv_sem=recv_sem,
        device_id=target,
        device_id_type=pl.DeviceIdType.MESH,
    )


Z_ORDER = (4, 3, 5, 2, 6, 1, 7)
SLOT_DX = (0, 1, 3, 2)


def halves(value):
    high = value.astype(BF)
    low = (value - high.astype(F32)).astype(BF)
    return high, low


def dot(left, right):
    return jnp.dot(left, right, preferred_element_type=F32)


def product3(left, right):
    left_high, left_low = left
    right_high, right_low = right
    return dot(
        jnp.concatenate([left_high, left_low], 1), jnp.concatenate([right_high, right_high], 0)
    ) + dot(left_high, right_low)


def swap(value):
    return pltpu.roll(value, NORB, 1)


def lane_masks():
    rows = lax.broadcasted_iota(jnp.int32, (NORB, WIDE), 0)
    lanes = lax.broadcasted_iota(jnp.int32, (NORB, WIDE), 1)
    return lanes, lanes < NORB, rows == lanes % NORB


def gather_kernel(
    w_hbm, n_hbm, h_hbm, s_hbm, g_hbm,
    gall, er_ref, ei_ref, ur_ref, ui_ref, count_ref,
    w_ref, n_ref, h_ref, s_ref, hall, zall, wh, wl, hcol, hrow, gcat, gz, zcol, zrow,
    zs, zr, ps, pr, ss, sr, gs, gr, own,
):
    f = lax.axis_index("freq")
    y = lax.axis_index("kgrp")
    x, t = f // LINE, f % LINE
    z, c = t // CORES, t % CORES
    partner = on_freq(x * LINE + z * CORES + (1 - c))
    lanes, first, eye_mask = lane_masks()
    eye = eye_mask.astype(F32)
    half = NORB // 2
    row_ids = lax.broadcasted_iota(jnp.int32, (NORB, WIDE), 0)
    below, above = row_ids > lanes % NORB, row_ids < lanes % NORB

    def along_z(dz):
        return on_freq(x * LINE + (z + dz) % ZS * CORES + c)

    def along_x(dx):
        return on_freq((x + dx) % XS * LINE + t)

    def both_parts(value):
        turned = swap(value)
        return jnp.concatenate([jnp.where(first, value, turned), jnp.where(first, turned, value)], 1)

    def as_right(real, imag):
        def build(r, i):
            return jnp.concatenate([jnp.concatenate([r, i], 1), jnp.concatenate([-i, r], 1)], 0)

        real_high, real_low = halves(real)
        imag_high, imag_low = halves(imag)
        return build(real_high, imag_high), build(real_low, imag_low)

    def diagonal_columns(value):
        kept = jnp.where(eye_mask, value, 0.0)
        left = jnp.sum(jnp.where(first, kept, 0.0), 1, keepdims=True)
        right = jnp.sum(jnp.where(first, 0.0, kept), 1, keepdims=True)
        return jnp.where(first, left, right)

    def diagonal_row(value):
        return jnp.sum(jnp.where(eye_mask, value, 0.0), 0, keepdims=True)

    def freq_of(slot, b):
        return (x + XS - SLOT_DX[slot]) % XS * (PER_FREQ * LINE) + t * PER_FREQ + b

    def share_freq(b):
        matsubara = (2 * freq_of(0, b) + 1).astype(F32) * (math.pi / (2 * FREQ))
        zed = jnp.where(eye_mask, jnp.where(first, chem_potential, matsubara), 0.0) - s_ref[b]
        turned = swap(zed)
        right = jnp.concatenate([zed, jnp.where(first, -turned, turned)], 0)
        zall[b, :NORB] = product3(halves(gall[b]), halves(right))
        zall[b, NORB:] = jnp.broadcast_to(diagonal_row(zed), (8, WIDE))

    def prepare_freqs(slot):
        for b in range(PER_FREQ):
            n = slot * PER_FREQ + b
            count_ref[n : n + 1] = jnp.full((1, WIDE), n_ref[freq_of(slot, b)].astype(F32))
            product, row = zall[n, :NORB], zall[n, NORB : NORB + 1]
            gcat[n] = jnp.concatenate(halves(gall[n]), 1)
            gz[n] = both_parts(product)
            zrow[n : n + 1] = jnp.concatenate(
                [jnp.where(first[:1], row, swap(row)), jnp.where(first[:1], swap(row), row)], 1
            )
            kept = jnp.where(eye_mask, row, 0.0)
            real = jnp.sum(jnp.where(first, kept, 0.0), 1, keepdims=True)
            imag = jnp.sum(jnp.where(first, 0.0, kept), 1, keepdims=True)
            zcol[n] = jnp.concatenate(
                [jnp.broadcast_to(part, (NORB, WIDE)) for part in (real, imag, imag * imag)], 1
            )

    def prepare_pair(p):
        one, two = hall[p, 0], hall[p, 1]
        packed = jnp.concatenate(
            [jnp.where(first[:half], one, swap(two)), jnp.where(first[:half], swap(one), two)], 0
        )
        flipped = jnp.concatenate([packed, swap(packed)], 0).T[:NORB]
        real = jnp.where(above, flipped, packed)
        imag = jnp.where(above, packed, jnp.where(below, -flipped, 0.0))
        high, low = as_right(real, imag)
        wh[p] = high
        wl[p] = low
        hcol[p] = diagonal_columns(real)
        hrow[p : p + 1] = diagonal_row(real)

    first_rows = pl.ds(0, PER_FREQ)
    own_h, own_z, own_g = hall.at[0, 0], zall.at[first_rows], gall.at[first_rows]
    loads = [
        pltpu.make_async_copy(src, dst, own.at[i])
        for i, (src, dst) in enumerate(
            ((h_hbm.at[0], h_ref), (g_hbm, own_g), (s_hbm, s_ref), (w_hbm, w_ref), (n_hbm, n_ref))
        )
    ]
    for load in loads:
        load.start()
    await_greetings = greet(
        [along_z(dz) for dz in Z_ORDER] + [along_x(dx) for dx in (2, 1, 3)] + [partner]
    )
    for load in loads:
        load.wait()
    h = h_ref[...]
    folded = jnp.where(above ^ first, h, swap(h))
    own_h[...] = jnp.where(first[:half], folded[:half], folded[half:])
    for b in range(PER_FREQ):
        share_freq(b)
    prepare_freqs(0)

    def add_up(i, total):
        for j in range(16):
            total = total + w_ref[i * 16 + j]
        return total

    inv_total = 1.0 / lax.fori_loop(0, KPTS // 16, add_up, jnp.int32(0)).astype(F32)
    await_greetings()

    def z_copy(dz):
        return send(own_h, hall.at[dz, 0], zs.at[dz], zr.at[dz], along_z(dz))

    def partner_copy(dz):
        return send(hall.at[dz, 0], hall.at[dz, 1], ps.at[dz], pr.at[dz], partner)

    def freq_copies(slot):
        rows = pl.ds(slot * PER_FREQ, PER_FREQ)
        if slot < 3:
            g_from, z_from = own_g, own_z
            g_to = z_to = along_x(SLOT_DX[slot])
        else:
            g_from, g_to = gall.at[pl.ds(1 * PER_FREQ, PER_FREQ)], along_x(1)
            z_from, z_to = zall.at[pl.ds(2 * PER_FREQ, PER_FREQ)], along_x(XS - 1)
        return (
            send(g_from, gall.at[rows], gs.at[slot], gr.at[slot], g_to),
            send(z_from, zall.at[rows], ss.at[slot], sr.at[slot], z_to),
        )

    started = []

    def begin(copy):
        copy.start()
        started.append(copy)

    begin(partner_copy(0))
    for dz in Z_ORDER:
        begin(z_copy(dz))
    begin(freq_copies(1)[0])
    begin(freq_copies(2)[1])
    begin(freq_copies(1)[1])
    begin(freq_copies(2)[0])

    def residuals(p, low, high):
        left = gcat[low:high].reshape((high - low) * NORB, 2 * WIDE)
        right = wh[p]
        gh = dot(left, jnp.concatenate([right, right], 0)) + dot(left[:, :WIDE], wl[p])
        h_diag = hcol[p]
        chip = x * LINE + (z + ZS - p) % ZS * CORES
        w_one = w_ref[(chip + c) * YS + y].astype(F32) * inv_total
        w_two = w_ref[(chip + 1 - c) * YS + y].astype(F32) * inv_total
        weight = jnp.where(first[: high - low], w_one, w_two)
        d_real, d_imag = zrow[low:high, :WIDE] - hrow[pl.ds(p, 1)], zrow[low:high, WIDE:]
        inv = weight / (d_real * d_real + d_imag * d_imag)
        ur_ref[p, low:high] = d_real * inv
        ui_ref[p, low:high] = -d_imag * inv
        for n in range(low, high):
            a = gz[n] - gh[(n - low) * NORB : (n - low + 1) * NORB]
            a_real, a_imag = a[:, :WIDE], a[:, WIDE:]
            d = zcol[n]
            d_real, d_imag = d[:, :WIDE] - h_diag, d[:, WIDE : 2 * WIDE]
            inv = 1.0 / (d_real * d_real + d[:, 2 * WIDE :])
            v_real, v_imag = d_real * inv, d_imag * inv
            e_real = eye - (v_real * a_real + v_imag * a_imag)
            e_imag = v_imag * a_real - v_real * a_imag
            er_ref[n, p] = e_real
            ei_ref[n, p] = e_imag

    def arrived_z(*steps):
        for dz in steps:
            z_copy(dz).wait_recv()
            begin(partner_copy(dz))

    def arrived_pair(*steps):
        for dz in steps:
            partner_copy(dz).wait_recv()
        for dz in steps:
            prepare_pair(dz)
        for dz in steps:
            residuals(dz, 0, PER_FREQ)

    near_g, near_z = freq_copies(1), freq_copies(2)
    far = freq_copies(3)
    arrived_pair(0)
    arrived_z(1, 7)
    near_g[0].wait_recv()
    begin(far[0])
    near_z[1].wait_recv()
    begin(far[1])
    arrived_z(2, 6)
    arrived_pair(1, 7)
    near_g[1].wait_recv()
    near_z[0].wait_recv()
    prepare_freqs(1)
    prepare_freqs(2)
    arrived_z(3, 5)

    def near_freqs(*pairs):
        for p in pairs:
            residuals(p, PER_FREQ, 3 * PER_FREQ)

    near_freqs(0, 1, 7)
    arrived_z(4)
    arrived_pair(2, 6)
    near_freqs(2, 6)
    arrived_pair(3, 5)
    near_freqs(3, 5)
    arrived_pair(4)
    near_freqs(4)
    for copy in far:
        copy.wait_recv()
    prepare_freqs(3)

    def far_freqs(p, carry):
        residuals(p, 3 * PER_FREQ, N_LOCAL)
        return carry

    lax.fori_loop(0, PAIRS, far_freqs, 0, unroll=4)
    for copy in started:
        copy.wait_send()


def gather(*values):
    dma = pltpu.SemaphoreType.DMA
    powers = jax.ShapeDtypeStruct((N_LOCAL, PAIRS, NORB, WIDE), F32)
    scales = jax.ShapeDtypeStruct((PAIRS, N_LOCAL, WIDE), F32)
    totals = jax.ShapeDtypeStruct((N_LOCAL, NORB, WIDE), F32)
    counted = jax.ShapeDtypeStruct((N_LOCAL, WIDE), F32)
    return pl.pallas_call(
        gather_kernel,
        name="gather",
        out_shape=(totals, powers, powers, scales, scales, counted),
        in_specs=[hbm()] * 5,
        out_specs=(vmem(),) * 6,
        scratch_shapes=[
            pltpu.SMEM((KPTS,), jnp.int32),
            pltpu.SMEM((FREQ,), jnp.int32),
            pltpu.VMEM((NORB, WIDE), F32),
            pltpu.VMEM((PER_FREQ, NORB, WIDE), F32),
            pltpu.VMEM((ZS, CORES, NORB // 2, WIDE), F32),
            pltpu.VMEM((N_LOCAL, NORB + 8, WIDE), F32),
            pltpu.VMEM((PAIRS, WIDE, 2 * WIDE), BF),
            pltpu.VMEM((PAIRS, WIDE, 2 * WIDE), BF),
            pltpu.VMEM((PAIRS, NORB, WIDE), F32),
            pltpu.VMEM((PAIRS, WIDE), F32),
            pltpu.VMEM((N_LOCAL, NORB, 2 * WIDE), BF),
            pltpu.VMEM((N_LOCAL, NORB, 2 * WIDE), F32),
            pltpu.VMEM((N_LOCAL, NORB, 3 * WIDE), F32),
            pltpu.VMEM((N_LOCAL, 2 * WIDE), F32),
        ]
        + [dma((ZS,))] * 4
        + [dma((XS,))] * 4
        + [dma((5,))],
        compiler_params=pltpu.CompilerParams(
            collective_id=0, has_side_effects=True, vmem_limit_bytes=20 << 20
        ),
    )(*(pltpu.with_memory_space_constraint(value, pltpu.HBM) for value in values))


def power_kernel(
    er_ref, ei_ref, ur_ref, ui_ref, count_ref, tr_ref, ti_ref, sr_ref, si_ref, qr_ref, qi_ref, steps_ref
):
    _, first, eye_mask = lane_masks()
    eye = eye_mask.astype(F32)
    first_bf = first.astype(F32).astype(BF)
    second_bf = (1.0 - first.astype(F32)).astype(BF)

    def right_blocks(real, imag):
        def build(r, i):
            return jnp.concatenate(
                [
                    jnp.concatenate([r * first_bf, i * first_bf], 1),
                    jnp.concatenate([r * second_bf, i * second_bf], 1),
                ],
                0,
            )

        r_high, r_low = halves(real)
        i_high, i_low = halves(imag)
        return build(r_high, i_high), build(r_low, i_low)

    def left_rows(real, imag):
        return halves(jnp.concatenate([real, imag], 0))

    def combine(out):
        return out[:NORB, :WIDE] - out[NORB:, WIDE:], out[:NORB, WIDE:] + out[NORB:, :WIDE]

    def weighted(n, p, real, imag):
        u_real, u_imag = ur_ref[p, pl.ds(n, 1)], ui_ref[p, pl.ds(n, 1)]
        return real * u_real - imag * u_imag, real * u_imag + imag * u_real

    def two_steps(n):
        for p in range(PAIRS):
            e_real, e_imag = er_ref[n, p], ei_ref[n, p]
            sr_ref[p], si_ref[p] = combine(product3(left_rows(e_real, e_imag), right_blocks(e_real, e_imag)))
        total = None
        for p in range(PAIRS):
            q_real, q_imag = eye + er_ref[n, p], ei_ref[n, p]
            real, imag = combine(product3(left_rows(q_real, q_imag), right_blocks(sr_ref[p], si_ref[p])))
            real, imag = weighted(n, p, q_real + real, q_imag + imag)
            total = (real, imag) if total is None else (total[0] + real, total[1] + imag)
        tr_ref[n], ti_ref[n] = total

    def three_steps(n):
        for p in range(PAIRS):
            e_real, e_imag = er_ref[n, p], ei_ref[n, p]
            sr_ref[p], si_ref[p] = combine(product3(left_rows(e_real, e_imag), right_blocks(e_real, e_imag)))
        for p in range(PAIRS):
            e_real, e_imag = er_ref[n, p], ei_ref[n, p]
            s_real, s_imag = sr_ref[p], si_ref[p]
            right = right_blocks(s_real, s_imag)
            real, imag = combine(product3(left_rows(eye + e_real, e_imag), right))
            qr_ref[p], qi_ref[p] = eye + e_real + real, e_imag + imag
            sr_ref[p], si_ref[p] = combine(product3(left_rows(s_real, s_imag), right))
        total = None
        for p in range(PAIRS):
            q_real, q_imag = qr_ref[p], qi_ref[p]
            real, imag = combine(product3(left_rows(q_real, q_imag), right_blocks(sr_ref[p], si_ref[p])))
            real, imag = weighted(n, p, q_real + real, q_imag + imag)
            total = (real, imag) if total is None else (total[0] + real, total[1] + imag)
        tr_ref[n], ti_ref[n] = total

    for n in range(N_LOCAL):
        steps_ref[n] = jnp.max(count_ref[n : n + 1])
    tr_ref[...] = jnp.zeros_like(tr_ref)
    ti_ref[...] = jnp.zeros_like(ti_ref)

    def one_freq(n, carry):
        steps = steps_ref[n]
        pl.when((steps > 1.5) & (steps < 2.5))(functools.partial(two_steps, n))
        pl.when(steps > 2.5)(functools.partial(three_steps, n))
        return carry

    lax.fori_loop(0, N_LOCAL, one_freq, 0)


def invert(*gathered):
    slots = pltpu.VMEM((PAIRS, NORB, WIDE), F32)
    totals = jax.ShapeDtypeStruct((N_LOCAL, NORB, WIDE), F32)
    return pl.pallas_call(
        power_kernel,
        name="invert",
        out_shape=(totals, totals),
        in_specs=[vmem()] * 5,
        out_specs=(vmem(),) * 2,
        scratch_shapes=[slots] * 4 + [pltpu.SMEM((N_LOCAL,), F32)],
        compiler_params=pltpu.CompilerParams(vmem_limit_bytes=16 << 20),
    )(*gathered)


def exit_kernel(
    g_ref, er_ref, ei_ref, ur_ref, ui_ref, count_ref, tr_ref, ti_ref, q_ref, o_ref, t_ref, landed, rows_ref, as_, ar, bs, br
):
    f = lax.axis_index("freq")
    y = lax.axis_index("kgrp")
    x, t = f // LINE, f % LINE
    z, c = t // CORES, t % CORES
    plane = [(dx, dy) for dx in (2, 1, 3, 0) for dy in (2, 1, 3, 0) if dx or dy]
    plane.sort(key=lambda step: -min(step[0], XS - step[0]) - min(step[1], YS - step[1]))
    line = [(dz, dc) for dz in (4, 3, 5, 2, 6, 1, 7, 0) for dc in (1, 0) if dz or dc]

    def in_plane(dx, dy):
        return {"freq": (x + dx) % XS * LINE + t, "kgrp": (y + dy) % YS}

    def place(dz, dc):
        return (z + dz) % ZS * CORES + (c + dc) % CORES

    await_greetings = greet([q for d, e in zip(plane, line) for q in (in_plane(*d), on_freq(x * LINE + place(*e)))])
    lanes, first, eye_mask = lane_masks()
    eye = eye_mask.astype(F32)
    quarter = lanes % NORB // (NORB // YS)

    def one_step(n, carry):
        t_real = t_imag = jnp.zeros((NORB, WIDE), F32)
        for p in range(PAIRS):
            q_real, q_imag = eye + er_ref[n, p], ei_ref[n, p]
            u_real, u_imag = ur_ref[p, pl.ds(n, 1)], ui_ref[p, pl.ds(n, 1)]
            t_real = t_real + (q_real * u_real - q_imag * u_imag)
            t_imag = t_imag + (q_real * u_imag + q_imag * u_real)
        single = count_ref[pl.ds(n, 1)] < 1.5
        t_real, t_imag = jnp.where(single, t_real, tr_ref[n]), jnp.where(single, t_imag, ti_ref[n])
        t_ref[n] = jnp.where(first, t_real + swap(t_real), t_imag + swap(t_imag))
        return carry

    lax.fori_loop(0, N_LOCAL, one_step, 0)
    for n_high in range(2):
        mixed = [None] * YS
        for n_low in range(4):
            dx = (x + XS - n_high * 2 - n_low // 2) % XS
            n = (dx + dx // 2 * (5 - 2 * dx)) * PER_FREQ + n_low % 2
            g = g_ref[n]
            turned = jnp.where(first, -swap(g), swap(g))
            right = jnp.concatenate(halves(jnp.concatenate([g, turned], 0)), 1)
            both = dot(jnp.concatenate(halves(t_ref[n]), 1), jnp.concatenate([right, right], 0))
            value = both[:, :WIDE] + both[:, WIDE:]
            for to_y in range(YS):
                shift = (n_low - to_y) * (NORB // YS) % WIDE
                moved = pltpu.roll(value, shift, 1) if shift else value
                mixed[to_y] = moved if n_low == 0 else jnp.where(quarter == n_low, moved, mixed[to_y])
        for to_y in range(YS):
            for to_x in range(XS):
                o_ref[to_x, to_y, n_high] = mixed[to_y][to_x * LINE : (to_x + 1) * LINE]
    await_greetings()
    started = []
    for dx, dy in plane:
        slot = dx * YS + dy
        copy = send(
            o_ref.at[(x + dx) % XS, (y + dy) % YS], landed.at[slot], as_.at[slot], ar.at[slot], in_plane(dx, dy)
        )
        copy.start()
        started.append(copy)
    total = o_ref[x, y]
    for dx, dy in reversed(plane):
        slot = dx * YS + dy
        send(o_ref.at[x, y], landed.at[slot], as_.at[slot], ar.at[slot], in_plane(dx, dy)).wait_recv()
        total = total + landed[slot]
    for to in range(LINE):
        for n_high in range(2):
            rows_ref[to, n_high : n_high + 1] = total[n_high, to : to + 1]
    for dz, dc in line:
        slot = dz * CORES + dc
        to = place(dz, dc)
        copy = send(rows_ref.at[to], q_ref.at[t], bs.at[slot], br.at[slot], on_freq(x * LINE + to))
        copy.start()
        started.append(copy)
    q_ref[pl.ds(t, 1)] = rows_ref[pl.ds(t, 1)]
    for dz, dc in reversed(line):
        slot = dz * CORES + dc
        source = (z + ZS - dz) % ZS * CORES + (c + CORES - dc) % CORES
        send(rows_ref.at[source], q_ref.at[source], bs.at[slot], br.at[slot], on_freq(x * LINE + place(dz, dc))).wait_recv()
    for copy in started:
        copy.wait_send()


def leave(*parts):
    dma = pltpu.SemaphoreType.DMA
    return pl.pallas_call(
        exit_kernel,
        name="leave",
        out_shape=jax.ShapeDtypeStruct((LINE, 2, WIDE), F32),
        in_specs=[vmem()] * 8,
        out_specs=vmem(),
        scratch_shapes=[
            pltpu.VMEM((XS, YS, 2, LINE, WIDE), F32),
            pltpu.VMEM((N_LOCAL, NORB, WIDE), F32),
            pltpu.VMEM((XS * YS, 2, LINE, WIDE), F32),
            pltpu.VMEM((LINE, 2, WIDE), F32),
            dma((XS * YS,)),
            dma((XS * YS,)),
            dma((LINE,)),
            dma((LINE,)),
        ],
        compiler_params=pltpu.CompilerParams(
            collective_id=1, has_side_effects=True, vmem_limit_bytes=8 << 20
        ),
    )(*parts)


def per_device(hamiltonian, self_energy, guess_factor, weights, counts):
    g_all, *gathered = gather(weights, counts, hamiltonian, self_energy, guess_factor)
    arrived = leave(g_all, *gathered, *invert(*gathered))
    pieces = arrived.reshape(LINE, 2, 2, 2, 2, NORB // YS)
    return pieces.transpose(5, 2, 1, 3, 0, 4).reshape(NORB // YS, 2 * FREQ)


def solution(mesh):
    return jax.shard_map(
        per_device,
        mesh=mesh,
        in_specs=(
            P(("freq", "kgrp"), None, None),
            P("freq", None, None),
            P("freq", None, None),
            P(),
            P(),
        ),
        out_specs=P(("freq", "kgrp"), None),
        check_vma=False,
    )
```

```python
import functools
import math

import jax
import jax.numpy as jnp
from jax import lax
from jax.experimental import pallas as pl
from jax.experimental.pallas import tpu as pltpu
from jax.sharding import PartitionSpec as P

chem_potential = 0.2

NORB = 64
WIDE = 2 * NORB
XS, YS, ZS, CORES = 4, 4, 8, 2
LINE = ZS * CORES
PER_FREQ = 2
N_LOCAL = XS * PER_FREQ
PAIRS = LINE // 2
FREQ = 128
KPTS = 256
BF = jnp.bfloat16
F32 = jnp.float32


def vmem():
    return pl.BlockSpec(memory_space=pltpu.VMEM)


def smem():
    return pl.BlockSpec(memory_space=pltpu.SMEM)


def hbm():
    return pl.BlockSpec(memory_space=pltpu.HBM)


def on_freq(index):
    return {"freq": index}


def greet(targets):
    barrier = pltpu.get_barrier_semaphore()
    for target in targets:
        pl.semaphore_signal(barrier, inc=1, device_id=target, device_id_type=pl.DeviceIdType.MESH)
    return lambda: pl.semaphore_wait(barrier, len(targets))


def send(src, dst, send_sem, recv_sem, target):
    return pltpu.make_async_remote_copy(
        src_ref=src,
        dst_ref=dst,
        send_sem=send_sem,
        recv_sem=recv_sem,
        device_id=target,
        device_id_type=pl.DeviceIdType.MESH,
    )


Z_ORDER = (4, 3, 5, 2, 6, 1, 7)
SLOT_DX = (0, 1, 3, 2)


def halves(value):
    high = value.astype(BF)
    low = (value - high.astype(F32)).astype(BF)
    return high, low


def dot(left, right):
    return jnp.dot(left, right, preferred_element_type=F32)


def product3(left, right):
    left_high, left_low = left
    right_high, right_low = right
    return dot(
        jnp.concatenate([left_high, left_low], 1), jnp.concatenate([right_high, right_high], 0)
    ) + dot(left_high, right_low)


def swap(value):
    return pltpu.roll(value, NORB, 1)


def lane_masks():
    rows = lax.broadcasted_iota(jnp.int32, (NORB, WIDE), 0)
    lanes = lax.broadcasted_iota(jnp.int32, (NORB, WIDE), 1)
    return lanes, lanes < NORB, rows == lanes % NORB


def right_blocks(real, imag):
    first = lane_masks()[1].astype(F32)
    first_bf, second_bf = first.astype(BF), (1.0 - first).astype(BF)

    def build(r, i):
        return jnp.concatenate(
            [
                jnp.concatenate([r * first_bf, i * first_bf], 1),
                jnp.concatenate([r * second_bf, i * second_bf], 1),
            ],
            0,
        )

    r_high, r_low = halves(real)
    i_high, i_low = halves(imag)
    return build(r_high, i_high), build(r_low, i_low)


def left_rows(real, imag):
    return halves(jnp.concatenate([real, imag], 0))


def combine(out):
    return out[:NORB, :WIDE] - out[NORB:, WIDE:], out[:NORB, WIDE:] + out[NORB:, :WIDE]


def gather_kernel(
    w_hbm, n_hbm, h_hbm, s_hbm, g_hbm,
    gall, er_ref, ei_ref, ur_ref, ui_ref, count_ref,
    w_ref, n_ref, h_ref, s_ref, hall, zall, wh, wl, hcol, hrow, gcat, gz, zcol, zrow,
    zs, zr, ps, pr, ss, sr, gs, gr, own,
):
    f = lax.axis_index("freq")
    y = lax.axis_index("kgrp")
    x, t = f // LINE, f % LINE
    z, c = t // CORES, t % CORES
    partner = on_freq(x * LINE + z * CORES + (1 - c))
    lanes, first, eye_mask = lane_masks()
    eye = eye_mask.astype(F32)
    half = NORB // 2
    row_ids = lax.broadcasted_iota(jnp.int32, (NORB, WIDE), 0)
    below, above = row_ids > lanes % NORB, row_ids < lanes % NORB

    def along_z(dz):
        return on_freq(x * LINE + (z + dz) % ZS * CORES + c)

    def along_x(dx):
        return on_freq((x + dx) % XS * LINE + t)

    def both_parts(value):
        turned = swap(value)
        return jnp.concatenate([jnp.where(first, value, turned), jnp.where(first, turned, value)], 1)

    def as_right(real, imag):
        def build(r, i):
            return jnp.concatenate([jnp.concatenate([r, i], 1), jnp.concatenate([-i, r], 1)], 0)

        real_high, real_low = halves(real)
        imag_high, imag_low = halves(imag)
        return build(real_high, imag_high), build(real_low, imag_low)

    def diagonal_columns(value):
        kept = jnp.where(eye_mask, value, 0.0)
        left = jnp.sum(jnp.where(first, kept, 0.0), 1, keepdims=True)
        right = jnp.sum(jnp.where(first, 0.0, kept), 1, keepdims=True)
        return jnp.where(first, left, right)

    def diagonal_row(value):
        return jnp.sum(jnp.where(eye_mask, value, 0.0), 0, keepdims=True)

    def freq_of(slot, b):
        return (x + XS - SLOT_DX[slot]) % XS * (PER_FREQ * LINE) + t * PER_FREQ + b

    def share_freq(b):
        matsubara = (2 * freq_of(0, b) + 1).astype(F32) * (math.pi / (2 * FREQ))
        zed = jnp.where(eye_mask, jnp.where(first, chem_potential, matsubara), 0.0) - s_ref[b]
        turned = swap(zed)
        right = jnp.concatenate([zed, jnp.where(first, -turned, turned)], 0)
        zall[b, :NORB] = product3(halves(gall[b]), halves(right))
        zall[b, NORB:] = jnp.broadcast_to(diagonal_row(zed), (8, WIDE))

    def prepare_freqs(slot):
        for b in range(PER_FREQ):
            n = slot * PER_FREQ + b
            count_ref[n : n + 1] = jnp.full((1, WIDE), n_ref[freq_of(slot, b)].astype(F32))
            product, row = zall[n, :NORB], zall[n, NORB : NORB + 1]
            gcat[n] = jnp.concatenate(halves(gall[n]), 1)
            gz[n] = both_parts(product)
            zrow[n : n + 1] = jnp.concatenate(
                [jnp.where(first[:1], row, swap(row)), jnp.where(first[:1], swap(row), row)], 1
            )
            kept = jnp.where(eye_mask, row, 0.0)
            real = jnp.sum(jnp.where(first, kept, 0.0), 1, keepdims=True)
            imag = jnp.sum(jnp.where(first, 0.0, kept), 1, keepdims=True)
            zcol[n] = jnp.concatenate(
                [jnp.broadcast_to(part, (NORB, WIDE)) for part in (real, imag, imag * imag)], 1
            )

    def prepare_pair(p):
        one, two = hall[p, 0], hall[p, 1]
        packed = jnp.concatenate(
            [jnp.where(first[:half], one, swap(two)), jnp.where(first[:half], swap(one), two)], 0
        )
        flipped = jnp.concatenate([packed, swap(packed)], 0).T[:NORB]
        real = jnp.where(above, flipped, packed)
        imag = jnp.where(above, packed, jnp.where(below, -flipped, 0.0))
        high, low = as_right(real, imag)
        wh[p] = high
        wl[p] = low
        hcol[p] = diagonal_columns(real)
        hrow[p : p + 1] = diagonal_row(real)

    first_rows = pl.ds(0, PER_FREQ)
    own_h, own_z, own_g = hall.at[0, 0], zall.at[first_rows], gall.at[first_rows]
    loads = [
        pltpu.make_async_copy(src, dst, own.at[i])
        for i, (src, dst) in enumerate(
            ((h_hbm.at[0], h_ref), (g_hbm, own_g), (s_hbm, s_ref), (w_hbm, w_ref), (n_hbm, n_ref))
        )
    ]
    for load in loads:
        load.start()
    await_greetings = greet(
        [along_z(dz) for dz in Z_ORDER] + [along_x(dx) for dx in (2, 1, 3)] + [partner]
    )
    for load in loads:
        load.wait()
    h = h_ref[...]
    folded = jnp.where(above ^ first, h, swap(h))
    own_h[...] = jnp.where(first[:half], folded[:half], folded[half:])
    for b in range(PER_FREQ):
        share_freq(b)
    prepare_freqs(0)

    def add_up(i, total):
        for j in range(16):
            total = total + w_ref[i * 16 + j]
        return total

    inv_total = 1.0 / lax.fori_loop(0, KPTS // 16, add_up, jnp.int32(0)).astype(F32)
    await_greetings()

    def z_copy(dz):
        return send(own_h, hall.at[dz, 0], zs.at[dz], zr.at[dz], along_z(dz))

    def partner_copy(dz):
        return send(hall.at[dz, 0], hall.at[dz, 1], ps.at[dz], pr.at[dz], partner)

    def freq_copies(slot):
        rows = pl.ds(slot * PER_FREQ, PER_FREQ)
        if slot < 3:
            g_from, z_from = own_g, own_z
            g_to = z_to = along_x(SLOT_DX[slot])
        else:
            g_from, g_to = gall.at[pl.ds(1 * PER_FREQ, PER_FREQ)], along_x(1)
            z_from, z_to = zall.at[pl.ds(2 * PER_FREQ, PER_FREQ)], along_x(XS - 1)
        return (
            send(g_from, gall.at[rows], gs.at[slot], gr.at[slot], g_to),
            send(z_from, zall.at[rows], ss.at[slot], sr.at[slot], z_to),
        )

    started = []

    def begin(copy):
        copy.start()
        started.append(copy)

    begin(partner_copy(0))
    for dz in Z_ORDER:
        begin(z_copy(dz))
    begin(freq_copies(1)[0])
    begin(freq_copies(2)[1])
    begin(freq_copies(1)[1])
    begin(freq_copies(2)[0])

    def residuals(p, low, high):
        left = gcat[low:high].reshape((high - low) * NORB, 2 * WIDE)
        right = wh[p]
        gh = dot(left, jnp.concatenate([right, right], 0)) + dot(left[:, :WIDE], wl[p])
        h_diag = hcol[p]
        chip = x * LINE + (z + ZS - p) % ZS * CORES
        w_one = w_ref[(chip + c) * YS + y].astype(F32) * inv_total
        w_two = w_ref[(chip + 1 - c) * YS + y].astype(F32) * inv_total
        weight = jnp.where(first[: high - low], w_one, w_two)
        d_real, d_imag = zrow[low:high, :WIDE] - hrow[pl.ds(p, 1)], zrow[low:high, WIDE:]
        inv = weight / (d_real * d_real + d_imag * d_imag)
        ur_ref[p, low:high] = d_real * inv
        ui_ref[p, low:high] = -d_imag * inv
        for n in range(low, high):
            a = gz[n] - gh[(n - low) * NORB : (n - low + 1) * NORB]
            a_real, a_imag = a[:, :WIDE], a[:, WIDE:]
            d = zcol[n]
            d_real, d_imag = d[:, :WIDE] - h_diag, d[:, WIDE : 2 * WIDE]
            inv = 1.0 / (d_real * d_real + d[:, 2 * WIDE :])
            v_real, v_imag = d_real * inv, d_imag * inv
            e_real = eye - (v_real * a_real + v_imag * a_imag)
            e_imag = v_imag * a_real - v_real * a_imag
            er_ref[n, p] = e_real
            ei_ref[n, p] = e_imag

    def arrived_z(*steps):
        for dz in steps:
            z_copy(dz).wait_recv()
            begin(partner_copy(dz))

    def arrived_pair(*steps):
        for dz in steps:
            partner_copy(dz).wait_recv()
        for dz in steps:
            prepare_pair(dz)
        for dz in steps:
            residuals(dz, 0, PER_FREQ)

    near_g, near_z = freq_copies(1), freq_copies(2)
    far = freq_copies(3)
    arrived_pair(0)
    arrived_z(1, 7)
    near_g[0].wait_recv()
    begin(far[0])
    near_z[1].wait_recv()
    begin(far[1])
    arrived_z(2, 6)
    arrived_pair(1, 7)
    near_g[1].wait_recv()
    near_z[0].wait_recv()
    prepare_freqs(1)
    prepare_freqs(2)
    arrived_z(3, 5)

    def near_freqs(*pairs):
        for p in pairs:
            residuals(p, PER_FREQ, 3 * PER_FREQ)

    near_freqs(0, 1, 7)
    arrived_z(4)
    arrived_pair(2, 6)
    near_freqs(2, 6)
    arrived_pair(3, 5)
    near_freqs(3, 5)
    for copy in far:
        copy.wait_recv()
    prepare_freqs(3)

    for p in (0, 1, 7, 2, 6, 3, 5):
        residuals(p, 3 * PER_FREQ, N_LOCAL)
    partner_copy(4).wait_recv()
    prepare_pair(4)
    residuals(4, 0, N_LOCAL)
    for copy in started:
        copy.wait_send()


def gather(*values):
    dma = pltpu.SemaphoreType.DMA
    powers = jax.ShapeDtypeStruct((N_LOCAL, PAIRS, NORB, WIDE), F32)
    scales = jax.ShapeDtypeStruct((PAIRS, N_LOCAL, WIDE), F32)
    totals = jax.ShapeDtypeStruct((N_LOCAL, NORB, WIDE), F32)
    counted = jax.ShapeDtypeStruct((N_LOCAL, WIDE), F32)
    return pl.pallas_call(
        gather_kernel,
        name="gather",
        out_shape=(totals, powers, powers, scales, scales, counted),
        in_specs=[hbm()] * 5,
        out_specs=(vmem(),) * 6,
        scratch_shapes=[
            pltpu.SMEM((KPTS,), jnp.int32),
            pltpu.SMEM((FREQ,), jnp.int32),
            pltpu.VMEM((NORB, WIDE), F32),
            pltpu.VMEM((PER_FREQ, NORB, WIDE), F32),
            pltpu.VMEM((ZS, CORES, NORB // 2, WIDE), F32),
            pltpu.VMEM((N_LOCAL, NORB + 8, WIDE), F32),
            pltpu.VMEM((PAIRS, WIDE, 2 * WIDE), BF),
            pltpu.VMEM((PAIRS, WIDE, 2 * WIDE), BF),
            pltpu.VMEM((PAIRS, NORB, WIDE), F32),
            pltpu.VMEM((PAIRS, WIDE), F32),
            pltpu.VMEM((N_LOCAL, NORB, 2 * WIDE), BF),
            pltpu.VMEM((N_LOCAL, NORB, 2 * WIDE), F32),
            pltpu.VMEM((N_LOCAL, NORB, 3 * WIDE), F32),
            pltpu.VMEM((N_LOCAL, 2 * WIDE), F32),
        ]
        + [dma((ZS,))] * 4
        + [dma((XS,))] * 4
        + [dma((5,))],
        compiler_params=pltpu.CompilerParams(
            collective_id=0, has_side_effects=True, vmem_limit_bytes=20 << 20
        ),
    )(*(pltpu.with_memory_space_constraint(value, pltpu.HBM) for value in values))


def power_kernel(e_in_real, e_in_imag, count_ref, er_ref, ei_ref, br_ref, bi_ref, sr_ref, si_ref, steps_ref):
    eye = lane_masks()[2].astype(F32)

    def one_step(n):
        for p in range(PAIRS):
            br_ref[n, p] = bi_ref[n, p] = jnp.zeros((NORB, WIDE), F32)

    def squares(n, real_ref, imag_ref):
        for p in range(PAIRS):
            e_real, e_imag = er_ref[n, p], ei_ref[n, p]
            real_ref[p], imag_ref[p] = combine(product3(left_rows(e_real, e_imag), right_blocks(e_real, e_imag)))

    def two_steps(n):
        squares(n, br_ref.at[n], bi_ref.at[n])

    def three_steps(n):
        squares(n, sr_ref, si_ref)
        for p in range(PAIRS):
            e_real, e_imag = er_ref[n, p], ei_ref[n, p]
            s_real, s_imag = sr_ref[p], si_ref[p]
            right = right_blocks(s_real, s_imag)
            real, imag = combine(product3(left_rows(eye + e_real, e_imag), right))
            er_ref[n, p], ei_ref[n, p] = e_real + real, e_imag + imag
            br_ref[n, p], bi_ref[n, p] = combine(product3(left_rows(s_real, s_imag), right))

    for n in range(N_LOCAL):
        steps_ref[n] = jnp.max(count_ref[n : n + 1])

    def one_freq(n, carry):
        steps = steps_ref[n]
        pl.when(steps < 1.5)(functools.partial(one_step, n))
        pl.when((steps > 1.5) & (steps < 2.5))(functools.partial(two_steps, n))
        pl.when(steps > 2.5)(functools.partial(three_steps, n))
        return carry

    lax.fori_loop(0, N_LOCAL, one_freq, 0)


def invert(*residuals_and_counts):
    slots = pltpu.VMEM((PAIRS, NORB, WIDE), F32)
    powers = jax.ShapeDtypeStruct((N_LOCAL, PAIRS, NORB, WIDE), F32)
    return pl.pallas_call(
        power_kernel,
        name="invert",
        out_shape=(powers,) * 4,
        in_specs=[vmem()] * 3,
        out_specs=(vmem(),) * 4,
        input_output_aliases={0: 0, 1: 1},
        scratch_shapes=[slots] * 2 + [pltpu.SMEM((N_LOCAL,), F32)],
        compiler_params=pltpu.CompilerParams(vmem_limit_bytes=24 << 20),
    )(*residuals_and_counts)


def exit_kernel(
    g_ref, ur_ref, ui_ref, er_ref, ei_ref, br_ref, bi_ref, q_ref, o_ref, t_ref, landed, rows_ref, as_, ar, bs, br
):
    f = lax.axis_index("freq")
    y = lax.axis_index("kgrp")
    x, t = f // LINE, f % LINE
    z, c = t // CORES, t % CORES
    plane = [(dx, dy) for dx in (2, 1, 3, 0) for dy in (2, 1, 3, 0) if dx or dy]
    plane.sort(key=lambda step: -min(step[0], XS - step[0]) - min(step[1], YS - step[1]))
    line = [(dz, dc) for dz in (4, 3, 5, 2, 6, 1, 7, 0) for dc in (1, 0) if dz or dc]

    def in_plane(dx, dy):
        return {"freq": (x + dx) % XS * LINE + t, "kgrp": (y + dy) % YS}

    def place(dz, dc):
        return (z + dz) % ZS * CORES + (c + dc) % CORES

    await_greetings = greet([q for d, e in zip(plane, line) for q in (in_plane(*d), on_freq(x * LINE + place(*e)))])
    lanes, first, eye_mask = lane_masks()
    eye = eye_mask.astype(F32)
    quarter = lanes % NORB // (NORB // YS)

    def last_product(n, carry):
        t_real = t_imag = jnp.zeros((NORB, WIDE), F32)
        for p in range(PAIRS):
            q_real, q_imag = eye + er_ref[n, p], ei_ref[n, p]
            right = right_blocks(br_ref[n, p], bi_ref[n, p])
            real, imag = combine(product3(left_rows(q_real, q_imag), right))
            q_real, q_imag = q_real + real, q_imag + imag
            u_real, u_imag = ur_ref[p, pl.ds(n, 1)], ui_ref[p, pl.ds(n, 1)]
            t_real = t_real + (q_real * u_real - q_imag * u_imag)
            t_imag = t_imag + (q_real * u_imag + q_imag * u_real)
        t_ref[n] = jnp.where(first, t_real + swap(t_real), t_imag + swap(t_imag))
        return carry

    lax.fori_loop(0, N_LOCAL, last_product, 0, unroll=2)
    for n_high in range(2):
        mixed = [None] * YS
        for n_low in range(4):
            dx = (x + XS - n_high * 2 - n_low // 2) % XS
            n = (dx + dx // 2 * (5 - 2 * dx)) * PER_FREQ + n_low % 2
            g = g_ref[n]
            turned = jnp.where(first, -swap(g), swap(g))
            right = jnp.concatenate(halves(jnp.concatenate([g, turned], 0)), 1)
            both = dot(jnp.concatenate(halves(t_ref[n]), 1), jnp.concatenate([right, right], 0))
            value = both[:, :WIDE] + both[:, WIDE:]
            for to_y in range(YS):
                shift = (n_low - to_y) * (NORB // YS) % WIDE
                moved = pltpu.roll(value, shift, 1) if shift else value
                mixed[to_y] = moved if n_low == 0 else jnp.where(quarter == n_low, moved, mixed[to_y])
        for to_y in range(YS):
            for to_x in range(XS):
                o_ref[to_x, to_y, n_high] = mixed[to_y][to_x * LINE : (to_x + 1) * LINE]
    await_greetings()
    started = []
    for dx, dy in plane:
        slot = dx * YS + dy
        copy = send(
            o_ref.at[(x + dx) % XS, (y + dy) % YS], landed.at[slot], as_.at[slot], ar.at[slot], in_plane(dx, dy)
        )
        copy.start()
        started.append(copy)
    total = o_ref[x, y]
    for dx, dy in reversed(plane):
        slot = dx * YS + dy
        send(o_ref.at[x, y], landed.at[slot], as_.at[slot], ar.at[slot], in_plane(dx, dy)).wait_recv()
        total = total + landed[slot]
    for to in range(LINE):
        for n_high in range(2):
            rows_ref[to, n_high : n_high + 1] = total[n_high, to : to + 1]
    for dz, dc in line:
        slot = dz * CORES + dc
        to = place(dz, dc)
        copy = send(rows_ref.at[to], q_ref.at[t], bs.at[slot], br.at[slot], on_freq(x * LINE + to))
        copy.start()
        started.append(copy)
    q_ref[pl.ds(t, 1)] = rows_ref[pl.ds(t, 1)]
    for dz, dc in reversed(line):
        slot = dz * CORES + dc
        source = (z + ZS - dz) % ZS * CORES + (c + CORES - dc) % CORES
        send(rows_ref.at[source], q_ref.at[source], bs.at[slot], br.at[slot], on_freq(x * LINE + place(dz, dc))).wait_recv()
    for copy in started:
        copy.wait_send()


def leave(*parts):
    dma = pltpu.SemaphoreType.DMA
    return pl.pallas_call(
        exit_kernel,
        name="leave",
        out_shape=jax.ShapeDtypeStruct((LINE, 2, WIDE), F32),
        in_specs=[vmem()] * 7,
        out_specs=vmem(),
        scratch_shapes=[
            pltpu.VMEM((XS, YS, 2, LINE, WIDE), F32),
            pltpu.VMEM((N_LOCAL, NORB, WIDE), F32),
            pltpu.VMEM((XS * YS, 2, LINE, WIDE), F32),
            pltpu.VMEM((LINE, 2, WIDE), F32),
            dma((XS * YS,)),
            dma((XS * YS,)),
            dma((LINE,)),
            dma((LINE,)),
        ],
        compiler_params=pltpu.CompilerParams(
            collective_id=1, has_side_effects=True, vmem_limit_bytes=16 << 20
        ),
    )(*parts)


def per_device(hamiltonian, self_energy, guess_factor, weights, counts):
    g_all, e_real, e_imag, u_real, u_imag, steps = gather(
        weights, counts, hamiltonian, self_energy, guess_factor
    )
    arrived = leave(g_all, u_real, u_imag, *invert(e_real, e_imag, steps))
    pieces = arrived.reshape(LINE, 2, 2, 2, 2, NORB // YS)
    return pieces.transpose(5, 2, 1, 3, 0, 4).reshape(NORB // YS, 2 * FREQ)


def solution(mesh):
    return jax.shard_map(
        per_device,
        mesh=mesh,
        in_specs=(
            P(("freq", "kgrp"), None, None),
            P("freq", None, None),
            P("freq", None, None),
            P(),
            P(),
        ),
        out_specs=P(("freq", "kgrp"), None),
        check_vma=False,
    )
```

```python
import functools
import math

import jax
import jax.numpy as jnp
from jax import lax
from jax.experimental import pallas as pl
from jax.experimental.pallas import tpu as pltpu
from jax.sharding import PartitionSpec as P

chem_potential = 0.2

NORB = 64
WIDE = 2 * NORB
XS, YS, ZS, CORES = 4, 4, 8, 2
LINE = ZS * CORES
PER_FREQ = 2
N_LOCAL = XS * PER_FREQ
PAIRS = LINE // 2
FREQ = 128
KPTS = 256
BF = jnp.bfloat16
F32 = jnp.float32


def vmem():
    return pl.BlockSpec(memory_space=pltpu.VMEM)


def smem():
    return pl.BlockSpec(memory_space=pltpu.SMEM)


def hbm():
    return pl.BlockSpec(memory_space=pltpu.HBM)


def on_freq(index):
    return {"freq": index}


def greet(targets):
    barrier = pltpu.get_barrier_semaphore()
    for target in targets:
        pl.semaphore_signal(barrier, inc=1, device_id=target, device_id_type=pl.DeviceIdType.MESH)
    return lambda: pl.semaphore_wait(barrier, len(targets))


def send(src, dst, send_sem, recv_sem, target):
    return pltpu.make_async_remote_copy(
        src_ref=src,
        dst_ref=dst,
        send_sem=send_sem,
        recv_sem=recv_sem,
        device_id=target,
        device_id_type=pl.DeviceIdType.MESH,
    )


Z_ORDER = (4, 3, 5, 2, 6, 1, 7)
SLOT_DX = (0, 1, 3, 2)


def halves(value):
    high = value.astype(BF)
    low = (value - high.astype(F32)).astype(BF)
    return high, low


def dot(left, right):
    return jnp.dot(left, right, preferred_element_type=F32)


def product3(left, right):
    left_high, left_low = left
    right_high, right_low = right
    return dot(
        jnp.concatenate([left_high, left_low], 1), jnp.concatenate([right_high, right_high], 0)
    ) + dot(left_high, right_low)


def swap(value):
    return pltpu.roll(value, NORB, 1)


def lane_masks():
    rows = lax.broadcasted_iota(jnp.int32, (NORB, WIDE), 0)
    lanes = lax.broadcasted_iota(jnp.int32, (NORB, WIDE), 1)
    return lanes, lanes < NORB, rows == lanes % NORB


def right_blocks(real, imag):
    first = lane_masks()[1].astype(F32)
    first_bf, second_bf = first.astype(BF), (1.0 - first).astype(BF)

    def build(r, i):
        return jnp.concatenate(
            [
                jnp.concatenate([r * first_bf, i * first_bf], 1),
                jnp.concatenate([r * second_bf, i * second_bf], 1),
            ],
            0,
        )

    r_high, r_low = halves(real)
    i_high, i_low = halves(imag)
    return build(r_high, i_high), build(r_low, i_low)


def left_rows(real, imag):
    return halves(jnp.concatenate([real, imag], 0))


def combine(out):
    return out[:NORB, :WIDE] - out[NORB:, WIDE:], out[:NORB, WIDE:] + out[NORB:, :WIDE]


def gather_kernel(
    w_hbm, n_hbm, h_hbm, s_hbm, g_hbm,
    gall, er_ref, ei_ref, ur_ref, ui_ref, count_ref,
    w_ref, n_ref, h_ref, s_ref, hall, zall, wh, wl, hcol, hrow, gcat, gz, zcol, zrow,
    zs, zr, ps, pr, ss, sr, gs, gr, own,
):
    f = lax.axis_index("freq")
    y = lax.axis_index("kgrp")
    x, t = f // LINE, f % LINE
    z, c = t // CORES, t % CORES
    partner = on_freq(x * LINE + z * CORES + (1 - c))
    lanes, first, eye_mask = lane_masks()
    eye = eye_mask.astype(F32)
    half = NORB // 2
    row_ids = lax.broadcasted_iota(jnp.int32, (NORB, WIDE), 0)
    below, above = row_ids > lanes % NORB, row_ids < lanes % NORB

    def along_z(dz):
        return on_freq(x * LINE + (z + dz) % ZS * CORES + c)

    def along_x(dx):
        return on_freq((x + dx) % XS * LINE + t)

    def both_parts(value):
        turned = swap(value)
        return jnp.concatenate([jnp.where(first, value, turned), jnp.where(first, turned, value)], 1)

    def as_right(real, imag):
        def build(r, i):
            return jnp.concatenate([jnp.concatenate([r, i], 1), jnp.concatenate([-i, r], 1)], 0)

        real_high, real_low = halves(real)
        imag_high, imag_low = halves(imag)
        return build(real_high, imag_high), build(real_low, imag_low)

    def diagonal_columns(value):
        kept = jnp.where(eye_mask, value, 0.0)
        left = jnp.sum(jnp.where(first, kept, 0.0), 1, keepdims=True)
        right = jnp.sum(jnp.where(first, 0.0, kept), 1, keepdims=True)
        return jnp.where(first, left, right)

    def diagonal_row(value):
        return jnp.sum(jnp.where(eye_mask, value, 0.0), 0, keepdims=True)

    def freq_of(slot, b):
        return (x + XS - SLOT_DX[slot]) % XS * (PER_FREQ * LINE) + t * PER_FREQ + b

    def share_freq(b):
        matsubara = (2 * freq_of(0, b) + 1).astype(F32) * (math.pi / (2 * FREQ))
        zed = jnp.where(eye_mask, jnp.where(first, chem_potential, matsubara), 0.0) - s_ref[b]
        turned = swap(zed)
        right = jnp.concatenate([zed, jnp.where(first, -turned, turned)], 0)
        zall[b, :NORB] = product3(halves(gall[b]), halves(right))
        zall[b, NORB:] = jnp.broadcast_to(diagonal_row(zed), (8, WIDE))

    def prepare_freqs(slot):
        for b in range(PER_FREQ):
            n = slot * PER_FREQ + b
            count_ref[n : n + 1] = jnp.full((1, WIDE), n_ref[freq_of(slot, b)].astype(F32))
            product, row = zall[n, :NORB], zall[n, NORB : NORB + 1]
            gcat[n] = jnp.concatenate(halves(gall[n]), 1)
            gz[n] = both_parts(product)
            zrow[n : n + 1] = jnp.concatenate(
                [jnp.where(first[:1], row, swap(row)), jnp.where(first[:1], swap(row), row)], 1
            )
            kept = jnp.where(eye_mask, row, 0.0)
            real = jnp.sum(jnp.where(first, kept, 0.0), 1, keepdims=True)
            imag = jnp.sum(jnp.where(first, 0.0, kept), 1, keepdims=True)
            zcol[n] = jnp.concatenate(
                [jnp.broadcast_to(part, (NORB, WIDE)) for part in (real, imag, imag * imag)], 1
            )

    def prepare_pair(p):
        one, two = hall[p, 0], hall[p, 1]
        packed = jnp.concatenate(
            [jnp.where(first[:half], one, swap(two)), jnp.where(first[:half], swap(one), two)], 0
        )
        flipped = jnp.concatenate([packed, swap(packed)], 0).T[:NORB]
        real = jnp.where(above, flipped, packed)
        imag = jnp.where(above, packed, jnp.where(below, -flipped, 0.0))
        high, low = as_right(real, imag)
        wh[p] = high
        wl[p] = low
        hcol[p] = diagonal_columns(real)
        hrow[p : p + 1] = diagonal_row(real)

    first_rows = pl.ds(0, PER_FREQ)
    own_h, own_z, own_g = hall.at[0, 0], zall.at[first_rows], gall.at[first_rows]
    loads = [
        pltpu.make_async_copy(src, dst, own.at[i])
        for i, (src, dst) in enumerate(
            ((h_hbm.at[0], h_ref), (g_hbm, own_g), (s_hbm, s_ref), (w_hbm, w_ref), (n_hbm, n_ref))
        )
    ]
    for load in loads:
        load.start()
    await_greetings = greet(
        [along_z(dz) for dz in Z_ORDER] + [along_x(dx) for dx in (2, 1, 3)] + [partner]
    )
    for load in loads:
        load.wait()
    h = h_ref[...]
    folded = jnp.where(above ^ first, h, swap(h))
    own_h[...] = jnp.where(first[:half], folded[:half], folded[half:])
    for b in range(PER_FREQ):
        share_freq(b)
    prepare_freqs(0)

    def add_up(i, total):
        for j in range(16):
            total = total + w_ref[i * 16 + j]
        return total

    inv_total = 1.0 / lax.fori_loop(0, KPTS // 16, add_up, jnp.int32(0)).astype(F32)
    await_greetings()

    def z_copy(dz):
        return send(own_h, hall.at[dz, 0], zs.at[dz], zr.at[dz], along_z(dz))

    def partner_copy(dz):
        return send(hall.at[dz, 0], hall.at[dz, 1], ps.at[dz], pr.at[dz], partner)

    def freq_copies(slot):
        rows = pl.ds(slot * PER_FREQ, PER_FREQ)
        if slot < 3:
            g_from, z_from = own_g, own_z
            g_to = z_to = along_x(SLOT_DX[slot])
        else:
            g_from, g_to = gall.at[pl.ds(1 * PER_FREQ, PER_FREQ)], along_x(1)
            z_from, z_to = zall.at[pl.ds(2 * PER_FREQ, PER_FREQ)], along_x(XS - 1)
        return (
            send(g_from, gall.at[rows], gs.at[slot], gr.at[slot], g_to),
            send(z_from, zall.at[rows], ss.at[slot], sr.at[slot], z_to),
        )

    started = []

    def begin(copy):
        copy.start()
        started.append(copy)

    begin(partner_copy(0))
    for dz in Z_ORDER:
        begin(z_copy(dz))
    begin(freq_copies(1)[0])
    begin(freq_copies(2)[1])
    begin(freq_copies(1)[1])
    begin(freq_copies(2)[0])

    def residuals(p, low, high):
        left = gcat[low:high].reshape((high - low) * NORB, 2 * WIDE)
        right = wh[p]
        gh = dot(left, jnp.concatenate([right, right], 0)) + dot(left[:, :WIDE], wl[p])
        h_diag = hcol[p]
        chip = x * LINE + (z + ZS - p) % ZS * CORES
        w_one = w_ref[(chip + c) * YS + y].astype(F32) * inv_total
        w_two = w_ref[(chip + 1 - c) * YS + y].astype(F32) * inv_total
        weight = jnp.where(first[: high - low], w_one, w_two)
        d_real, d_imag = zrow[low:high, :WIDE] - hrow[pl.ds(p, 1)], zrow[low:high, WIDE:]
        inv = weight / (d_real * d_real + d_imag * d_imag)
        ur_ref[p, low:high] = d_real * inv
        ui_ref[p, low:high] = -d_imag * inv
        for n in range(low, high):
            a = gz[n] - gh[(n - low) * NORB : (n - low + 1) * NORB]
            a_real, a_imag = a[:, :WIDE], a[:, WIDE:]
            d = zcol[n]
            d_real, d_imag = d[:, :WIDE] - h_diag, d[:, WIDE : 2 * WIDE]
            inv = 1.0 / (d_real * d_real + d[:, 2 * WIDE :])
            v_real, v_imag = d_real * inv, d_imag * inv
            e_real = eye - (v_real * a_real + v_imag * a_imag)
            e_imag = v_imag * a_real - v_real * a_imag
            er_ref[n, p] = e_real
            ei_ref[n, p] = e_imag

    def arrived_z(*steps):
        for dz in steps:
            z_copy(dz).wait_recv()
            begin(partner_copy(dz))

    def await_pairs(*steps):
        for dz in steps:
            partner_copy(dz).wait_recv()

    def all_residuals(pairs, low, high):
        for p in pairs:
            residuals(p, low, high)

    def prepare_pairs(*pairs):
        for p in pairs:
            prepare_pair(p)

    near_g, near_z = freq_copies(1), freq_copies(2)
    far = freq_copies(3)
    await_pairs(0)
    prepare_pairs(0)
    all_residuals((0,), 0, 2)
    arrived_z(1, 7)
    near_g[0].wait_recv()
    begin(far[0])
    near_z[1].wait_recv()
    begin(far[1])
    arrived_z(2, 6)
    await_pairs(1, 7)
    prepare_pairs(1, 7)
    all_residuals((1, 7), 0, 2)
    near_g[1].wait_recv()
    near_z[0].wait_recv()
    arrived_z(3, 5)
    await_pairs(2, 6)
    prepare_freqs(1)
    prepare_freqs(2)
    prepare_pairs(2, 6)
    all_residuals((0, 1, 7), 2, 6)
    arrived_z(4)
    await_pairs(3, 5)
    prepare_pairs(3, 5)
    all_residuals((2, 6, 3, 5), 0, 6)
    for copy in far:
        copy.wait_recv()
    await_pairs(4)
    prepare_freqs(3)
    prepare_pairs(4)
    all_residuals((4,), 0, 6)
    all_residuals((0, 1, 7, 2, 6, 3, 5, 4), 6, 8)
    for copy in started:
        copy.wait_send()


def gather(*values):
    dma = pltpu.SemaphoreType.DMA
    powers = jax.ShapeDtypeStruct((N_LOCAL, PAIRS, NORB, WIDE), F32)
    scales = jax.ShapeDtypeStruct((PAIRS, N_LOCAL, WIDE), F32)
    totals = jax.ShapeDtypeStruct((N_LOCAL, NORB, WIDE), F32)
    counted = jax.ShapeDtypeStruct((N_LOCAL, WIDE), F32)
    return pl.pallas_call(
        gather_kernel,
        name="gather",
        out_shape=(totals, powers, powers, scales, scales, counted),
        in_specs=[hbm()] * 5,
        out_specs=(vmem(),) * 6,
        scratch_shapes=[
            pltpu.SMEM((KPTS,), jnp.int32),
            pltpu.SMEM((FREQ,), jnp.int32),
            pltpu.VMEM((NORB, WIDE), F32),
            pltpu.VMEM((PER_FREQ, NORB, WIDE), F32),
            pltpu.VMEM((ZS, CORES, NORB // 2, WIDE), F32),
            pltpu.VMEM((N_LOCAL, NORB + 8, WIDE), F32),
            pltpu.VMEM((PAIRS, WIDE, 2 * WIDE), BF),
            pltpu.VMEM((PAIRS, WIDE, 2 * WIDE), BF),
            pltpu.VMEM((PAIRS, NORB, WIDE), F32),
            pltpu.VMEM((PAIRS, WIDE), F32),
            pltpu.VMEM((N_LOCAL, NORB, 2 * WIDE), BF),
            pltpu.VMEM((N_LOCAL, NORB, 2 * WIDE), F32),
            pltpu.VMEM((N_LOCAL, NORB, 3 * WIDE), F32),
            pltpu.VMEM((N_LOCAL, 2 * WIDE), F32),
        ]
        + [dma((ZS,))] * 4
        + [dma((XS,))] * 4
        + [dma((5,))],
        compiler_params=pltpu.CompilerParams(
            collective_id=0, has_side_effects=True, vmem_limit_bytes=20 << 20
        ),
    )(*(pltpu.with_memory_space_constraint(value, pltpu.HBM) for value in values))


def power_kernel(e_in_real, e_in_imag, count_ref, er_ref, ei_ref, br_ref, bi_ref, sr_ref, si_ref, steps_ref):
    eye = lane_masks()[2].astype(F32)

    def one_step(n):
        for p in range(PAIRS):
            br_ref[n, p] = bi_ref[n, p] = jnp.zeros((NORB, WIDE), F32)

    def squares(n, real_ref, imag_ref):
        for p in range(PAIRS):
            e_real, e_imag = er_ref[n, p], ei_ref[n, p]
            real_ref[p], imag_ref[p] = combine(product3(left_rows(e_real, e_imag), right_blocks(e_real, e_imag)))

    def two_steps(n):
        squares(n, br_ref.at[n], bi_ref.at[n])

    def three_steps(n):
        squares(n, sr_ref, si_ref)
        for p in range(PAIRS):
            e_real, e_imag = er_ref[n, p], ei_ref[n, p]
            s_real, s_imag = sr_ref[p], si_ref[p]
            right = right_blocks(s_real, s_imag)
            real, imag = combine(product3(left_rows(eye + e_real, e_imag), right))
            er_ref[n, p], ei_ref[n, p] = e_real + real, e_imag + imag
            br_ref[n, p], bi_ref[n, p] = combine(product3(left_rows(s_real, s_imag), right))

    for n in range(N_LOCAL):
        steps_ref[n] = jnp.max(count_ref[n : n + 1])

    def one_freq(n, carry):
        steps = steps_ref[n]
        pl.when(steps < 1.5)(functools.partial(one_step, n))
        pl.when((steps > 1.5) & (steps < 2.5))(functools.partial(two_steps, n))
        pl.when(steps > 2.5)(functools.partial(three_steps, n))
        return carry

    lax.fori_loop(0, N_LOCAL, one_freq, 0)


def invert(*residuals_and_counts):
    slots = pltpu.VMEM((PAIRS, NORB, WIDE), F32)
    powers = jax.ShapeDtypeStruct((N_LOCAL, PAIRS, NORB, WIDE), F32)
    return pl.pallas_call(
        power_kernel,
        name="invert",
        out_shape=(powers,) * 4,
        in_specs=[vmem()] * 3,
        out_specs=(vmem(),) * 4,
        input_output_aliases={0: 0, 1: 1},
        scratch_shapes=[slots] * 2 + [pltpu.SMEM((N_LOCAL,), F32)],
        compiler_params=pltpu.CompilerParams(vmem_limit_bytes=24 << 20),
    )(*residuals_and_counts)


def exit_kernel(
    g_ref, ur_ref, ui_ref, er_ref, ei_ref, br_ref, bi_ref, q_ref, o_ref, t_ref, landed, rows_ref, as_, ar, bs, br
):
    f = lax.axis_index("freq")
    y = lax.axis_index("kgrp")
    x, t = f // LINE, f % LINE
    z, c = t // CORES, t % CORES
    plane = [(dx, dy) for dx in (2, 1, 3, 0) for dy in (2, 1, 3, 0) if dx or dy]
    plane.sort(key=lambda step: -min(step[0], XS - step[0]) - min(step[1], YS - step[1]))
    line = [(dz, dc) for dz in (4, 3, 5, 2, 6, 1, 7, 0) for dc in (1, 0) if dz or dc]

    def in_plane(dx, dy):
        return {"freq": (x + dx) % XS * LINE + t, "kgrp": (y + dy) % YS}

    def place(dz, dc):
        return (z + dz) % ZS * CORES + (c + dc) % CORES

    await_greetings = greet([q for d, e in zip(plane, line) for q in (in_plane(*d), on_freq(x * LINE + place(*e)))])
    lanes, first, eye_mask = lane_masks()
    eye = eye_mask.astype(F32)
    quarter = lanes % NORB // (NORB // YS)

    def last_product(n, carry):
        t_real = t_imag = jnp.zeros((NORB, WIDE), F32)
        for p in range(PAIRS):
            q_real, q_imag = eye + er_ref[n, p], ei_ref[n, p]
            right = right_blocks(br_ref[n, p], bi_ref[n, p])
            real, imag = combine(product3(left_rows(q_real, q_imag), right))
            q_real, q_imag = q_real + real, q_imag + imag
            u_real, u_imag = ur_ref[p, pl.ds(n, 1)], ui_ref[p, pl.ds(n, 1)]
            t_real = t_real + (q_real * u_real - q_imag * u_imag)
            t_imag = t_imag + (q_real * u_imag + q_imag * u_real)
        t_ref[n] = jnp.where(first, t_real + swap(t_real), t_imag + swap(t_imag))
        return carry

    lax.fori_loop(0, N_LOCAL, last_product, 0, unroll=4)
    for n_high in range(2):
        mixed = [None] * YS
        for n_low in range(4):
            dx = (x + XS - n_high * 2 - n_low // 2) % XS
            n = (dx + dx // 2 * (5 - 2 * dx)) * PER_FREQ + n_low % 2
            g = g_ref[n]
            turned = jnp.where(first, -swap(g), swap(g))
            right = jnp.concatenate(halves(jnp.concatenate([g, turned], 0)), 1)
            both = dot(jnp.concatenate(halves(t_ref[n]), 1), jnp.concatenate([right, right], 0))
            value = both[:, :WIDE] + both[:, WIDE:]
            for to_y in range(YS):
                shift = (n_low - to_y) * (NORB // YS) % WIDE
                moved = pltpu.roll(value, shift, 1) if shift else value
                mixed[to_y] = moved if n_low == 0 else jnp.where(quarter == n_low, moved, mixed[to_y])
        for to_y in range(YS):
            for to_x in range(XS):
                o_ref[to_x, to_y, n_high] = mixed[to_y][to_x * LINE : (to_x + 1) * LINE]
    await_greetings()
    started = []
    for dx, dy in plane:
        slot = dx * YS + dy
        copy = send(
            o_ref.at[(x + dx) % XS, (y + dy) % YS], landed.at[slot], as_.at[slot], ar.at[slot], in_plane(dx, dy)
        )
        copy.start()
        started.append(copy)
    total = o_ref[x, y]
    for dx, dy in reversed(plane):
        slot = dx * YS + dy
        send(o_ref.at[x, y], landed.at[slot], as_.at[slot], ar.at[slot], in_plane(dx, dy)).wait_recv()
        total = total + landed[slot]
    for to in range(LINE):
        for n_high in range(2):
            rows_ref[to, n_high : n_high + 1] = total[n_high, to : to + 1]
    for dz, dc in line:
        slot = dz * CORES + dc
        to = place(dz, dc)
        copy = send(rows_ref.at[to], q_ref.at[t], bs.at[slot], br.at[slot], on_freq(x * LINE + to))
        copy.start()
        started.append(copy)
    q_ref[pl.ds(t, 1)] = rows_ref[pl.ds(t, 1)]
    for dz, dc in reversed(line):
        slot = dz * CORES + dc
        source = (z + ZS - dz) % ZS * CORES + (c + CORES - dc) % CORES
        send(rows_ref.at[source], q_ref.at[source], bs.at[slot], br.at[slot], on_freq(x * LINE + place(dz, dc))).wait_recv()
    for copy in started:
        copy.wait_send()


def leave(*parts):
    dma = pltpu.SemaphoreType.DMA
    return pl.pallas_call(
        exit_kernel,
        name="leave",
        out_shape=jax.ShapeDtypeStruct((LINE, 2, WIDE), F32),
        in_specs=[vmem()] * 7,
        out_specs=vmem(),
        scratch_shapes=[
            pltpu.VMEM((XS, YS, 2, LINE, WIDE), F32),
            pltpu.VMEM((N_LOCAL, NORB, WIDE), F32),
            pltpu.VMEM((XS * YS, 2, LINE, WIDE), F32),
            pltpu.VMEM((LINE, 2, WIDE), F32),
            dma((XS * YS,)),
            dma((XS * YS,)),
            dma((LINE,)),
            dma((LINE,)),
        ],
        compiler_params=pltpu.CompilerParams(
            collective_id=1, has_side_effects=True, vmem_limit_bytes=16 << 20
        ),
    )(*parts)


def per_device(hamiltonian, self_energy, guess_factor, weights, counts):
    g_all, e_real, e_imag, u_real, u_imag, steps = gather(
        weights, counts, hamiltonian, self_energy, guess_factor
    )
    arrived = leave(g_all, u_real, u_imag, *invert(e_real, e_imag, steps))
    pieces = arrived.reshape(LINE, 2, 2, 2, 2, NORB // YS)
    return pieces.transpose(5, 2, 1, 3, 0, 4).reshape(NORB // YS, 2 * FREQ)


def solution(mesh):
    return jax.shard_map(
        per_device,
        mesh=mesh,
        in_specs=(
            P(("freq", "kgrp"), None, None),
            P("freq", None, None),
            P("freq", None, None),
            P(),
            P(),
        ),
        out_specs=P(("freq", "kgrp"), None),
        check_vma=False,
    )
```

```python
import functools
import math

import jax
import jax.numpy as jnp
from jax import lax
from jax.experimental import pallas as pl
from jax.experimental.pallas import tpu as pltpu
from jax.sharding import PartitionSpec as P

chem_potential = 0.2

NORB = 64
WIDE = 2 * NORB
XS, YS, ZS, CORES = 4, 4, 8, 2
LINE = ZS * CORES
PER_FREQ = 2
N_LOCAL = XS * PER_FREQ
PAIRS = LINE // 2
FREQ = 128
KPTS = 256
BF = jnp.bfloat16
F32 = jnp.float32


def vmem():
    return pl.BlockSpec(memory_space=pltpu.VMEM)


def smem():
    return pl.BlockSpec(memory_space=pltpu.SMEM)


def hbm():
    return pl.BlockSpec(memory_space=pltpu.HBM)


def on_freq(index):
    return {"freq": index}


def greet(targets):
    barrier = pltpu.get_barrier_semaphore()
    for target in targets:
        pl.semaphore_signal(barrier, inc=1, device_id=target, device_id_type=pl.DeviceIdType.MESH)
    return lambda: pl.semaphore_wait(barrier, len(targets))


def send(src, dst, send_sem, recv_sem, target):
    return pltpu.make_async_remote_copy(
        src_ref=src,
        dst_ref=dst,
        send_sem=send_sem,
        recv_sem=recv_sem,
        device_id=target,
        device_id_type=pl.DeviceIdType.MESH,
    )


Z_ORDER = (1, 7, 4, 3, 5, 2, 6)
SLOT_DX = (0, 1, 3, 2)


def halves(value):
    high = value.astype(BF)
    low = (value - high.astype(F32)).astype(BF)
    return high, low


def dot(left, right):
    return jnp.dot(left, right, preferred_element_type=F32)


def product3(left, right):
    left_high, left_low = left
    right_high, right_low = right
    return dot(
        jnp.concatenate([left_high, left_low], 1), jnp.concatenate([right_high, right_high], 0)
    ) + dot(left_high, right_low)


def swap(value):
    return pltpu.roll(value, NORB, 1)


def lane_masks():
    rows = lax.broadcasted_iota(jnp.int32, (NORB, WIDE), 0)
    lanes = lax.broadcasted_iota(jnp.int32, (NORB, WIDE), 1)
    return lanes, lanes < NORB, rows == lanes % NORB


def right_blocks(real, imag):
    first = lane_masks()[1].astype(F32)
    first_bf, second_bf = first.astype(BF), (1.0 - first).astype(BF)

    def build(r, i):
        return jnp.concatenate(
            [
                jnp.concatenate([r * first_bf, i * first_bf], 1),
                jnp.concatenate([r * second_bf, i * second_bf], 1),
            ],
            0,
        )

    r_high, r_low = halves(real)
    i_high, i_low = halves(imag)
    return build(r_high, i_high), build(r_low, i_low)


def left_rows(real, imag):
    return halves(jnp.concatenate([real, imag], 0))


def combine(out):
    return out[:NORB, :WIDE] - out[NORB:, WIDE:], out[:NORB, WIDE:] + out[NORB:, :WIDE]


def gather_kernel(
    w_hbm, n_hbm, h_hbm, s_hbm, g_hbm,
    gall, er_ref, ei_ref, ur_ref, ui_ref, count_ref,
    w_ref, n_ref, h_ref, s_ref, hall, zall, wh, wl, hcol, hrow, gcat, gz, zcol, zrow,
    zs, zr, ps, pr, ss, sr, gs, gr, own,
):
    f = lax.axis_index("freq")
    y = lax.axis_index("kgrp")
    x, t = f // LINE, f % LINE
    z, c = t // CORES, t % CORES
    partner = on_freq(x * LINE + z * CORES + (1 - c))
    lanes, first, eye_mask = lane_masks()
    eye = eye_mask.astype(F32)
    half = NORB // 2
    row_ids = lax.broadcasted_iota(jnp.int32, (NORB, WIDE), 0)
    below, above = row_ids > lanes % NORB, row_ids < lanes % NORB

    def along_z(dz):
        return on_freq(x * LINE + (z + dz) % ZS * CORES + c)

    def along_x(dx):
        return on_freq((x + dx) % XS * LINE + t)

    def both_parts(value):
        turned = swap(value)
        return jnp.concatenate([jnp.where(first, value, turned), jnp.where(first, turned, value)], 1)

    def as_right(real, imag):
        def build(r, i):
            return jnp.concatenate([jnp.concatenate([r, i], 1), jnp.concatenate([-i, r], 1)], 0)

        real_high, real_low = halves(real)
        imag_high, imag_low = halves(imag)
        return build(real_high, imag_high), build(real_low, imag_low)

    def diagonal_columns(value):
        kept = jnp.where(eye_mask, value, 0.0)
        left = jnp.sum(jnp.where(first, kept, 0.0), 1, keepdims=True)
        right = jnp.sum(jnp.where(first, 0.0, kept), 1, keepdims=True)
        return jnp.where(first, left, right)

    def diagonal_row(value):
        return jnp.sum(jnp.where(eye_mask, value, 0.0), 0, keepdims=True)

    def freq_of(slot, b):
        return (x + XS - SLOT_DX[slot]) % XS * (PER_FREQ * LINE) + t * PER_FREQ + b

    def share_freq(b):
        matsubara = (2 * freq_of(0, b) + 1).astype(F32) * (math.pi / (2 * FREQ))
        zed = jnp.where(eye_mask, jnp.where(first, chem_potential, matsubara), 0.0) - s_ref[b]
        turned = swap(zed)
        right = jnp.concatenate([zed, jnp.where(first, -turned, turned)], 0)
        zall[b, :NORB] = product3(halves(gall[b]), halves(right))
        zall[b, NORB:] = jnp.broadcast_to(diagonal_row(zed), (8, WIDE))

    def prepare_freqs(slot):
        for b in range(PER_FREQ):
            n = slot * PER_FREQ + b
            count_ref[n : n + 1] = jnp.full((1, WIDE), n_ref[freq_of(slot, b)].astype(F32))
            product, row = zall[n, :NORB], zall[n, NORB : NORB + 1]
            gcat[n] = jnp.concatenate(halves(gall[n]), 1)
            gz[n] = both_parts(product)
            zrow[n : n + 1] = jnp.concatenate(
                [jnp.where(first[:1], row, swap(row)), jnp.where(first[:1], swap(row), row)], 1
            )
            kept = jnp.where(eye_mask, row, 0.0)
            real = jnp.sum(jnp.where(first, kept, 0.0), 1, keepdims=True)
            imag = jnp.sum(jnp.where(first, 0.0, kept), 1, keepdims=True)
            zcol[n] = jnp.concatenate(
                [jnp.broadcast_to(part, (NORB, WIDE)) for part in (real, imag, imag * imag)], 1
            )

    def prepare_pair(p):
        one, two = hall[p, 0], hall[p, 1]
        packed = jnp.concatenate(
            [jnp.where(first[:half], one, swap(two)), jnp.where(first[:half], swap(one), two)], 0
        )
        flipped = jnp.concatenate([packed, swap(packed)], 0).T[:NORB]
        real = jnp.where(above, flipped, packed)
        imag = jnp.where(above, packed, jnp.where(below, -flipped, 0.0))
        high, low = as_right(real, imag)
        wh[p] = high
        wl[p] = low
        hcol[p] = diagonal_columns(real)
        hrow[p : p + 1] = diagonal_row(real)

    await_greetings = greet(
        [along_z(dz) for dz in Z_ORDER] + [along_x(dx) for dx in (2, 1, 3)] + [partner]
    )
    first_rows = pl.ds(0, PER_FREQ)
    own_h, own_z, own_g = hall.at[0, 0], zall.at[first_rows], gall.at[first_rows]
    loads = [
        pltpu.make_async_copy(src, dst, own.at[i])
        for i, (src, dst) in enumerate(
            ((h_hbm.at[0], h_ref), (g_hbm, own_g), (s_hbm, s_ref), (w_hbm, w_ref), (n_hbm, n_ref))
        )
    ]
    for load in loads:
        load.start()
    for load in loads:
        load.wait()
    h = h_ref[...]
    folded = jnp.where(above ^ first, h, swap(h))
    own_h[...] = jnp.where(first[:half], folded[:half], folded[half:])
    for b in range(PER_FREQ):
        share_freq(b)
    prepare_freqs(0)

    def add_up(i, total):
        for j in range(16):
            total = total + w_ref[i * 16 + j]
        return total

    inv_total = 1.0 / lax.fori_loop(0, KPTS // 16, add_up, jnp.int32(0)).astype(F32)
    await_greetings()

    def z_copy(dz):
        return send(own_h, hall.at[dz, 0], zs.at[dz], zr.at[dz], along_z(dz))

    def partner_copy(dz):
        return send(hall.at[dz, 0], hall.at[dz, 1], ps.at[dz], pr.at[dz], partner)

    def freq_copies(slot):
        rows = pl.ds(slot * PER_FREQ, PER_FREQ)
        if slot < 3:
            g_from, z_from = own_g, own_z
            g_to = z_to = along_x(SLOT_DX[slot])
        else:
            g_from, g_to = gall.at[pl.ds(1 * PER_FREQ, PER_FREQ)], along_x(1)
            z_from, z_to = zall.at[pl.ds(2 * PER_FREQ, PER_FREQ)], along_x(XS - 1)
        return (
            send(g_from, gall.at[rows], gs.at[slot], gr.at[slot], g_to),
            send(z_from, zall.at[rows], ss.at[slot], sr.at[slot], z_to),
        )

    started = []

    def begin(copy):
        copy.start()
        started.append(copy)

    begin(partner_copy(0))
    for dz in Z_ORDER:
        begin(z_copy(dz))
    begin(freq_copies(1)[0])
    begin(freq_copies(2)[1])
    begin(freq_copies(1)[1])
    begin(freq_copies(2)[0])

    def residuals(p, low, high):
        left = gcat[low:high].reshape((high - low) * NORB, 2 * WIDE)
        right = wh[p]
        gh = dot(left, jnp.concatenate([right, right], 0)) + dot(left[:, :WIDE], wl[p])
        h_diag = hcol[p]
        chip = x * LINE + (z + ZS - p) % ZS * CORES
        w_one = w_ref[(chip + c) * YS + y].astype(F32) * inv_total
        w_two = w_ref[(chip + 1 - c) * YS + y].astype(F32) * inv_total
        weight = jnp.where(first[: high - low], w_one, w_two)
        d_real, d_imag = zrow[low:high, :WIDE] - hrow[pl.ds(p, 1)], zrow[low:high, WIDE:]
        inv = weight / (d_real * d_real + d_imag * d_imag)
        ur_ref[p, low:high] = d_real * inv
        ui_ref[p, low:high] = -d_imag * inv
        for n in range(low, high):
            a = gz[n] - gh[(n - low) * NORB : (n - low + 1) * NORB]
            a_real, a_imag = a[:, :WIDE], a[:, WIDE:]
            d = zcol[n]
            d_real, d_imag = d[:, :WIDE] - h_diag, d[:, WIDE : 2 * WIDE]
            inv = 1.0 / (d_real * d_real + d[:, 2 * WIDE :])
            v_real, v_imag = d_real * inv, d_imag * inv
            e_real = eye - (v_real * a_real + v_imag * a_imag)
            e_imag = v_imag * a_real - v_real * a_imag
            er_ref[n, p] = e_real
            ei_ref[n, p] = e_imag

    def arrived_z(*steps):
        for dz in steps:
            z_copy(dz).wait_recv()
            begin(partner_copy(dz))

    def await_pairs(*steps):
        for dz in steps:
            partner_copy(dz).wait_recv()

    def all_residuals(pairs, low, high):
        for p in pairs:
            residuals(p, low, high)

    def prepare_pairs(*pairs):
        for p in pairs:
            prepare_pair(p)

    near_g, near_z = freq_copies(1), freq_copies(2)
    far = freq_copies(3)
    await_pairs(0)
    prepare_pairs(0)
    all_residuals((0,), 0, 2)
    arrived_z(1, 7)
    near_g[0].wait_recv()
    begin(far[0])
    near_z[1].wait_recv()
    begin(far[1])
    arrived_z(2, 6)
    await_pairs(1, 7)
    prepare_pairs(1, 7)
    all_residuals((1, 7), 0, 2)
    near_g[1].wait_recv()
    near_z[0].wait_recv()
    arrived_z(3, 5)
    await_pairs(2, 6)
    prepare_freqs(1)
    prepare_freqs(2)
    prepare_pairs(2, 6)
    all_residuals((0, 1, 7), 2, 6)
    arrived_z(4)
    await_pairs(3, 5)
    prepare_pairs(3, 5)
    all_residuals((2, 6, 3, 5), 0, 6)
    for copy in far:
        copy.wait_recv()
    await_pairs(4)
    prepare_freqs(3)
    prepare_pairs(4)
    all_residuals((4,), 0, 6)
    all_residuals((0, 1, 7, 2, 6, 3, 5, 4), 6, 8)
    for copy in started:
        copy.wait_send()


def gather(*values):
    dma = pltpu.SemaphoreType.DMA
    powers = jax.ShapeDtypeStruct((N_LOCAL, PAIRS, NORB, WIDE), F32)
    scales = jax.ShapeDtypeStruct((PAIRS, N_LOCAL, WIDE), F32)
    totals = jax.ShapeDtypeStruct((N_LOCAL, NORB, WIDE), F32)
    counted = jax.ShapeDtypeStruct((N_LOCAL, WIDE), F32)
    return pl.pallas_call(
        gather_kernel,
        name="gather",
        out_shape=(totals, powers, powers, scales, scales, counted),
        in_specs=[hbm()] * 5,
        out_specs=(vmem(),) * 6,
        scratch_shapes=[
            pltpu.SMEM((KPTS,), jnp.int32),
            pltpu.SMEM((FREQ,), jnp.int32),
            pltpu.VMEM((NORB, WIDE), F32),
            pltpu.VMEM((PER_FREQ, NORB, WIDE), F32),
            pltpu.VMEM((ZS, CORES, NORB // 2, WIDE), F32),
            pltpu.VMEM((N_LOCAL, NORB + 8, WIDE), F32),
            pltpu.VMEM((PAIRS, WIDE, 2 * WIDE), BF),
            pltpu.VMEM((PAIRS, WIDE, 2 * WIDE), BF),
            pltpu.VMEM((PAIRS, NORB, WIDE), F32),
            pltpu.VMEM((PAIRS, WIDE), F32),
            pltpu.VMEM((N_LOCAL, NORB, 2 * WIDE), BF),
            pltpu.VMEM((N_LOCAL, NORB, 2 * WIDE), F32),
            pltpu.VMEM((N_LOCAL, NORB, 3 * WIDE), F32),
            pltpu.VMEM((N_LOCAL, 2 * WIDE), F32),
        ]
        + [dma((ZS,))] * 4
        + [dma((XS,))] * 4
        + [dma((5,))],
        compiler_params=pltpu.CompilerParams(
            collective_id=0, has_side_effects=True, vmem_limit_bytes=20 << 20
        ),
    )(*(pltpu.with_memory_space_constraint(value, pltpu.HBM) for value in values))


def power_kernel(e_in_real, e_in_imag, count_ref, er_ref, ei_ref, br_ref, bi_ref, sr_ref, si_ref, steps_ref):
    eye = lane_masks()[2].astype(F32)

    def one_step(n):
        for p in range(PAIRS):
            br_ref[n, p] = bi_ref[n, p] = jnp.zeros((NORB, WIDE), F32)

    def squares(n, real_ref, imag_ref):
        for p in range(PAIRS):
            e_real, e_imag = er_ref[n, p], ei_ref[n, p]
            real_ref[p], imag_ref[p] = combine(product3(left_rows(e_real, e_imag), right_blocks(e_real, e_imag)))

    def two_steps(n):
        squares(n, br_ref.at[n], bi_ref.at[n])

    def three_steps(n):
        squares(n, sr_ref, si_ref)
        for p in range(PAIRS):
            e_real, e_imag = er_ref[n, p], ei_ref[n, p]
            s_real, s_imag = sr_ref[p], si_ref[p]
            right = right_blocks(s_real, s_imag)
            real, imag = combine(product3(left_rows(eye + e_real, e_imag), right))
            er_ref[n, p], ei_ref[n, p] = e_real + real, e_imag + imag
            br_ref[n, p], bi_ref[n, p] = combine(product3(left_rows(s_real, s_imag), right))

    for n in range(N_LOCAL):
        steps_ref[n] = jnp.max(count_ref[n : n + 1])

    def one_freq(n, carry):
        steps = steps_ref[n]
        pl.when(steps < 1.5)(functools.partial(one_step, n))
        pl.when((steps > 1.5) & (steps < 2.5))(functools.partial(two_steps, n))
        pl.when(steps > 2.5)(functools.partial(three_steps, n))
        return carry

    lax.fori_loop(0, N_LOCAL, one_freq, 0)


def invert(*residuals_and_counts):
    slots = pltpu.VMEM((PAIRS, NORB, WIDE), F32)
    powers = jax.ShapeDtypeStruct((N_LOCAL, PAIRS, NORB, WIDE), F32)
    return pl.pallas_call(
        power_kernel,
        name="invert",
        out_shape=(powers,) * 4,
        in_specs=[vmem()] * 3,
        out_specs=(vmem(),) * 4,
        input_output_aliases={0: 0, 1: 1},
        scratch_shapes=[slots] * 2 + [pltpu.SMEM((N_LOCAL,), F32)],
        compiler_params=pltpu.CompilerParams(vmem_limit_bytes=24 << 20),
    )(*residuals_and_counts)


def exit_kernel(
    g_ref, ur_ref, ui_ref, er_ref, ei_ref, br_ref, bi_ref, q_ref, o_ref, t_ref, landed, rows_ref, as_, ar, bs, br
):
    f = lax.axis_index("freq")
    y = lax.axis_index("kgrp")
    x, t = f // LINE, f % LINE
    z, c = t // CORES, t % CORES
    plane = [(dx, dy) for dx in (2, 1, 3, 0) for dy in (2, 1, 3, 0) if dx or dy]
    plane.sort(key=lambda step: -min(step[0], XS - step[0]) - min(step[1], YS - step[1]))
    line = [(dz, dc) for dz in (4, 3, 5, 2, 6, 1, 7, 0) for dc in (1, 0) if dz or dc]

    def in_plane(dx, dy):
        return {"freq": (x + dx) % XS * LINE + t, "kgrp": (y + dy) % YS}

    def place(dz, dc):
        return (z + dz) % ZS * CORES + (c + dc) % CORES

    await_greetings = greet([q for d, e in zip(plane, line) for q in (in_plane(*d), on_freq(x * LINE + place(*e)))])
    lanes, first, eye_mask = lane_masks()
    eye = eye_mask.astype(F32)
    quarter = lanes % NORB // (NORB // YS)

    def last_product(n, carry):
        totals = [None, None]
        for p in range(PAIRS):
            x_real, x_imag = eye + br_ref[n, p], bi_ref[n, p]
            u_real, u_imag = ur_ref[p, pl.ds(n, 1)], ui_ref[p, pl.ds(n, 1)]
            x_real, x_imag = x_real * u_real - x_imag * u_imag, x_real * u_imag + x_imag * u_real
            right = jnp.concatenate(
                [jnp.where(first, x_real, swap(x_imag)), jnp.where(first, swap(x_real), x_imag)], 0
            )
            right = jnp.concatenate(halves(right), 1)
            left = jnp.concatenate(left_rows(eye + er_ref[n, p], ei_ref[n, p]), 1)
            out = dot(left, jnp.concatenate([right, right], 0))
            totals[p % 2] = out if p < 2 else totals[p % 2] + out
        total = totals[0] + totals[1]
        total = total[:, :WIDE] + total[:, WIDE:]
        turned = swap(total[NORB:])
        t_ref[n] = total[:NORB] + jnp.where(first, -turned, turned)
        return carry

    lax.fori_loop(0, N_LOCAL, last_product, 0, unroll=2)
    for n_high in range(2):
        mixed = [None] * YS
        for n_low in range(4):
            dx = (x + XS - n_high * 2 - n_low // 2) % XS
            n = (dx + dx // 2 * (5 - 2 * dx)) * PER_FREQ + n_low % 2
            g = g_ref[n]
            turned = jnp.where(first, -swap(g), swap(g))
            right = jnp.concatenate(halves(jnp.concatenate([g, turned], 0)), 1)
            both = dot(jnp.concatenate(halves(t_ref[n]), 1), jnp.concatenate([right, right], 0))
            value = both[:, :WIDE] + both[:, WIDE:]
            for to_y in range(YS):
                shift = (n_low - to_y) * (NORB // YS) % WIDE
                moved = pltpu.roll(value, shift, 1) if shift else value
                mixed[to_y] = moved if n_low == 0 else jnp.where(quarter == n_low, moved, mixed[to_y])
        for to_y in range(YS):
            for to_x in range(XS):
                o_ref[to_x, to_y, n_high] = mixed[to_y][to_x * LINE : (to_x + 1) * LINE]
    await_greetings()
    started = []
    for dx, dy in plane:
        slot = dx * YS + dy
        copy = send(
            o_ref.at[(x + dx) % XS, (y + dy) % YS], landed.at[slot], as_.at[slot], ar.at[slot], in_plane(dx, dy)
        )
        copy.start()
        started.append(copy)
    total = o_ref[x, y]
    for dx, dy in reversed(plane):
        slot = dx * YS + dy
        send(o_ref.at[x, y], landed.at[slot], as_.at[slot], ar.at[slot], in_plane(dx, dy)).wait_recv()
        total = total + landed[slot]
    for to in range(LINE):
        for n_high in range(2):
            rows_ref[to, n_high : n_high + 1] = total[n_high, to : to + 1]
    for dz, dc in line:
        slot = dz * CORES + dc
        to = place(dz, dc)
        copy = send(rows_ref.at[to], q_ref.at[t], bs.at[slot], br.at[slot], on_freq(x * LINE + to))
        copy.start()
        started.append(copy)
    q_ref[pl.ds(t, 1)] = rows_ref[pl.ds(t, 1)]
    for dz, dc in reversed(line):
        slot = dz * CORES + dc
        source = (z + ZS - dz) % ZS * CORES + (c + CORES - dc) % CORES
        send(rows_ref.at[source], q_ref.at[source], bs.at[slot], br.at[slot], on_freq(x * LINE + place(dz, dc))).wait_recv()
    for copy in started:
        copy.wait_send()


def leave(*parts):
    dma = pltpu.SemaphoreType.DMA
    return pl.pallas_call(
        exit_kernel,
        name="leave",
        out_shape=jax.ShapeDtypeStruct((LINE, 2, WIDE), F32),
        in_specs=[vmem()] * 7,
        out_specs=vmem(),
        scratch_shapes=[
            pltpu.VMEM((XS, YS, 2, LINE, WIDE), F32),
            pltpu.VMEM((N_LOCAL, NORB, WIDE), F32),
            pltpu.VMEM((XS * YS, 2, LINE, WIDE), F32),
            pltpu.VMEM((LINE, 2, WIDE), F32),
            dma((XS * YS,)),
            dma((XS * YS,)),
            dma((LINE,)),
            dma((LINE,)),
        ],
        compiler_params=pltpu.CompilerParams(
            collective_id=1, has_side_effects=True, vmem_limit_bytes=16 << 20
        ),
    )(*parts)


def per_device(hamiltonian, self_energy, guess_factor, weights, counts):
    g_all, e_real, e_imag, u_real, u_imag, steps = gather(
        weights, counts, hamiltonian, self_energy, guess_factor
    )
    arrived = leave(g_all, u_real, u_imag, *invert(e_real, e_imag, steps))
    pieces = arrived.reshape(LINE, 2, 2, 2, 2, NORB // YS)
    return pieces.transpose(5, 2, 1, 3, 0, 4).reshape(NORB // YS, 2 * FREQ)


def solution(mesh):
    return jax.shard_map(
        per_device,
        mesh=mesh,
        in_specs=(
            P(("freq", "kgrp"), None, None),
            P("freq", None, None),
            P("freq", None, None),
            P(),
            P(),
        ),
        out_specs=P(("freq", "kgrp"), None),
        check_vma=False,
    )
```

```python
import functools
import math

import jax
import jax.numpy as jnp
from jax import lax
from jax.experimental import pallas as pl
from jax.experimental.pallas import tpu as pltpu
from jax.sharding import PartitionSpec as P

chem_potential = 0.2

NORB = 64
WIDE = 2 * NORB
XS, YS, ZS, CORES = 4, 4, 8, 2
LINE = ZS * CORES
PER_FREQ = 2
N_LOCAL = XS * PER_FREQ
PAIRS = LINE // 2
FREQ = 128
KPTS = 256
BF = jnp.bfloat16
F32 = jnp.float32


def vmem():
    return pl.BlockSpec(memory_space=pltpu.VMEM)


def smem():
    return pl.BlockSpec(memory_space=pltpu.SMEM)


def hbm():
    return pl.BlockSpec(memory_space=pltpu.HBM)


def on_freq(index):
    return {"freq": index}


def greet(targets):
    barrier = pltpu.get_barrier_semaphore()
    for target in targets:
        pl.semaphore_signal(barrier, inc=1, device_id=target, device_id_type=pl.DeviceIdType.MESH)
    return lambda: pl.semaphore_wait(barrier, len(targets))


def send(src, dst, send_sem, recv_sem, target):
    return pltpu.make_async_remote_copy(
        src_ref=src,
        dst_ref=dst,
        send_sem=send_sem,
        recv_sem=recv_sem,
        device_id=target,
        device_id_type=pl.DeviceIdType.MESH,
    )


Z_ORDER = (1, 7, 4, 3, 5, 2, 6)
SLOT_DX = (0, 1, 3, 2)


def halves(value):
    high = value.astype(BF)
    low = (value - high.astype(F32)).astype(BF)
    return high, low


def dot(left, right):
    return jnp.dot(left, right, preferred_element_type=F32)


def product3(left, right):
    left_high, left_low = left
    right_high, right_low = right
    return dot(
        jnp.concatenate([left_high, left_low], 1), jnp.concatenate([right_high, right_high], 0)
    ) + dot(left_high, right_low)


def swap(value):
    return pltpu.roll(value, NORB, 1)


def lane_masks():
    rows = lax.broadcasted_iota(jnp.int32, (NORB, WIDE), 0)
    lanes = lax.broadcasted_iota(jnp.int32, (NORB, WIDE), 1)
    return lanes, lanes < NORB, rows == lanes % NORB


def right_blocks(real, imag):
    first = lane_masks()[1].astype(F32)
    first_bf, second_bf = first.astype(BF), (1.0 - first).astype(BF)

    def build(r, i):
        return jnp.concatenate(
            [
                jnp.concatenate([r * first_bf, i * first_bf], 1),
                jnp.concatenate([r * second_bf, i * second_bf], 1),
            ],
            0,
        )

    r_high, r_low = halves(real)
    i_high, i_low = halves(imag)
    return build(r_high, i_high), build(r_low, i_low)


def left_rows(real, imag):
    return halves(jnp.concatenate([real, imag], 0))


def combine(out):
    return out[:NORB, :WIDE] - out[NORB:, WIDE:], out[:NORB, WIDE:] + out[NORB:, :WIDE]


def gather_kernel(
    w_hbm, n_hbm, h_hbm, s_hbm, g_hbm,
    gall, er_ref, ei_ref, ur_ref, ui_ref, count_ref,
    w_ref, n_ref, h_ref, s_ref, hall, zall, wh, wl, hcol, hrow, gcat, gz, zcol, zrow,
    zs, zr, ps, pr, ss, sr, gs, gr, own,
):
    f = lax.axis_index("freq")
    y = lax.axis_index("kgrp")
    x, t = f // LINE, f % LINE
    z, c = t // CORES, t % CORES
    partner = on_freq(x * LINE + z * CORES + (1 - c))
    lanes, first, eye_mask = lane_masks()
    eye = eye_mask.astype(F32)
    half = NORB // 2
    row_ids = lax.broadcasted_iota(jnp.int32, (NORB, WIDE), 0)
    below, above = row_ids > lanes % NORB, row_ids < lanes % NORB

    def along_z(dz):
        return on_freq(x * LINE + (z + dz) % ZS * CORES + c)

    def along_x(dx):
        return on_freq((x + dx) % XS * LINE + t)

    def both_parts(value):
        turned = swap(value)
        return jnp.concatenate([jnp.where(first, value, turned), jnp.where(first, turned, value)], 1)

    def as_right(real, imag):
        def build(r, i):
            return jnp.concatenate([jnp.concatenate([r, i], 1), jnp.concatenate([-i, r], 1)], 0)

        real_high, real_low = halves(real)
        imag_high, imag_low = halves(imag)
        return build(real_high, imag_high), build(real_low, imag_low)

    def diagonal_columns(value):
        kept = jnp.where(eye_mask, value, 0.0)
        left = jnp.sum(jnp.where(first, kept, 0.0), 1, keepdims=True)
        right = jnp.sum(jnp.where(first, 0.0, kept), 1, keepdims=True)
        return jnp.where(first, left, right)

    def diagonal_row(value):
        return jnp.sum(jnp.where(eye_mask, value, 0.0), 0, keepdims=True)

    def freq_of(slot, b):
        return (x + XS - SLOT_DX[slot]) % XS * (PER_FREQ * LINE) + t * PER_FREQ + b

    def share_freq(b):
        matsubara = (2 * freq_of(0, b) + 1).astype(F32) * (math.pi / (2 * FREQ))
        zed = jnp.where(eye_mask, jnp.where(first, chem_potential, matsubara), 0.0) - s_ref[b]
        turned = swap(zed)
        right = jnp.concatenate([zed, jnp.where(first, -turned, turned)], 0)
        zall[b, :NORB] = product3(halves(gall[b]), halves(right))
        zall[b, NORB:] = jnp.broadcast_to(diagonal_row(zed), (8, WIDE))

    def prepare_freqs(slot):
        for b in range(PER_FREQ):
            n = slot * PER_FREQ + b
            count_ref[n : n + 1] = jnp.full((1, WIDE), n_ref[freq_of(slot, b)].astype(F32))
            product, row = zall[n, :NORB], zall[n, NORB : NORB + 1]
            gcat[n] = jnp.concatenate(halves(gall[n]), 1)
            gz[n] = both_parts(product)
            zrow[n : n + 1] = jnp.concatenate(
                [jnp.where(first[:1], row, swap(row)), jnp.where(first[:1], swap(row), row)], 1
            )
            kept = jnp.where(eye_mask, row, 0.0)
            real = jnp.sum(jnp.where(first, kept, 0.0), 1, keepdims=True)
            imag = jnp.sum(jnp.where(first, 0.0, kept), 1, keepdims=True)
            zcol[n] = jnp.concatenate(
                [jnp.broadcast_to(part, (NORB, WIDE)) for part in (real, imag, imag * imag)], 1
            )

    def prepare_pair(p):
        one, two = hall[p, 0], hall[p, 1]
        packed = jnp.concatenate(
            [jnp.where(first[:half], one, swap(two)), jnp.where(first[:half], swap(one), two)], 0
        )
        flipped = jnp.concatenate([packed, swap(packed)], 0).T[:NORB]
        real = jnp.where(above, flipped, packed)
        imag = jnp.where(above, packed, jnp.where(below, -flipped, 0.0))
        high, low = as_right(real, imag)
        wh[p] = high
        wl[p] = low
        hcol[p] = diagonal_columns(real)
        hrow[p : p + 1] = diagonal_row(real)

    await_greetings = greet(
        [along_z(dz) for dz in Z_ORDER] + [along_x(dx) for dx in (2, 1, 3)] + [partner]
    )
    first_rows = pl.ds(0, PER_FREQ)
    own_h, own_z, own_g = hall.at[0, 0], zall.at[first_rows], gall.at[first_rows]
    loads = [
        pltpu.make_async_copy(src, dst, own.at[i])
        for i, (src, dst) in enumerate(
            ((h_hbm.at[0], h_ref), (g_hbm, own_g), (s_hbm, s_ref), (w_hbm, w_ref), (n_hbm, n_ref))
        )
    ]
    for load in loads:
        load.start()
    for load in loads:
        load.wait()
    h = h_ref[...]
    folded = jnp.where(above ^ first, h, swap(h))
    own_h[...] = jnp.where(first[:half], folded[:half], folded[half:])
    for b in range(PER_FREQ):
        share_freq(b)
    prepare_freqs(0)

    def add_up(i, total):
        for j in range(16):
            total = total + w_ref[i * 16 + j]
        return total

    inv_total = 1.0 / lax.fori_loop(0, KPTS // 16, add_up, jnp.int32(0)).astype(F32)
    await_greetings()

    def z_copy(dz):
        return send(own_h, hall.at[dz, 0], zs.at[dz], zr.at[dz], along_z(dz))

    def partner_copy(dz):
        return send(hall.at[dz, 0], hall.at[dz, 1], ps.at[dz], pr.at[dz], partner)

    def freq_copies(slot):
        rows = pl.ds(slot * PER_FREQ, PER_FREQ)
        if slot < 3:
            g_from, z_from = own_g, own_z
            g_to = z_to = along_x(SLOT_DX[slot])
        else:
            g_from, g_to = gall.at[pl.ds(1 * PER_FREQ, PER_FREQ)], along_x(1)
            z_from, z_to = zall.at[pl.ds(2 * PER_FREQ, PER_FREQ)], along_x(XS - 1)
        return (
            send(g_from, gall.at[rows], gs.at[slot], gr.at[slot], g_to),
            send(z_from, zall.at[rows], ss.at[slot], sr.at[slot], z_to),
        )

    started = []

    def begin(copy):
        copy.start()
        started.append(copy)

    begin(partner_copy(0))
    for dz in Z_ORDER:
        begin(z_copy(dz))
    begin(freq_copies(1)[0])
    begin(freq_copies(2)[1])
    begin(freq_copies(1)[1])
    begin(freq_copies(2)[0])

    def residuals(p, low, high):
        left = gcat[low:high].reshape((high - low) * NORB, 2 * WIDE)
        right = wh[p]
        gh = dot(left, jnp.concatenate([right, right], 0)) + dot(left[:, :WIDE], wl[p])
        h_diag = hcol[p]
        chip = x * LINE + (z + ZS - p) % ZS * CORES
        w_one = w_ref[(chip + c) * YS + y].astype(F32) * inv_total
        w_two = w_ref[(chip + 1 - c) * YS + y].astype(F32) * inv_total
        weight = jnp.where(first[: high - low], w_one, w_two)
        d_real, d_imag = zrow[low:high, :WIDE] - hrow[pl.ds(p, 1)], zrow[low:high, WIDE:]
        inv = weight / (d_real * d_real + d_imag * d_imag)
        ur_ref[p, low:high] = d_real * inv
        ui_ref[p, low:high] = -d_imag * inv
        for n in range(low, high):
            a = gz[n] - gh[(n - low) * NORB : (n - low + 1) * NORB]
            a_real, a_imag = a[:, :WIDE], a[:, WIDE:]
            d = zcol[n]
            d_real, d_imag = d[:, :WIDE] - h_diag, d[:, WIDE : 2 * WIDE]
            inv = 1.0 / (d_real * d_real + d[:, 2 * WIDE :])
            v_real, v_imag = d_real * inv, d_imag * inv
            e_real = eye - (v_real * a_real + v_imag * a_imag)
            e_imag = v_imag * a_real - v_real * a_imag
            er_ref[n, p] = e_real
            ei_ref[n, p] = e_imag

    def arrived_z(*steps):
        for dz in steps:
            z_copy(dz).wait_recv()
            begin(partner_copy(dz))

    def await_pairs(*steps):
        for dz in steps:
            partner_copy(dz).wait_recv()

    def all_residuals(pairs, low, high):
        for p in pairs:
            residuals(p, low, high)

    def prepare_pairs(*pairs):
        for p in pairs:
            prepare_pair(p)

    near_g, near_z = freq_copies(1), freq_copies(2)
    far = freq_copies(3)
    await_pairs(0)
    prepare_pairs(0)
    all_residuals((0,), 0, 2)
    arrived_z(1, 7)
    near_g[0].wait_recv()
    begin(far[0])
    near_z[1].wait_recv()
    begin(far[1])
    arrived_z(2, 6)
    await_pairs(1, 7)
    prepare_pairs(1, 7)
    all_residuals((1, 7), 0, 2)
    near_g[1].wait_recv()
    near_z[0].wait_recv()
    arrived_z(3, 5)
    await_pairs(2, 6)
    prepare_freqs(1)
    prepare_freqs(2)
    prepare_pairs(2, 6)
    all_residuals((0, 1, 7), 2, 6)
    arrived_z(4)
    await_pairs(3, 5)
    prepare_pairs(3, 5)
    all_residuals((2, 6, 3, 5), 0, 6)
    for copy in far:
        copy.wait_recv()
    await_pairs(4)
    prepare_freqs(3)
    prepare_pairs(4)
    all_residuals((4,), 0, 6)
    all_residuals((0, 1, 7, 2, 6, 3, 5, 4), 6, 8)
    for copy in started:
        copy.wait_send()


def gather(*values):
    dma = pltpu.SemaphoreType.DMA
    powers = jax.ShapeDtypeStruct((N_LOCAL, PAIRS, NORB, WIDE), F32)
    scales = jax.ShapeDtypeStruct((PAIRS, N_LOCAL, WIDE), F32)
    totals = jax.ShapeDtypeStruct((N_LOCAL, NORB, WIDE), F32)
    counted = jax.ShapeDtypeStruct((N_LOCAL, WIDE), F32)
    return pl.pallas_call(
        gather_kernel,
        name="gather",
        out_shape=(totals, powers, powers, scales, scales, counted),
        in_specs=[hbm()] * 5,
        out_specs=(vmem(),) * 6,
        scratch_shapes=[
            pltpu.SMEM((KPTS,), jnp.int32),
            pltpu.SMEM((FREQ,), jnp.int32),
            pltpu.VMEM((NORB, WIDE), F32),
            pltpu.VMEM((PER_FREQ, NORB, WIDE), F32),
            pltpu.VMEM((ZS, CORES, NORB // 2, WIDE), F32),
            pltpu.VMEM((N_LOCAL, NORB + 8, WIDE), F32),
            pltpu.VMEM((PAIRS, WIDE, 2 * WIDE), BF),
            pltpu.VMEM((PAIRS, WIDE, 2 * WIDE), BF),
            pltpu.VMEM((PAIRS, NORB, WIDE), F32),
            pltpu.VMEM((PAIRS, WIDE), F32),
            pltpu.VMEM((N_LOCAL, NORB, 2 * WIDE), BF),
            pltpu.VMEM((N_LOCAL, NORB, 2 * WIDE), F32),
            pltpu.VMEM((N_LOCAL, NORB, 3 * WIDE), F32),
            pltpu.VMEM((N_LOCAL, 2 * WIDE), F32),
        ]
        + [dma((ZS,))] * 4
        + [dma((XS,))] * 4
        + [dma((5,))],
        compiler_params=pltpu.CompilerParams(
            collective_id=0, has_side_effects=True, vmem_limit_bytes=20 << 20
        ),
    )(*(pltpu.with_memory_space_constraint(value, pltpu.HBM) for value in values))


def power_kernel(e_in_real, e_in_imag, count_ref, er_ref, ei_ref, br_ref, bi_ref, sr_ref, si_ref, steps_ref):
    eye = lane_masks()[2].astype(F32)

    def squares(n, real_ref, imag_ref):
        for p in range(PAIRS):
            e_real, e_imag = er_ref[n, p], ei_ref[n, p]
            real_ref[p], imag_ref[p] = combine(product3(left_rows(e_real, e_imag), right_blocks(e_real, e_imag)))

    def two_steps(n):
        squares(n, br_ref.at[n], bi_ref.at[n])

    def three_steps(n):
        squares(n, sr_ref, si_ref)
        for p in range(PAIRS):
            e_real, e_imag = er_ref[n, p], ei_ref[n, p]
            s_real, s_imag = sr_ref[p], si_ref[p]
            right = right_blocks(s_real, s_imag)
            real, imag = combine(product3(left_rows(eye + e_real, e_imag), right))
            er_ref[n, p], ei_ref[n, p] = e_real + real, e_imag + imag
            br_ref[n, p], bi_ref[n, p] = combine(product3(left_rows(s_real, s_imag), right))

    for n in range(N_LOCAL):
        steps_ref[n] = count_ref[n, 0]

    def one_freq(n, carry):
        steps = steps_ref[n]
        pl.when((steps > 1.5) & (steps < 2.5))(functools.partial(two_steps, n))
        pl.when(steps > 2.5)(functools.partial(three_steps, n))
        return carry

    lax.fori_loop(0, N_LOCAL, one_freq, 0)


def invert(*residuals_and_counts):
    slots = pltpu.VMEM((PAIRS, NORB, WIDE), F32)
    powers = jax.ShapeDtypeStruct((N_LOCAL, PAIRS, NORB, WIDE), F32)
    return pl.pallas_call(
        power_kernel,
        name="invert",
        out_shape=(powers,) * 4,
        in_specs=[vmem()] * 3,
        out_specs=(vmem(),) * 4,
        input_output_aliases={0: 0, 1: 1},
        scratch_shapes=[slots] * 2 + [pltpu.SMEM((N_LOCAL,), F32)],
        compiler_params=pltpu.CompilerParams(vmem_limit_bytes=24 << 20),
    )(*residuals_and_counts)


def exit_kernel(
    g_ref, ur_ref, ui_ref, count_ref, er_ref, ei_ref, br_ref, bi_ref, q_ref, o_ref, t_ref, landed, rows_ref, as_, ar, bs, br
):
    f = lax.axis_index("freq")
    y = lax.axis_index("kgrp")
    x, t = f // LINE, f % LINE
    z, c = t // CORES, t % CORES
    plane = [(dx, dy) for dx in (2, 1, 3, 0) for dy in (2, 1, 3, 0) if dx or dy]
    plane.sort(key=lambda step: -min(step[0], XS - step[0]) - min(step[1], YS - step[1]))
    line = [(dz, dc) for dz in (4, 3, 5, 2, 6, 1, 7, 0) for dc in (1, 0) if dz or dc]

    def in_plane(dx, dy):
        return {"freq": (x + dx) % XS * LINE + t, "kgrp": (y + dy) % YS}

    def place(dz, dc):
        return (z + dz) % ZS * CORES + (c + dc) % CORES

    await_greetings = greet([q for d, e in zip(plane, line) for q in (in_plane(*d), on_freq(x * LINE + place(*e)))])
    lanes, first, eye_mask = lane_masks()
    eye = eye_mask.astype(F32)
    quarter = lanes % NORB // (NORB // YS)

    def last_product(n, carry):
        several = count_ref[pl.ds(n, 1)] > 1.5
        totals = [None, None]
        for p in range(PAIRS):
            x_real = jnp.where(several, eye + br_ref[n, p], eye)
            x_imag = jnp.where(several, bi_ref[n, p], 0.0)
            u_real, u_imag = ur_ref[p, pl.ds(n, 1)], ui_ref[p, pl.ds(n, 1)]
            x_real, x_imag = x_real * u_real - x_imag * u_imag, x_real * u_imag + x_imag * u_real
            right = jnp.concatenate(
                [jnp.where(first, x_real, swap(x_imag)), jnp.where(first, swap(x_real), x_imag)], 0
            )
            right = jnp.concatenate(halves(right), 1)
            left = jnp.concatenate(left_rows(eye + er_ref[n, p], ei_ref[n, p]), 1)
            out = dot(left, jnp.concatenate([right, right], 0))
            totals[p % 2] = out if p < 2 else totals[p % 2] + out
        total = totals[0] + totals[1]
        total = total[:, :WIDE] + total[:, WIDE:]
        turned = swap(total[NORB:])
        t_ref[n] = total[:NORB] + jnp.where(first, -turned, turned)
        return carry

    lax.fori_loop(0, N_LOCAL, last_product, 0, unroll=2)
    for n_high in range(2):
        mixed = [None] * YS
        for n_low in range(4):
            dx = (x + XS - n_high * 2 - n_low // 2) % XS
            n = (dx + dx // 2 * (5 - 2 * dx)) * PER_FREQ + n_low % 2
            g = g_ref[n]
            turned = jnp.where(first, -swap(g), swap(g))
            right = jnp.concatenate(halves(jnp.concatenate([g, turned], 0)), 1)
            both = dot(jnp.concatenate(halves(t_ref[n]), 1), jnp.concatenate([right, right], 0))
            value = both[:, :WIDE] + both[:, WIDE:]
            for to_y in range(YS):
                shift = (n_low - to_y) * (NORB // YS) % WIDE
                moved = pltpu.roll(value, shift, 1) if shift else value
                mixed[to_y] = moved if n_low == 0 else jnp.where(quarter == n_low, moved, mixed[to_y])
        for to_y in range(YS):
            for to_x in range(XS):
                o_ref[to_x, to_y, n_high] = mixed[to_y][to_x * LINE : (to_x + 1) * LINE]
    await_greetings()
    started = []
    for dx, dy in plane:
        slot = dx * YS + dy
        copy = send(
            o_ref.at[(x + dx) % XS, (y + dy) % YS], landed.at[slot], as_.at[slot], ar.at[slot], in_plane(dx, dy)
        )
        copy.start()
        started.append(copy)
    total = o_ref[x, y]
    for dx, dy in reversed(plane):
        slot = dx * YS + dy
        send(o_ref.at[x, y], landed.at[slot], as_.at[slot], ar.at[slot], in_plane(dx, dy)).wait_recv()
        total = total + landed[slot]
    for to in range(LINE):
        for n_high in range(2):
            rows_ref[to, n_high : n_high + 1] = total[n_high, to : to + 1]
    for dz, dc in line:
        slot = dz * CORES + dc
        to = place(dz, dc)
        copy = send(rows_ref.at[to], q_ref.at[t], bs.at[slot], br.at[slot], on_freq(x * LINE + to))
        copy.start()
        started.append(copy)
    q_ref[pl.ds(t, 1)] = rows_ref[pl.ds(t, 1)]
    for dz, dc in reversed(line):
        slot = dz * CORES + dc
        source = (z + ZS - dz) % ZS * CORES + (c + CORES - dc) % CORES
        send(rows_ref.at[source], q_ref.at[source], bs.at[slot], br.at[slot], on_freq(x * LINE + place(dz, dc))).wait_recv()
    for copy in started:
        copy.wait_send()


def leave(*parts):
    dma = pltpu.SemaphoreType.DMA
    return pl.pallas_call(
        exit_kernel,
        name="leave",
        out_shape=jax.ShapeDtypeStruct((LINE, 2, WIDE), F32),
        in_specs=[vmem()] * 8,
        out_specs=vmem(),
        scratch_shapes=[
            pltpu.VMEM((XS, YS, 2, LINE, WIDE), F32),
            pltpu.VMEM((N_LOCAL, NORB, WIDE), F32),
            pltpu.VMEM((XS * YS, 2, LINE, WIDE), F32),
            pltpu.VMEM((LINE, 2, WIDE), F32),
            dma((XS * YS,)),
            dma((XS * YS,)),
            dma((LINE,)),
            dma((LINE,)),
        ],
        compiler_params=pltpu.CompilerParams(
            collective_id=1, has_side_effects=True, vmem_limit_bytes=16 << 20
        ),
    )(*parts)


def per_device(hamiltonian, self_energy, guess_factor, weights, counts):
    g_all, e_real, e_imag, u_real, u_imag, steps = gather(
        weights, counts, hamiltonian, self_energy, guess_factor
    )
    arrived = leave(g_all, u_real, u_imag, steps, *invert(e_real, e_imag, steps))
    pieces = arrived.reshape(LINE, 2, 2, 2, 2, NORB // YS)
    return pieces.transpose(5, 2, 1, 3, 0, 4).reshape(NORB // YS, 2 * FREQ)


def solution(mesh):
    return jax.shard_map(
        per_device,
        mesh=mesh,
        in_specs=(
            P(("freq", "kgrp"), None, None),
            P("freq", None, None),
            P("freq", None, None),
            P(),
            P(),
        ),
        out_specs=P(("freq", "kgrp"), None),
        check_vma=False,
    )
```
